256 devices in a mesh: gx: 4 (over y), gy: 8 (over x, core), gz: 8 (over z).
Axes of the slice: x: 4, y: 4, z: 8, core: 2. Of those that a mesh axis runs over, the one named last changes fastest.
Arguments:
- flow_state: float32 [5, 256, 128, 512], P(None, 'gz', 'gy', 'gx'), may hold values from -5 to 120, as said below
- advection: float32 [3, 5], replicated, may hold values from -400 to 400, as said below
- inverse_x: float32 [5, 128, 128], replicated, may hold values from -1 to 1, as said below
- inverse_y: float32 [5, 16, 16], replicated, may hold values from -1 to 1, as said below
- inverse_z: float32 [5, 32, 32], replicated, may hold values from -1 to 1, as said below
- reduced_x: float32 [5, 16, 16], replicated, as said below
- reduced_y: float32 [5, 32, 32], replicated, as said below
- reduced_z: float32 [5, 32, 32], replicated, as said below
Outputs:
- update: float32 [5, 256, 128, 512], P(None, 'gz', 'gy', 'gx')
- rms_norm: float32 [5], replicated
The draws below stay inside these ranges and needn't reach their ends.
Inputs may be any that keep to these rules, and one draw needn't show every extreme that they name: flow_state[0] (density) lies between 0.5 and 2, and flow_state[4] / density minus half the squared velocity is at least 0.6 in every cell. `advection`: every entry has magnitude between 100 and 400. inverse_x[v] is the inverse of the 128 x 128 matrix with 4 on the diagonal, advection[0, v] / 2 - 2 just above it, -advection[0, v] / 2 - 2 just below it and 0.5 two places off it. inverse_y[v] is the inverse of the 16 x 16 matrix built likewise from advection[1, v]. inverse_z[v] is the inverse of the 32 x 32 matrix built likewise from advection[2, v]. reduced_x[v] is the inverse of I + K, K being the boundary rows and columns of the block inverses times the coupling between blocks, so that S_x equals the exact solution of the banded system along whole x lines with nothing beyond the grid's ends. reduced_y[v] is built likewise for y lines. reduced_z[v] is built likewise for z lines.
All inputs are finite; a program needn't handle non-finite values.
Results may differ from the reference program's by a relative error of at most 0.0002.
Values sent between devices are 32-bit elements.
A program may use at most 64 MiB of HBM per device.

```python
import jax
import jax.numpy as jnp
import numpy as np
from jax import lax

VARS = 5
CX = 128
CY = 16
CZ = 32
NX = 512
NY = 128
NZ = 256


fourth_coef = 0.5


def advection_table(key):
    subkeys = jax.random.split(jax.random.fold_in(key, 17), 2)
    magnitude = 100.0 * 4.0 ** jax.random.uniform(subkeys[0], (3, VARS), jnp.float32)
    signs = 2.0 * jax.random.randint(subkeys[1], (3, VARS), 0, 2).astype(jnp.float32) - 1.0
    return signs * magnitude


def band_matrix(length, speed):
    identity = jnp.eye(length, dtype=jnp.float32)
    upper_band = jnp.eye(length, k=1, dtype=jnp.float32)
    lower_band = jnp.eye(length, k=-1, dtype=jnp.float32)
    second_band = jnp.eye(length, k=2, dtype=jnp.float32) + jnp.eye(length, k=-2, dtype=jnp.float32)
    return (1.0 + 6.0 * fourth_coef) * identity + (0.5 * speed - 4.0 * fourth_coef) * upper_band + (-0.5 * speed - 4.0 * fourth_coef) * lower_band + fourth_coef * second_band


def block_inverse(key, direction, block_len):
    speeds = advection_table(key)[direction]
    return jax.vmap(lambda speed: jnp.linalg.inv(band_matrix(block_len, speed)))(speeds)


def reduced_inverse(key, direction, block_len, blocks):
    speeds = advection_table(key)[direction]
    length = block_len * blocks
    picked = (block_len * np.arange(blocks)[:, None] + np.array([0, 1, block_len - 2, block_len - 1])[None, :]).reshape(-1)

    def single(speed):
        local_block = band_matrix(block_len, speed)
        whole_line = band_matrix(length, speed)
        spread_inv = jnp.kron(jnp.eye(blocks, dtype=jnp.float32), jnp.linalg.inv(local_block))
        coupling = whole_line - jnp.kron(jnp.eye(blocks, dtype=jnp.float32), local_block)
        product = jnp.dot(spread_inv, coupling, precision=lax.Precision.HIGHEST)
        reduced_k = product[picked][:, picked]
        return jnp.linalg.inv(jnp.eye(4 * blocks, dtype=jnp.float32) + reduced_k)
    return jax.vmap(single)(speeds)


def region_envelope(key):
    phases = jax.random.uniform(jax.random.fold_in(key, 29), (2,), jnp.float32, 0.0, 6.2831853)
    along_z = jnp.arange(NZ, dtype=jnp.float32) * (6.2831853 / NZ)
    along_y = jnp.arange(NY, dtype=jnp.float32) * (6.2831853 / NY)
    shape_z = 0.5 + 0.5 * jnp.sin(along_z + phases[0])
    shape_y = 0.5 + 0.5 * jnp.cos(along_y + phases[1])
    envelope = 0.2 + 0.8 * shape_z[:, None] * shape_y[None, :]
    return envelope[:, :, None]


def draw_flow_state(key, part):
    subkeys = jax.random.split(jax.random.fold_in(key, 11), 6)
    grid_shape = (NZ, NY, NX)
    envelope = region_envelope(key)
    density = 0.5 * 4.0 ** jax.random.uniform(subkeys[0], grid_shape, jnp.float32)
    velocity = jnp.clip(0.6 * jax.random.normal(subkeys[1], (3,) + grid_shape, jnp.float32), -2.5, 2.5)
    baseline = jax.random.uniform(subkeys[2], grid_shape, jnp.float32, 0.6, 1.8)
    density = 1.0 + envelope * (density - 1.0)
    velocity = envelope[None] * velocity
    baseline = 0.6 + envelope * (baseline - 0.6)
    cell_total = NZ * NY * NX
    segment = cell_total // 8
    offsets = jax.random.randint(subkeys[3], (8,), 0, segment)
    hot_cells = jnp.arange(8, dtype=jnp.int32) * segment + offsets
    ranking = jax.random.permutation(subkeys[4], 8)
    levels = 10.0 * 1.25 ** ranking.astype(jnp.float32)
    hot_extra = jnp.zeros((cell_total,), jnp.float32).at[hot_cells].add(levels).reshape(grid_shape)
    internal = baseline + hot_extra
    momentum = density * velocity
    energy = density * (internal + 0.5 * jnp.sum(velocity * velocity, axis=0))
    return jnp.stack([density, momentum[0], momentum[1], momentum[2], energy])


def draw_advection(key, part):
    return advection_table(key)


def draw_inverse_x(key, part):
    return block_inverse(key, 0, CX)


def draw_inverse_y(key, part):
    return block_inverse(key, 1, CY)


def draw_inverse_z(key, part):
    return block_inverse(key, 2, CZ)


def draw_reduced_x(key, part):
    return reduced_inverse(key, 0, CX, NX // CX)


def draw_reduced_y(key, part):
    return reduced_inverse(key, 1, CY, NY // CY)


def draw_reduced_z(key, part):
    return reduced_inverse(key, 2, CZ, NZ // CZ)


def setup_inputs(seed: int = 0) -> dict:
    arg_keys = jax.random.split(jax.random.key(seed), 9)
    return {
        "flow_state": draw_flow_state(jax.random.fold_in(arg_keys[8], 71), 0),
        "advection": draw_advection(jax.random.fold_in(arg_keys[8], 71), 0),
        "inverse_x": draw_inverse_x(jax.random.fold_in(arg_keys[8], 71), 0),
        "inverse_y": draw_inverse_y(jax.random.fold_in(arg_keys[8], 71), 0),
        "inverse_z": draw_inverse_z(jax.random.fold_in(arg_keys[8], 71), 0),
        "reduced_x": draw_reduced_x(jax.random.fold_in(arg_keys[8], 71), 0),
        "reduced_y": draw_reduced_y(jax.random.fold_in(arg_keys[8], 71), 0),
        "reduced_z": draw_reduced_z(jax.random.fold_in(arg_keys[8], 71), 0),
    }


exact_mode = lax.Precision.HIGHEST
gas_ratio = 0.4
courant = 8000.0
damping = 0.0625
fourth_coef = 0.5

def primitives(flow_state):
    density = flow_state[0]
    velocity = flow_state[1:4] / density
    kinetic = 0.5 * lax.optimization_barrier(jnp.sum(velocity * velocity, axis=0))
    internal = jnp.maximum(flow_state[4] / density - kinetic, 0.25)
    pressure = gas_ratio * density * internal
    return (velocity, internal, pressure)

def flux_component(flow_state, velocity, pressure, variable, direction):
    carried = velocity[direction]
    if variable == 0:
        return flow_state[1 + direction]
    if variable < 4:
        moment = flow_state[variable] * carried
        if variable - 1 == direction:
            moment = moment + pressure
        return moment
    return (flow_state[4] + pressure) * carried

def residual_field(flow_state, velocity, pressure):
    collected = []
    for variable in range(VARS):
        field = flow_state[variable]
        running = jnp.zeros_like(field)
        for direction in range(3):
            line_axis = 2 - direction
            flux = flux_component(flow_state, velocity, pressure, variable, direction)
            running = running - 0.5 * (jnp.roll(flux, -1, line_axis) - jnp.roll(flux, 1, line_axis))
            fourth = jnp.roll(field, 2, line_axis) - 4.0 * jnp.roll(field, 1, line_axis) + 6.0 * field - 4.0 * jnp.roll(field, -1, line_axis) + jnp.roll(field, -2, line_axis)
            running = running - damping * fourth
        collected.append(running)
    return jnp.stack(collected)

def neighbour_table(reduced):
    blocks = reduced.shape[0] // 4
    padded = jnp.pad(reduced, ((2, 2), (0, 0)))
    picked = (4 * np.arange(blocks)[:, None] + np.array([0, 1, 6, 7])[None, :]).reshape(-1)
    return padded[picked]

def line_solve(line_field, line_axis, inverse, reduced, speed):
    moved = jnp.moveaxis(line_field, line_axis, -1)
    block_len = inverse.shape[0]
    blocks = reduced.shape[0] // 4
    leading = moved.shape[:-1]
    split = moved.reshape(leading + (blocks, block_len))
    local_part = jnp.einsum('ij,abpj->abpi', inverse, split, precision=exact_mode)
    boundary = jnp.stack([local_part[..., 0], local_part[..., 1], local_part[..., block_len - 2], local_part[..., block_len - 1]], axis=-1).reshape(leading + (4 * blocks,))
    nearby = jnp.einsum('rq,abq->abr', neighbour_table(reduced), boundary, precision=exact_mode).reshape(leading + (blocks, 4))
    lower_one = -0.5 * speed - 4.0 * fourth_coef
    upper_one = 0.5 * speed - 4.0 * fourth_coef
    left_first = fourth_coef * nearby[..., 0] + lower_one * nearby[..., 1]
    left_second = fourth_coef * nearby[..., 1]
    right_first = fourth_coef * nearby[..., 2]
    right_second = upper_one * nearby[..., 2] + fourth_coef * nearby[..., 3]
    correction = inverse[:, 0] * left_first[..., None] + inverse[:, 1] * left_second[..., None] + inverse[:, block_len - 2] * right_first[..., None] + inverse[:, block_len - 1] * right_second[..., None]
    solved = (local_part - correction).reshape(moved.shape)
    return jnp.moveaxis(solved, -1, line_axis)

def reference(flow_state, advection, inverse_x, inverse_y, inverse_z, reduced_x, reduced_y, reduced_z):
    velocity, internal, pressure = primitives(flow_state)
    wave_speed = lax.optimization_barrier(jnp.sum(jnp.abs(velocity), axis=0)) + jnp.sqrt(3.0 * 1.4 * gas_ratio * internal)
    top_speed = jnp.max(wave_speed)
    time_step = courant / top_speed
    residual = residual_field(flow_state, velocity, pressure)
    rms_norm = jnp.sqrt(lax.optimization_barrier(jnp.sum(residual * residual, axis=(1, 2, 3))) / (NX * NY * NZ))
    inverses = (inverse_x, inverse_y, inverse_z)
    reduceds = (reduced_x, reduced_y, reduced_z)
    collected = []
    for variable in range(VARS):
        line_field = time_step * residual[variable]
        for direction in range(3):
            line_field = line_solve(line_field, 2 - direction, inverses[direction][variable], reduceds[direction][variable], advection[direction, variable])
        collected.append(line_field)
    return (jnp.stack(collected), rms_norm)
```

```python
import functools

import jax
import jax.numpy as jnp
from jax import lax
from jax.experimental import pallas as pl
from jax.experimental.pallas import tpu as pltpu
from jax.sharding import PartitionSpec as P

VARS, CX, CY, CZ = 5, 128, 16, 32
PLANE = CY
ROWS = CZ * CY
F32, BF16 = jnp.float32, jnp.bfloat16
MESH = pl.DeviceIdType.MESH
NT = (((1,), (1,)), ((), ()))


def iota(shape, dim):
    return lax.broadcasted_iota(jnp.int32, shape, dim)


def log2(n):
    return n.bit_length() - 1


def split(x):
    hi = x.astype(BF16)
    return hi, (x - hi.astype(F32)).astype(BF16)


def dot(a, b):
    return jnp.dot(a, b, preferred_element_type=F32)


def dot_nt(a, b):
    return lax.dot_general(a, b, NT, preferred_element_type=F32)


def mm3(left_hi, left_lo, right):
    hi, lo = split(right)
    return dot(left_hi, hi) + (dot(left_hi, lo) + dot(left_lo, hi))


def nt3(a_hi, a_lo, b_hi, b_lo):
    return dot_nt(a_hi, b_hi) + (dot_nt(a_lo, b_hi) + dot_nt(a_hi, b_lo))


def one_hot(cond):
    return jnp.where(cond, 1.0, 0.0).astype(BF16)


def edge(k, length):
    return jnp.where(k < 2, k, k + (length - 4))


def expand(parts, rows, row_map, cols, col_map):
    n, m = parts[0].shape
    row_i, _ = row_map(iota((rows, n), 0))
    pick_rows = one_hot(row_i == iota((rows, n), 1))
    col_j, _ = col_map(iota((m, cols), 1))
    pick_cols = one_hot(col_j == iota((m, cols), 0))
    _, row_r = row_map(iota((rows, cols), 0))
    _, col_c = col_map(iota((rows, cols), 1))
    keep = row_r == col_c
    return [
        jnp.where(keep, dot(pick_rows, dot(part, pick_cols).astype(BF16)), 0.0).astype(BF16)
        for part in parts
    ]


def coupling(shape, blocks_row, speed, row_of):
    row, col = iota(shape, 0), iota(shape, 1)
    base, k = row_of(row)
    lower, upper = -0.5 * speed - 2.0, 0.5 * speed - 2.0
    out = jnp.where((k == 0) & (col == base - 2), 0.5, 0.0)
    out = out + jnp.where((k == 0) & (col == base - 1), lower, 0.0)
    out = out + jnp.where((k == 1) & (col == base - 1), 0.5, 0.0)
    out = out + jnp.where((k == 2) & (col == base + 4), 0.5, 0.0)
    out = out + jnp.where((k == 3) & (col == base + 4), upper, 0.0)
    return out + jnp.where((k == 3) & (col == base + 5), 0.5, 0.0)


def primitives(u):
    scale = 1.0 / u[0]
    vel = [u[1] * scale, u[2] * scale, u[3] * scale]
    kinetic = 0.5 * (vel[0] * vel[0] + vel[1] * vel[1] + vel[2] * vel[2])
    internal = jnp.maximum(u[4] * scale - kinetic, 0.25)
    return vel, internal, 0.4 * u[0] * internal


def fluxes(u, w, pressure, direction):
    out = [u[1 + direction]]
    for c in range(3):
        moment = u[1 + c] * w
        out.append(moment + pressure if c == direction else moment)
    return out + [(u[4] + pressure) * w]


def kernel(
    px, py, pz,
    adv, flow, inv_x, inv_y, inv_z, red_x, red_y, red_z,
    out, rms,
    U, PR, YS, YH, FYH, PK, XH, XC, F, XL, YL, ZL, XR, CT,
    YF, YR1, Y2, YR2, ZF, ZR1, Z2, ZR2, STX, STY, STZ,
    AX, WX, LX, PY, PZ, KY, KZ, WY, WZ,
    in_sem, out_sem, hs, hr, xs, xrv, ysem, yr1s, y2sem, yr2s, zsem, zr1s, z2sem, zr2s, ss, sr,
):
    ix, iy, iz = lax.axis_index("gx"), lax.axis_index("gy"), lax.axis_index("gz")
    zc, yc = CZ // py, CY // pz
    yr, zr = 4 * zc, 4 * yc
    lzc, lyc, lyr, lzr = log2(zc), log2(yc), log2(4 * zc), log2(4 * yc)

    def peer(axis, d):
        me, n = {"gx": (ix, px), "gy": (iy, py), "gz": (iz, pz)}[axis]
        return {axis: (me + d + n) & (n - 1)}

    def remote(src, dst, send, recv, device):
        return pltpu.make_async_remote_copy(
            src_ref=src, dst_ref=dst, send_sem=send, recv_sem=recv,
            device_id=device, device_id_type=MESH,
        )

    def drain(ref, sem):
        pltpu.make_async_copy(ref, ref, sem).wait()

    load = pltpu.make_async_copy(flow, U.at[:, pl.ds(2 * PLANE, ROWS)], in_sem)
    load.start()
    barrier = pltpu.get_barrier_semaphore()
    for axis, n in (("gz", pz), ("gy", py), ("gx", px)):
        for d in range(1, n):
            pl.semaphore_signal(barrier, inc=1, device_id=peer(axis, d), device_id_type=MESH)
    load.wait()

    def pack_rows(v, carry):
        for r in range(2):
            for t in range(CZ // 8):
                for side, first in ((0, CY - 2), (1, 0)):
                    start = 2 * PLANE + 8 * t * PLANE + first + r
                    YS[side, v, pl.ds(r * CZ + 8 * t, 8), :] = U[v, pl.ds(start, 8, stride=PLANE), :]
        return carry

    lax.fori_loop(0, VARS, pack_rows, 0)
    lane = iota((CY, CX), 1)
    row = iota((CY, CX), 0)

    def pack_lanes(z, acc):
        base = pl.multiple_of(2 * PLANE + z * PLANE, PLANE)
        here = (lane >> 2) == z
        return [
            jnp.where(here, pltpu.roll(U[v, pl.ds(base, PLANE), :], 4 * z + 2, 1), acc[v])
            for v in range(VARS)
        ]

    packed = lax.fori_loop(0, CZ, pack_lanes, [jnp.zeros((CY, CX), F32)] * VARS)
    for v in range(VARS):
        PK[v] = packed[v]

    pl.semaphore_wait(barrier, px + py + pz - 3)
    last = 2 * PLANE + ROWS
    halos = [
        remote(flow.at[:, pl.ds(ROWS - 2 * PLANE, 2 * PLANE)], U.at[:, pl.ds(0, 2 * PLANE)],
               hs.at[0], hr.at[0], peer("gz", 1)),
        remote(flow.at[:, pl.ds(0, 2 * PLANE)], U.at[:, pl.ds(last, 2 * PLANE)],
               hs.at[1], hr.at[1], peer("gz", -1)),
        remote(YS.at[0], YH.at[0], hs.at[2], hr.at[2], peer("gy", 1)),
        remote(YS.at[1], YH.at[1], hs.at[3], hr.at[3], peer("gy", -1)),
        remote(PK, XH.at[0], hs.at[4], hr.at[4], peer("gx", 1)),
        remote(PK, XH.at[1], hs.at[5], hr.at[5], peer("gx", -1)),
    ]
    for copy in halos:
        copy.start()

    def plane_primitives(base):
        u = [U[v, pl.ds(base, PLANE), :] for v in range(VARS)]
        vel, internal, pressure = primitives(u)
        for c in range(3):
            PR[c, pl.ds(base, PLANE), :] = vel[c]
        PR[3, pl.ds(base, PLANE), :] = pressure
        return vel, internal

    def first_pass(z, top):
        base = pl.multiple_of(2 * PLANE + z * PLANE, PLANE)
        vel, internal = plane_primitives(base)
        speed = jnp.abs(vel[0]) + jnp.abs(vel[1]) + jnp.abs(vel[2]) + jnp.sqrt(3.0 * 1.4 * 0.4 * internal)
        return jnp.maximum(top, speed)

    top = lax.fori_loop(0, CZ, first_pass, jnp.zeros((CY, CX), F32))

    def build_first(v, carry):
        x_hi, x_lo = split(inv_x[v])
        AX[0, v], AX[1, v] = x_hi, x_lo
        col = iota((CX, CX), 1)
        pick = one_hot(((col >> 2) == v) & (iota((CX, CX), 0) == edge(col & 3, CX)))
        WX[0, v], WX[1, v] = dot(x_hi, pick).astype(BF16), dot(x_lo, pick).astype(BF16)

        def y_row(r):
            s = r - 256
            face = (edge((s >> lzc) & 3, CY), ((s >> lyr) << lzc) + (s & (zc - 1)))
            return jnp.where(s < 0, r >> 4, face[0]), jnp.where(s < 0, r & 15, face[1])

        PY[0, v], PY[1, v] = expand(split(inv_y[v]), 320, y_row, 256, lambda c: (c & 15, c >> 4))
        return carry

    lax.fori_loop(0, VARS, build_first, 0)
    for t in range(3):
        acc = jnp.zeros((8, 8 * px), F32)
        for v in (2 * t, 2 * t + 1):
            if v == VARS:
                continue
            shape = (8, 4 * px)
            own = coupling(shape, 8, adv[0, v], lambda r: (4 * ix, r & 3))
            rows = jnp.dot(own, red_x[v], precision=lax.Precision.HIGHEST, preferred_element_type=F32)
            r, c = iota((4 * px, 8 * px), 0), iota((4 * px, 8 * px), 1)
            spread = jnp.where(r == ((c >> 3) << 2) + (c & 3), 1.0, 0.0)
            wide = jnp.dot(rows, spread, precision=lax.Precision.HIGHEST, preferred_element_type=F32)
            r, c = iota((8, 8 * px), 0), iota((8, 8 * px), 1)
            acc = acc + jnp.where(((r >> 2) == v - 2 * t) & (((c >> 2) & 1) == v - 2 * t), wide, 0.0)
        LX[t] = acc

    for copy in halos:
        copy.wait_recv()
    plane_primitives(PLANE)
    plane_primitives(last)
    for side in range(2):
        mine = pl.ds((1 - side) * CZ, CZ)
        u = [YH[side, v, mine, :] for v in range(VARS)]
        vel, _, pressure = primitives(u)
        for v, f in enumerate(fluxes(u, vel[1], pressure, 1)):
            FYH[side, v] = f
    j = lane & 3
    near = [jnp.where(j < 2, XH[0, v], XH[1, v]) for v in range(VARS)]
    mine = [PK[v] for v in range(VARS)]
    vel, _, pressure = primitives(near)
    near_flux = fluxes(near, vel[0], pressure, 0)
    vel, _, pressure = primitives(mine)
    mine_flux = fluxes(mine, vel[0], pressure, 0)
    for v in range(VARS):
        du, df = near[v] - mine[v], near_flux[v] - mine_flux[v]
        far = -0.0625 * jnp.where(j < 2, pltpu.roll(du, CX - 2, 1), pltpu.roll(du, 2, 1))
        right = pltpu.roll(-0.5 * df + 0.25 * du, CX - 1, 1)
        left = pltpu.roll(0.5 * df + 0.25 * du, 1, 1)
        XC[v] = far + jnp.where(j == 1, right, 0.0) + jnp.where(j == 2, left, 0.0)

    ends = ((lane + 2) & (CX - 1)) < 4

    def second_pass(z, sums):
        base = pl.multiple_of(2 * PLANE + z * PLANE, PLANE)

        def at(ref, k, step):
            return ref[k, pl.ds(base + step * PLANE, PLANE), :]

        u = [at(U, v, 0) for v in range(VARS)]
        ahead = [at(U, v, 1) for v in range(VARS)]
        behind = [at(U, v, -1) for v in range(VARS)]
        pressure = at(PR, 3, 0)
        x_flux = fluxes(u, at(PR, 0, 0), pressure, 0)
        y_flux = fluxes(u, at(PR, 1, 0), pressure, 1)
        z_ahead = fluxes(ahead, at(PR, 2, 1), at(PR, 3, 1), 2)
        z_behind = fluxes(behind, at(PR, 2, -1), at(PR, 3, -1), 2)
        done = []
        for v in range(VARS):
            f = u[v]

            def halo(ref, side, line):
                return jnp.broadcast_to(ref[side, v, pl.ds(line + z, 1), :], (CY, CX))

            low2, low1 = halo(YH, 0, 0), halo(YH, 0, CZ)
            high1, high2 = halo(YH, 1, 0), halo(YH, 1, CZ)
            y_m1 = jnp.where(row == 0, low1, pltpu.roll(f, 1, 0))
            y_m2 = jnp.where(row == 0, low2, jnp.where(row == 1, low1, pltpu.roll(f, 2, 0)))
            y_p1 = jnp.where(row == CY - 1, high1, pltpu.roll(f, CY - 1, 0))
            y_p2 = jnp.where(row == CY - 1, high2, jnp.where(row == CY - 2, high1, pltpu.roll(f, CY - 2, 0)))
            y_fwd = jnp.where(row == CY - 1, halo(FYH, 1, 0), pltpu.roll(y_flux[v], CY - 1, 0))
            y_back = jnp.where(row == 0, halo(FYH, 0, 0), pltpu.roll(y_flux[v], 1, 0))
            near1 = (ahead[v] + behind[v]) + (y_m1 + y_p1) + (pltpu.roll(f, 1, 1) + pltpu.roll(f, CX - 1, 1))
            near2 = (at(U, v, 2) + at(U, v, -2)) + (y_m2 + y_p2) + (pltpu.roll(f, 2, 1) + pltpu.roll(f, CX - 2, 1))
            slope = (z_ahead[v] - z_behind[v]) + (y_fwd - y_back)
            slope = slope + (pltpu.roll(x_flux[v], CX - 1, 1) - pltpu.roll(x_flux[v], 1, 1))
            fix = jnp.where(ends, pltpu.roll(XC[v], (2 * CX - 2 - 4 * z) & (CX - 1), 1), 0.0)
            r = fix - 0.5 * slope - 0.0625 * near2 + 0.25 * near1 - 1.125 * f
            F[v, pl.ds(pl.multiple_of(z * PLANE, PLANE), PLANE), :] = r
            done.append(sums[v] + r * r)
        return done

    sums = lax.fori_loop(0, CZ, second_pass, [jnp.zeros((CY, CX), F32)] * VARS)

    row8 = iota((8, 4 * CX), 0)
    for t in range(3):
        pair = []
        for v in (2 * t, 2 * t + 1):
            if v == VARS:
                pair.append(jnp.zeros((8, ROWS), F32))
                continue
            tile = jnp.where(iota((8, CX), 0) < 2, inv_x[v, 0:8, :], pltpu.roll(inv_x[v, CX - 8 : CX, :], 4, 0))
            if v & 1:
                tile = pltpu.roll(tile, 4, 0)
            pair.append(nt3(*split(tile), *split(F[v])))
        XR[t, ix] = jnp.where(row8 < 4, pair[0], pair[1])
    for d in range(1, px):
        remote(XR.at[:, ix], XR.at[:, ix], xs, xrv, peer("gx", d)).start()

    stat_row = iota((8, CX), 0)
    tile = jnp.where(stat_row == VARS, jnp.max(top), 0.0)
    for v in range(VARS):
        tile = jnp.where(stat_row == v, jnp.sum(sums[v]), tile)
    STX[ix] = tile
    for d in range(1, px):
        remote(STX.at[ix], STX.at[ix], ss.at[0], sr.at[0], peer("gx", d)).start()

    def combine(ref, n):
        total = ref[0]
        for k in range(1, n):
            total = jnp.where(stat_row == VARS, jnp.maximum(total, ref[k]), total + ref[k])
        return total

    def local_x(v, carry):
        XL[v] = nt3(*split(F[v]), AX[0, v], AX[1, v])

        def z_row(r):
            s = r - 256
            face = (edge((s >> lyc) & 3, CZ), ((s >> lzr) << lyc) + (s & (yc - 1)))
            return jnp.where(s < 0, r >> 3, face[0]), jnp.where(s < 0, r & 7, face[1])

        PZ[0, v], PZ[1, v] = expand(split(inv_z[v]), 288, z_row, 256, lambda c: (c & 31, c >> 5))

        def reduced(red, n, speed):
            g = coupling((4 * n, 4 * n), n, speed, lambda r: ((r >> 2) << 2, r & 3))
            return split(jnp.dot(g, red, precision=lax.Precision.HIGHEST, preferred_element_type=F32))

        y_side = lambda r: (r >> lzc, r & (zc - 1))
        KY[0, v], KY[1, v] = expand(reduced(red_y[v], py, adv[1, v]), 4 * CZ, y_side, 4 * CZ, y_side)
        z_side = lambda r: (r >> lyc, r & (yc - 1))
        KZ[0, v], KZ[1, v] = expand(reduced(red_z[v], pz, adv[2, v]), 4 * CY, z_side, 4 * CY, z_side)
        return carry

    lax.fori_loop(0, VARS, local_x, 0)

    drain(XR.at[:, pl.ds(0, px - 1)], xrv)
    factors = [mm3(*split(LX[t]), XR[t].reshape(8 * px, ROWS)) for t in range(3)]
    factors = jnp.concatenate(factors + [jnp.zeros((CX - 24, ROWS), F32)], axis=0).T
    CT[0], CT[1] = split(factors)

    def send_y(src, dst, v, send, recv):
        for d in range(1, py):
            to = peer("gy", d)
            remote(src.at[v, pl.ds(pl.multiple_of(to["gy"] * yr, yr), yr)],
                   dst.at[v, pl.ds(pl.multiple_of(iy * yr, yr), yr)], send, recv, to).start()
        mine = pl.ds(pl.multiple_of(iy * yr, yr), yr)
        dst[v, mine, :] = src[v, mine, :]

    def send_z(src, dst, v, send, recv):
        for d in range(1, pz):
            to = peer("gz", d)
            remote(src.at[v, pl.ds(pl.multiple_of(to["gz"] * zr, zr), zr)],
                   dst.at[v, pl.ds(pl.multiple_of(iz * zr, zr), zr)], send, recv, to).start()
        mine = pl.ds(pl.multiple_of(iz * zr, zr), zr)
        dst[v, mine, :] = src[v, mine, :]

    def local_y(v, carry):
        field = XL[v] - nt3(CT[0], CT[1], WX[0, v], WX[1, v])
        for g in range(2):
            solved = mm3(PY[0, v], PY[1, v], field[256 * g : 256 * g + 256])
            for y in range(CY):
                YL[v, pl.ds(y * CZ + 16 * g, 16), :] = solved[16 * y : 16 * y + 16]
            YF[v, pl.ds(64 * g, 64), :] = solved[256:320]
        send_y(YF, YR1, v, ysem, yr1s.at[v])
        return carry

    lax.fori_loop(0, VARS, local_y, 0)
    drain(STX.at[pl.ds(0, px - 1)], sr.at[0])
    STY[iy] = combine(STX, px)
    for d in range(1, py):
        remote(STY.at[iy], STY.at[iy], ss.at[1], sr.at[1], peer("gy", d)).start()

    def build_last(v, carry):
        WY[0, v], WY[1, v] = expand(
            split(inv_y[v]), ROWS, lambda r: (r >> 5, r & 31),
            4 * CZ, lambda c: (edge((c >> lzc) & 3, CY), ((c >> lyr) << lzc) + (c & (zc - 1))),
        )
        WZ[0, v], WZ[1, v] = expand(
            split(inv_z[v]), ROWS, lambda r: (r >> 4, r & 15),
            4 * CY, lambda c: (edge((c >> lyc) & 3, CZ), ((c >> lzr) << lyc) + (c & (yc - 1))),
        )
        return carry

    lax.fori_loop(0, VARS, build_last, 0)

    def reduced_y(v, carry):
        drain(YR1.at[v, pl.ds(0, (py - 1) * yr)], yr1s.at[v])
        Y2[v] = mm3(KY[0, v], KY[1, v], YR1[v])
        send_y(Y2, YR2, v, y2sem, yr2s.at[v])
        return carry

    lax.fori_loop(0, VARS, reduced_y, 0)
    drain(STY.at[pl.ds(0, py - 1)], sr.at[1])
    STZ[iz] = combine(STY, py)
    for d in range(1, pz):
        remote(STZ.at[iz], STZ.at[iz], ss.at[2], sr.at[2], peer("gz", d)).start()

    def local_z(v, carry):
        drain(YR2.at[v, pl.ds(0, (py - 1) * yr)], yr2s.at[v])
        field = YL[v] - mm3(WY[0, v], WY[1, v], YR2[v])
        for g in range(2):
            solved = mm3(PZ[0, v], PZ[1, v], field[256 * g : 256 * g + 256])
            for z in range(CZ):
                ZL[v, pl.ds(z * CY + 8 * g, 8), :] = solved[8 * z : 8 * z + 8]
            ZF[v, pl.ds(32 * g, 32), :] = solved[256:288]
        send_z(ZF, ZR1, v, zsem, zr1s.at[v])
        return carry

    lax.fori_loop(0, VARS, local_z, 0)

    def reduced_z(v, carry):
        drain(ZR1.at[v, pl.ds(0, (pz - 1) * zr)], zr1s.at[v])
        Z2[v] = mm3(KZ[0, v], KZ[1, v], ZR1[v])
        send_z(Z2, ZR2, v, z2sem, zr2s.at[v])
        return carry

    lax.fori_loop(0, VARS, reduced_z, 0)
    drain(STZ.at[pl.ds(0, pz - 1)], sr.at[2])
    stats = combine(STZ, pz)
    step = 8000.0 / stats[VARS : VARS + 1]
    norms = jnp.sqrt(stats / float(px * py * pz * ROWS * CX))
    for v in range(VARS):
        rms[v] = jnp.max(norms[v : v + 1])

    def finish(v, carry):
        drain(ZR2.at[v, pl.ds(0, (pz - 1) * zr)], zr2s.at[v])
        F[v] = step * (ZL[v] - mm3(WZ[0, v], WZ[1, v], ZR2[v]))
        pltpu.make_async_copy(F.at[v], out.at[v], out_sem).start()
        return carry

    lax.fori_loop(0, VARS, finish, 0)
    for copy in halos:
        copy.wait_send()
    drain(XR.at[:, pl.ds(0, px - 1)], xs)
    drain(STX.at[pl.ds(0, px - 1)], ss.at[0])
    drain(STY.at[pl.ds(0, py - 1)], ss.at[1])
    drain(STZ.at[pl.ds(0, pz - 1)], ss.at[2])
    drain(YF.at[:, pl.ds(0, (py - 1) * yr)], ysem)
    drain(Y2.at[:, pl.ds(0, (py - 1) * yr)], y2sem)
    drain(ZF.at[:, pl.ds(0, (pz - 1) * zr)], zsem)
    drain(Z2.at[:, pl.ds(0, (pz - 1) * zr)], z2sem)
    drain(F, out_sem)


def shards(px, py, pz, flow_state, advection, *tables):
    vmem = pl.BlockSpec(memory_space=pltpu.VMEM)
    smem = pl.BlockSpec(memory_space=pltpu.SMEM)
    hbm = pl.BlockSpec(memory_space=pl.ANY)
    f32 = lambda *shape: pltpu.VMEM(shape, F32)
    b16 = lambda *shape: pltpu.VMEM(shape, BF16)
    dma = pltpu.SemaphoreType.DMA
    field = (VARS, ROWS, CX)
    padded_rows = ROWS + 4 * PLANE
    update, rms = pl.pallas_call(
        functools.partial(kernel, px, py, pz),
        out_shape=(jax.ShapeDtypeStruct(field, F32), jax.ShapeDtypeStruct((VARS,), F32)),
        in_specs=[smem, hbm] + [vmem] * 6,
        out_specs=(hbm, smem),
        scratch_shapes=[
            f32(VARS, padded_rows, CX), f32(4, padded_rows, CX),
            f32(2, VARS, 2 * CZ, CX), f32(2, VARS, 2 * CZ, CX), f32(2, VARS, CZ, CX),
            f32(VARS, CY, CX), f32(2, VARS, CY, CX), f32(VARS, CY, CX),
            f32(*field), f32(*field), f32(*field), f32(*field),
            f32(3, px, 8, ROWS), b16(2, ROWS, CX),
            f32(VARS, 4 * CZ, CX), f32(VARS, 4 * CZ, CX), f32(VARS, 4 * CZ, CX), f32(VARS, 4 * CZ, CX),
            f32(VARS, 4 * CY, CX), f32(VARS, 4 * CY, CX), f32(VARS, 4 * CY, CX), f32(VARS, 4 * CY, CX),
            f32(px, 8, CX), f32(py, 8, CX), f32(pz, 8, CX),
            b16(2, VARS, CX, CX), b16(2, VARS, CX, CX), f32(3, 8, 8 * px),
            b16(2, VARS, 320, 256), b16(2, VARS, 288, 256),
            b16(2, VARS, 4 * CZ, 4 * CZ), b16(2, VARS, 4 * CY, 4 * CY),
            b16(2, VARS, ROWS, 4 * CZ), b16(2, VARS, ROWS, 4 * CY),
            dma, dma, dma((6,)), dma((6,)), dma, dma,
            dma, dma((VARS,)), dma, dma((VARS,)), dma, dma((VARS,)), dma, dma((VARS,)),
            dma((3,)), dma((3,)),
        ],
        compiler_params=pltpu.CompilerParams(
            collective_id=0, has_side_effects=True, vmem_limit_bytes=60 * 1024 * 1024
        ),
        name="adi_step",
    )(advection, flow_state.reshape(field), *tables)
    return update.reshape(flow_state.shape), rms


def solution(mesh):
    sizes = [mesh.shape[axis] for axis in ("gx", "gy", "gz")]
    return jax.shard_map(
        functools.partial(shards, *sizes),
        mesh=mesh,
        in_specs=(P(None, "gz", "gy", "gx"), P(), P(), P(), P(), P(), P(), P()),
        out_specs=(P(None, "gz", "gy", "gx"), P()),
        check_vma=False,
    )
```

```python
import functools

import jax
import jax.numpy as jnp
from jax import lax
from jax.experimental import pallas as pl
from jax.experimental.pallas import tpu as pltpu
from jax.sharding import PartitionSpec as P

VARS, CX, CY, CZ = 5, 128, 16, 32
PLANE = CY
ROWS = CZ * CY
F32, BF16 = jnp.float32, jnp.bfloat16
MESH = pl.DeviceIdType.MESH
NT = (((1,), (1,)), ((), ()))


def iota(shape, dim):
    return lax.broadcasted_iota(jnp.int32, shape, dim)


def log2(n):
    return n.bit_length() - 1


def split(x):
    hi = x.astype(BF16)
    return hi, (x - hi.astype(F32)).astype(BF16)


def dot(a, b):
    return jnp.dot(a, b, preferred_element_type=F32)


def dot_nt(a, b):
    return lax.dot_general(a, b, NT, preferred_element_type=F32)


def mm2(left, right):
    wide = dot(left, jnp.concatenate(split(right), axis=1))
    m, n = left.shape[0] // 2, right.shape[1]
    return (wide[:m, :n] + wide[:m, n:]) + wide[m:, :n]


def nt2(left, right):
    wide = dot_nt(left, right)
    n = right.shape[0] // 2
    return wide[:, :n] + wide[:, n:]


def mm3(left_hi, left_lo, right):
    hi, lo = split(right)
    return dot(left_hi, hi) + (dot(left_hi, lo) + dot(left_lo, hi))


def one_hot(cond):
    return jnp.where(cond, 1.0, 0.0).astype(BF16)


def edge(k, length):
    return jnp.where(k < 2, k, k + (length - 4))


def expand(parts, rows, row_map, cols, col_map):
    n, m = parts[0].shape
    row_i, _ = row_map(iota((rows, n), 0))
    pick_rows = one_hot(row_i == iota((rows, n), 1))
    col_j, _ = col_map(iota((m, cols), 1))
    pick_cols = one_hot(col_j == iota((m, cols), 0))
    _, row_r = row_map(iota((rows, cols), 0))
    _, col_c = col_map(iota((rows, cols), 1))
    keep = row_r == col_c
    return [
        jnp.where(keep, dot(pick_rows, dot(part, pick_cols).astype(BF16)), 0.0).astype(BF16)
        for part in parts
    ]


def coupling(shape, speed, row_of):
    row, col = iota(shape, 0), iota(shape, 1)
    base, k = row_of(row)
    lower, upper = -0.5 * speed - 2.0, 0.5 * speed - 2.0
    out = jnp.where((k == 0) & (col == base - 2), 0.5, 0.0)
    out = out + jnp.where((k == 0) & (col == base - 1), lower, 0.0)
    out = out + jnp.where((k == 1) & (col == base - 1), 0.5, 0.0)
    out = out + jnp.where((k == 2) & (col == base + 4), 0.5, 0.0)
    out = out + jnp.where((k == 3) & (col == base + 4), upper, 0.0)
    return out + jnp.where((k == 3) & (col == base + 5), 0.5, 0.0)


def primitives(u):
    scale = 1.0 / u[0]
    vel = [u[1] * scale, u[2] * scale, u[3] * scale]
    kinetic = 0.5 * (vel[0] * vel[0] + vel[1] * vel[1] + vel[2] * vel[2])
    internal = jnp.maximum(u[4] * scale - kinetic, 0.25)
    return vel, internal, 0.4 * u[0] * internal


def fluxes(u, w, pressure, direction):
    out = [u[1 + direction]]
    for c in range(3):
        moment = u[1 + c] * w
        out.append(moment + pressure if c == direction else moment)
    return out + [(u[4] + pressure) * w]


def kernel(
    px, py, pz,
    tab_adv, flow, *refs,
):
    (
        tab_x, tab_y, tab_z, tab_rx, tab_ry, tab_rz,
        F, rms,
        adv, inv_x, inv_y, inv_z, red_x, red_y, red_z,
        U, PR, FZ, YS, YH, HY, PK, XH, XC, FS, XL, YL, ZL, FG, XR, CT,
        YF, YR1, Y2, YR2, ZF, ZR1, Z2, ZR2, STX, STY, STZ,
        AX, WX, LX, MY, MZ, KY, KZ, SY, SZ,
        in_sem, hs, hr, xs, xrv, ysem, yr1s, y2sem, yr2s, zsem, zr1s, z2sem, zr2s, ss, sr,
    ) = refs
    ix, iy, iz = lax.axis_index("gx"), lax.axis_index("gy"), lax.axis_index("gz")
    zc, yc = CZ // py, CY // pz
    yr, zr = 4 * zc, 4 * yc

    def peer(axis, d):
        me, n = {"gx": (ix, px), "gy": (iy, py), "gz": (iz, pz)}[axis]
        return {axis: (me + d + n) & (n - 1)}

    def remote(src, dst, send, recv, device):
        return pltpu.make_async_remote_copy(
            src_ref=src, dst_ref=dst, send_sem=send, recv_sem=recv,
            device_id=device, device_id_type=MESH,
        )

    def drain(ref, sem):
        pltpu.make_async_copy(ref, ref, sem).wait()

    load = pltpu.make_async_copy(flow, U.at[:, pl.ds(2 * PLANE, ROWS)], in_sem.at[0])
    load.start()
    tables = [
        pltpu.make_async_copy(src, dst, in_sem.at[1 + k])
        for k, (src, dst) in enumerate(zip(
            (tab_adv, tab_x, tab_y, tab_z, tab_rx, tab_ry, tab_rz),
            (adv, inv_x, inv_y, inv_z, red_x, red_y, red_z),
        ))
    ]
    for copy in tables:
        copy.start()
    barrier = pltpu.get_barrier_semaphore()
    for axis, n in (("gz", pz), ("gy", py), ("gx", px)):
        for d in range(1, n):
            pl.semaphore_signal(barrier, inc=1, device_id=peer(axis, d), device_id_type=MESH)
    load.wait()

    def pack_rows(v, carry):
        for r in range(2):
            for t in range(CZ // 8):
                for side, first in ((0, CY - 2), (1, 0)):
                    start = 2 * PLANE + 8 * t * PLANE + first + r
                    YS[side, v, pl.ds(r * CZ + 8 * t, 8), :] = U[v, pl.ds(start, 8, stride=PLANE), :]
        return carry

    lax.fori_loop(0, VARS, pack_rows, 0)
    lane = iota((CY, CX), 1)
    row = iota((CY, CX), 0)

    def pack_lanes(v, carry):
        acc = jnp.zeros((CY, CX), F32)
        for z in range(CZ):
            plane = U[v, pl.ds((2 + z) * PLANE, PLANE), :]
            acc = jnp.where((lane >> 2) == z, pltpu.roll(plane, (4 * z + 2) % CX, 1), acc)
        PK[v] = acc
        return carry

    lax.fori_loop(0, VARS, pack_lanes, 0)

    def plane_primitives(base):
        here = pl.ds(base, PLANE)
        u = [U[v, here, :] for v in range(VARS)]
        vel, internal, pressure = primitives(u)
        PR[0, here, :], PR[1, here, :], PR[2, here, :] = vel[0], vel[1], pressure
        for k, f in enumerate(fluxes(u, vel[2], pressure, 2)[1:]):
            FZ[k, here, :] = f
        return vel, internal

    def first_pass(step, top):
        for k in range(2):
            base = pl.multiple_of(2 * PLANE + (2 * step + k) * PLANE, PLANE)
            vel, internal = plane_primitives(base)
            speed = jnp.abs(vel[0]) + jnp.abs(vel[1]) + jnp.abs(vel[2]) + jnp.sqrt(3.0 * 1.4 * 0.4 * internal)
            top = jnp.maximum(top, speed)
        return top

    top = lax.fori_loop(0, CZ // 2, first_pass, jnp.zeros((CY, CX), F32))

    for copy in tables:
        copy.wait()
    high = lax.Precision.HIGHEST

    def exact_dot(a, b):
        return jnp.dot(a, b, precision=high, preferred_element_type=F32)

    def columns(table, length):
        shape = (length, 4 * CX)
        pick = one_hot(iota(shape, 0) == edge(iota(shape, 1) >> 7, length))
        hi, lo = split(table)
        return dot(hi, pick) + dot(lo, pick)

    def build_first(v, carry):
        hi, lo = split(inv_x[v])
        AX[v] = jnp.concatenate([jnp.concatenate([hi, hi], 1), jnp.concatenate([lo, lo], 1)], 0)
        col = iota((CX, CX), 1)
        pick = one_hot(((col >> 2) == v) & (iota((CX, CX), 0) == edge(col & 3, CX)))
        hi, lo = dot(hi, pick).astype(BF16), dot(lo, pick).astype(BF16)
        WX[v] = jnp.concatenate([jnp.concatenate([hi, hi], 1), jnp.concatenate([lo, lo], 1)], 0)

        pick = one_hot(iota((CY, CX), 0) == (iota((CY, CX), 1) & (CY - 1)))
        for part, table in enumerate(split(inv_y[v])):
            spread = dot(table, pick)
            for z in range(8):
                block = jnp.where((lane >> 4) == z, spread, 0.0)
                MY[v, part * CX + 16 * z : part * CX + 16 * z + 16, :] = block.astype(BF16)
        return carry

    lax.fori_loop(0, VARS, build_first, 0)
    for t in range(3):
        acc = jnp.zeros((8, 8 * px), F32)
        for v in (2 * t, 2 * t + 1):
            if v == VARS:
                continue
            own = coupling((8, 4 * px), adv[0, v], lambda r: (4 * ix, r & 3))
            rows = exact_dot(own, red_x[v])
            r, c = iota((4 * px, 8 * px), 0), iota((4 * px, 8 * px), 1)
            wide = exact_dot(rows, jnp.where(r == ((c >> 3) << 2) + (c & 3), 1.0, 0.0))
            r, c = iota((8, 8 * px), 0), iota((8, 8 * px), 1)
            acc = acc + jnp.where(((r >> 2) == v - 2 * t) & (((c >> 2) & 1) == v - 2 * t), wide, 0.0)
        LX[t] = acc

    pl.semaphore_wait(barrier, px + py + pz - 3)
    last = 2 * PLANE + ROWS
    halos = [
        remote(flow.at[:, pl.ds(ROWS - 2 * PLANE, 2 * PLANE)], U.at[:, pl.ds(0, 2 * PLANE)],
               hs.at[0], hr.at[0], peer("gz", 1)),
        remote(flow.at[:, pl.ds(0, 2 * PLANE)], U.at[:, pl.ds(last, 2 * PLANE)],
               hs.at[1], hr.at[1], peer("gz", -1)),
        remote(YS.at[0], YH.at[0], hs.at[2], hr.at[2], peer("gy", 1)),
        remote(YS.at[1], YH.at[1], hs.at[3], hr.at[3], peer("gy", -1)),
        remote(PK, XH.at[0], hs.at[4], hr.at[4], peer("gx", 1)),
        remote(PK, XH.at[1], hs.at[5], hr.at[5], peer("gx", -1)),
    ]
    for copy in halos:
        copy.start()

    def build_second(v, carry):
        SY[v] = columns(inv_y[v], CY)

        wide = iota((CZ, 8 * CZ), 1)
        pick = one_hot(iota((CZ, 8 * CZ), 0) == (wide >> 3))
        r, c = iota((16, 8 * CZ), 0), iota((16, 8 * CZ), 1)
        keep, first = (r & 7) == (c & 7), r < 8
        for part, table in enumerate(split(inv_z[v])):
            spread = dot(table, pick)
            for k in range(CZ // 2):
                pair = [jnp.broadcast_to(spread[z : z + 1], (16, 8 * CZ)) for z in (2 * k, 2 * k + 1)]
                block = jnp.where(keep, jnp.where(first, pair[0], pair[1]), 0.0)
                MZ[v, part * 256 + 16 * k : part * 256 + 16 * k + 16, :] = block.astype(BF16)
        SZ[v] = columns(inv_z[v], CZ)

        def reduced(red, n, speed):
            g = coupling((4 * n, 4 * n), speed, lambda r: ((r >> 2) << 2, r & 3))
            return split(exact_dot(g, red))

        y_side = lambda r: (r >> log2(zc), r & (zc - 1))
        hi, lo = expand(reduced(red_y[v], py, adv[1, v]), 4 * CZ, y_side, 4 * CZ, y_side)
        KY[v, 0:CX, :], KY[v, CX : 2 * CX, :] = hi, lo
        z_side = lambda r: (r >> log2(yc), r & (yc - 1))
        KZ[0, v], KZ[1, v] = expand(reduced(red_z[v], pz, adv[2, v]), 4 * CY, z_side, 4 * CY, z_side)
        return carry

    lax.fori_loop(0, VARS, build_second, 0)
    for copy in halos:
        copy.wait_recv()
    plane_primitives(PLANE)
    plane_primitives(last)
    for side in range(2):
        near1, near2 = pl.ds((1 - side) * CZ, CZ), pl.ds(side * CZ, CZ)
        u = [YH[side, v, near1, :] for v in range(VARS)]
        vel, _, pressure = primitives(u)
        half = 0.5 - side
        for v, f in enumerate(fluxes(u, vel[1], pressure, 1)):
            HY[2 * side, v] = -0.0625 * u[v]
            HY[2 * side + 1, v] = 0.25 * u[v] + half * f - 0.0625 * YH[side, v, near2, :]
    j = lane & 3
    near = [jnp.where(j < 2, XH[0, v], XH[1, v]) for v in range(VARS)]
    mine = [PK[v] for v in range(VARS)]
    vel, _, pressure = primitives(near)
    near_flux = fluxes(near, vel[0], pressure, 0)
    vel, _, pressure = primitives(mine)
    mine_flux = fluxes(mine, vel[0], pressure, 0)
    for v in range(VARS):
        du, df = near[v] - mine[v], near_flux[v] - mine_flux[v]
        far = -0.0625 * jnp.where(j < 2, pltpu.roll(du, CX - 2, 1), pltpu.roll(du, 2, 1))
        right = pltpu.roll(-0.5 * df + 0.25 * du, CX - 1, 1)
        left = pltpu.roll(0.5 * df + 0.25 * du, 1, 1)
        XC[v] = far + jnp.where(j == 1, right, 0.0) + jnp.where(j == 2, left, 0.0)

    ends = ((lane + 2) & (CX - 1)) < 4
    bottom, ceiling = row == 0, row == CY - 1

    def residual_plane(z, sums):
        base = pl.multiple_of(2 * PLANE + z * PLANE, PLANE)

        def at(ref, k, step):
            return ref[k, pl.ds(base + step * PLANE, PLANE), :]

        u = [at(U, v, 0) for v in range(VARS)]
        pressure = at(PR, 2, 0)
        x_flux = fluxes(u, at(PR, 0, 0), pressure, 0)
        y_flux = fluxes(u, at(PR, 1, 0), pressure, 1)
        done = []
        for v in range(VARS):
            f = u[v]
            ahead, behind = at(U, v, 1), at(U, v, -1)
            if v == 0:
                slope = at(U, 3, 1) - at(U, 3, -1)
            else:
                slope = at(FZ, v - 1, 1) - at(FZ, v - 1, -1)

            def halo(k):
                return jnp.broadcast_to(HY[k, v, pl.ds(z, 1), :], (CY, CX))

            far, quarter = -0.0625 * f, 0.25 * f
            half = 0.5 * y_flux[v]
            up = quarter + half + jnp.where(bottom, halo(0), pltpu.roll(far, 1, 0))
            down = quarter - half + jnp.where(ceiling, halo(2), pltpu.roll(far, CY - 1, 0))
            r = jnp.where(bottom, halo(1), pltpu.roll(up, 1, 0))
            r = r + jnp.where(ceiling, halo(3), pltpu.roll(down, CY - 1, 0))
            half = 0.5 * x_flux[v]
            up = quarter + half + pltpu.roll(far, 1, 1)
            down = quarter - half + pltpu.roll(far, CX - 1, 1)
            r = r + (pltpu.roll(up, 1, 1) + pltpu.roll(down, CX - 1, 1))
            fix = jnp.where(ends, pltpu.roll(XC[v], (2 * CX - 2 - 4 * z) & (CX - 1), 1), 0.0)
            r = r + (0.25 * (ahead + behind) - 0.5 * slope)
            r = r + (fix - 0.0625 * (at(U, v, 2) + at(U, v, -2))) - 1.125 * f
            F[v, pl.ds(pl.multiple_of(z * PLANE, PLANE), PLANE), :] = r
            done.append(sums[v] + r * r)
        return done

    def second_pass(step, sums):
        for k in range(2):
            sums = residual_plane(2 * step + k, sums)
        return sums

    sums = lax.fori_loop(0, CZ // 2, second_pass, [jnp.zeros((CY, CX), F32)] * VARS)

    row8 = iota((8, 4 * CX), 0)
    for t in range(3):
        pair = []
        for v in (2 * t, 2 * t + 1):
            if v == VARS:
                pair.append(jnp.zeros((8, ROWS), F32))
                continue
            tile = jnp.where(iota((8, CX), 0) < 2, inv_x[v, 0:8, :], pltpu.roll(inv_x[v, CX - 8 : CX, :], 4, 0))
            if v & 1:
                tile = pltpu.roll(tile, 4, 0)
            FS[v] = jnp.concatenate(split(F[v]), axis=1)
            hi, lo = split(tile)
            left = jnp.concatenate([jnp.concatenate([hi, hi], 1), jnp.concatenate([lo, lo], 1)], 0)
            both = dot_nt(left, FS[v])
            pair.append(both[0:8] + both[8:16])
        XR[t, ix] = jnp.where(row8 < 4, pair[0], pair[1])
    for d in range(1, px):
        remote(XR.at[:, ix], XR.at[:, ix], xs, xrv, peer("gx", d)).start()

    stat_row = iota((8, CX), 0)
    tile = jnp.where(stat_row == VARS, jnp.max(top), 0.0)
    for v in range(VARS):
        tile = jnp.where(stat_row == v, jnp.sum(sums[v]), tile)
    STX[ix] = tile
    for d in range(1, px):
        remote(STX.at[ix], STX.at[ix], ss.at[0], sr.at[0], peer("gx", d)).start()

    def combine(ref, n):
        total = ref[0]
        for k in range(1, n):
            total = jnp.where(stat_row == VARS, jnp.maximum(total, ref[k]), total + ref[k])
        return total

    def local_x(v, carry):
        XL[v] = nt2(FS[v], AX[v])
        return carry

    lax.fori_loop(0, VARS, local_x, 0)

    drain(XR.at[:, pl.ds(0, px - 1)], xrv)
    factors = [mm3(*split(LX[t]), XR[t].reshape(8 * px, ROWS)) for t in range(3)]
    factors = jnp.concatenate(factors + [jnp.zeros((CX - 24, ROWS), F32)], axis=0).T
    CT[...] = jnp.concatenate(split(factors), axis=1)

    def exchange(axis, me, n, rows, src, dst, v, send, recv):
        mine = pl.ds(pl.multiple_of(me * rows, rows), rows)
        for d in range(1, n):
            to = peer(axis, d)
            there = pl.ds(pl.multiple_of(to[axis] * rows, rows), rows)
            remote(src.at[v, there], dst.at[v, mine], send, recv, to).start()
        dst[v, mine, :] = src[v, mine, :]

    def local_y(v, carry):
        field = XL[v] - nt2(CT[...], WX[v])
        for g in range(4):
            here = slice(128 * g, 128 * g + 128)
            YL[v, here, :] = mm2(MY[v], field[here])
        for k, y in enumerate((0, 1, CY - 2, CY - 1)):
            for t in range(zc):
                lines = YL[v, pl.ds(8 * t * PLANE + y, 8, stride=PLANE), :]
                YF[v, pl.ds(zc * k + t, 8, stride=yr), :] = lines
        exchange("gy", iy, py, yr, YF, YR1, v, ysem, yr1s.at[v])
        return carry

    lax.fori_loop(0, VARS, local_y, 0)
    drain(STX.at[pl.ds(0, px - 1)], sr.at[0])
    STY[iy] = combine(STX, px)
    for d in range(1, py):
        remote(STY.at[iy], STY.at[iy], ss.at[1], sr.at[1], peer("gy", d)).start()

    def reduced_y(v, carry):
        drain(YR1.at[v, pl.ds(0, (py - 1) * yr)], yr1s.at[v])
        Y2[v] = mm2(KY[v], YR1[v])
        exchange("gy", iy, py, yr, Y2, YR2, v, y2sem, yr2s.at[v])
        return carry

    lax.fori_loop(0, VARS, reduced_y, 0)
    drain(STY.at[pl.ds(0, py - 1)], sr.at[1])
    STZ[iz] = combine(STY, py)
    for d in range(1, pz):
        remote(STZ.at[iz], STZ.at[iz], ss.at[2], sr.at[2], peer("gz", d)).start()

    def local_z(v, carry):
        drain(YR2.at[v, pl.ds(0, (py - 1) * yr)], yr2s.at[v])
        column = [SY[v, :, CX * k : CX * k + CX] for k in range(4)]
        for z in range(CZ):
            field = YL[v, z * PLANE : z * PLANE + PLANE, :]
            for k in range(4):
                line = (z & 7) * yr + zc * k + (z >> 3)
                field = field - column[k] * jnp.broadcast_to(YR2[v, line : line + 1, :], (CY, CX))
            FG[0, 8 * z : 8 * z + 8, :] = field[0:8]
            FG[1, 8 * z : 8 * z + 8, :] = field[8:16]
        for g in range(2):
            solved = mm2(MZ[v], FG[g])
            for z in range(CZ):
                ZL[v, z * PLANE + 8 * g : z * PLANE + 8 * g + 8, :] = solved[8 * z : 8 * z + 8]
            for k, z in enumerate((0, 1, CZ - 2, CZ - 1)):
                ZF[v, pl.ds(yc * k + g, 8, stride=zr), :] = solved[8 * z : 8 * z + 8]
        exchange("gz", iz, pz, zr, ZF, ZR1, v, zsem, zr1s.at[v])
        return carry

    lax.fori_loop(0, VARS, local_z, 0)

    def reduced_z(v, carry):
        drain(ZR1.at[v, pl.ds(0, (pz - 1) * zr)], zr1s.at[v])
        Z2[v] = mm3(KZ[0, v], KZ[1, v], ZR1[v])
        exchange("gz", iz, pz, zr, Z2, ZR2, v, z2sem, zr2s.at[v])
        return carry

    lax.fori_loop(0, VARS, reduced_z, 0)
    drain(STZ.at[pl.ds(0, pz - 1)], sr.at[2])
    stats = combine(STZ, pz)
    step = 8000.0 / stats[VARS : VARS + 1]
    rms[...] = jnp.sqrt(stats / float(px * py * pz * ROWS * CX))

    def finish(v, carry):
        drain(ZR2.at[v, pl.ds(0, (pz - 1) * zr)], zr2s.at[v])
        factor = [[ZR2[v, pl.ds(yc * k + g, 8, stride=zr), :] for g in range(2)] for k in range(4)]
        for z in range(CZ):
            weight = [jnp.broadcast_to(SZ[v, z : z + 1, CX * k : CX * k + CX], (8, CX)) for k in range(4)]
            for g in range(2):
                here = slice(z * PLANE + 8 * g, z * PLANE + 8 * g + 8)
                total = ZL[v, here, :]
                for k in range(4):
                    total = total - weight[k] * factor[k][g]
                F[v, here, :] = step * total
        return carry

    lax.fori_loop(0, VARS, finish, 0)
    for copy in halos:
        copy.wait_send()
    drain(XR.at[:, pl.ds(0, px - 1)], xs)
    drain(STX.at[pl.ds(0, px - 1)], ss.at[0])
    drain(STY.at[pl.ds(0, py - 1)], ss.at[1])
    drain(STZ.at[pl.ds(0, pz - 1)], ss.at[2])
    drain(YF.at[:, pl.ds(0, (py - 1) * yr)], ysem)
    drain(Y2.at[:, pl.ds(0, (py - 1) * yr)], y2sem)
    drain(ZF.at[:, pl.ds(0, (pz - 1) * zr)], zsem)
    drain(Z2.at[:, pl.ds(0, (pz - 1) * zr)], z2sem)


def shards(px, py, pz, flow_state, advection, *tables):
    vmem = pl.BlockSpec(memory_space=pltpu.VMEM)
    hbm = pl.BlockSpec(memory_space=pltpu.HBM)
    f32 = lambda *shape: pltpu.VMEM(shape, F32)
    b16 = lambda *shape: pltpu.VMEM(shape, BF16)
    dma = pltpu.SemaphoreType.DMA
    field = (VARS, ROWS, CX)
    padded_rows = ROWS + 4 * PLANE
    y_face, z_face = (VARS, 4 * CZ, CX), (VARS, 4 * CY, CX)
    update, rms = pl.pallas_call(
        functools.partial(kernel, px, py, pz),
        out_shape=(jax.ShapeDtypeStruct(field, F32), jax.ShapeDtypeStruct((8, CX), F32)),
        in_specs=[hbm] * 8,
        out_specs=(vmem, vmem),
        scratch_shapes=[
            pltpu.SMEM(advection.shape, F32), *[f32(*table.shape) for table in tables],
            f32(VARS, padded_rows, CX), f32(3, padded_rows, CX), f32(4, padded_rows, CX),
            f32(2, VARS, 2 * CZ, CX), f32(2, VARS, 2 * CZ, CX), f32(4, VARS, CZ, CX),
            f32(VARS, CY, CX), f32(2, VARS, CY, CX), f32(VARS, CY, CX),
            b16(VARS, ROWS, 2 * CX), f32(*field), f32(*field), f32(*field), f32(2, 256, CX),
            f32(3, px, 8, ROWS), b16(ROWS, 2 * CX),
            *[f32(*y_face)] * 4, *[f32(*z_face)] * 4,
            f32(px, 8, CX), f32(py, 8, CX), f32(pz, 8, CX),
            b16(VARS, 2 * CX, 2 * CX), b16(VARS, 2 * CX, 2 * CX), f32(3, 8, 8 * px),
            b16(VARS, 2 * CX, CX), b16(VARS, 512, 256),
            b16(VARS, 8 * CZ, 4 * CZ), b16(2, VARS, 4 * CY, 4 * CY),
            f32(VARS, CY, 4 * CX), f32(VARS, CZ, 4 * CX),
            dma((8,)), dma((6,)), dma((6,)), dma, dma,
            dma, dma((VARS,)), dma, dma((VARS,)), dma, dma((VARS,)), dma, dma((VARS,)),
            dma((3,)), dma((3,)),
        ],
        compiler_params=pltpu.CompilerParams(
            collective_id=0, has_side_effects=True, vmem_limit_bytes=32 * 1024 * 1024
        ),
        name="adi_step",
    )(*[pltpu.with_memory_space_constraint(x, pltpu.HBM) for x in (advection, flow_state.reshape(field), *tables)])
    return update.reshape(flow_state.shape), rms[:VARS, 0]


def solution(mesh):
    sizes = [mesh.shape[axis] for axis in ("gx", "gy", "gz")]
    return jax.shard_map(
        functools.partial(shards, *sizes),
        mesh=mesh,
        in_specs=(P(None, "gz", "gy", "gx"), P(), P(), P(), P(), P(), P(), P()),
        out_specs=(P(None, "gz", "gy", "gx"), P()),
        check_vma=False,
    )
```

```python
import functools

import jax
import jax.numpy as jnp
from jax import lax
from jax.experimental import pallas as pl
from jax.experimental.pallas import tpu as pltpu
from jax.sharding import PartitionSpec as P

VARS, CX, CY, CZ = 5, 128, 16, 32
PLANE = CY
ROWS = CZ * CY
F32, BF16 = jnp.float32, jnp.bfloat16
MESH = pl.DeviceIdType.MESH
NT = (((1,), (1,)), ((), ()))


def iota(shape, dim):
    return lax.broadcasted_iota(jnp.int32, shape, dim)


def log2(n):
    return n.bit_length() - 1


def split(x):
    hi = x.astype(BF16)
    return hi, (x - hi.astype(F32)).astype(BF16)


def dot(a, b):
    return jnp.dot(a, b, preferred_element_type=F32)


def dot_nt(a, b):
    return lax.dot_general(a, b, NT, preferred_element_type=F32)


def mm2(left, right):
    wide = dot(left, jnp.concatenate(split(right), axis=1))
    m, n = left.shape[0] // 2, right.shape[1]
    return (wide[:m, :n] + wide[:m, n:]) + wide[m:, :n]


def nt2(left, right):
    wide = dot_nt(left, right)
    n = right.shape[0] // 2
    return wide[:, :n] + wide[:, n:]


def mm3(left_hi, left_lo, right):
    hi, lo = split(right)
    return dot(left_hi, hi) + (dot(left_hi, lo) + dot(left_lo, hi))


def one_hot(cond):
    return jnp.where(cond, 1.0, 0.0).astype(BF16)


def edge(k, length):
    return jnp.where(k < 2, k, k + (length - 4))


def expand(parts, rows, row_map, cols, col_map):
    n, m = parts[0].shape
    row_i, _ = row_map(iota((rows, n), 0))
    pick_rows = one_hot(row_i == iota((rows, n), 1))
    col_j, _ = col_map(iota((m, cols), 1))
    pick_cols = one_hot(col_j == iota((m, cols), 0))
    _, row_r = row_map(iota((rows, cols), 0))
    _, col_c = col_map(iota((rows, cols), 1))
    keep = row_r == col_c
    return [
        jnp.where(keep, dot(pick_rows, dot(part, pick_cols).astype(BF16)), 0.0).astype(BF16)
        for part in parts
    ]


def coupling(shape, speed, row_of):
    row, col = iota(shape, 0), iota(shape, 1)
    base, k = row_of(row)
    lower, upper = -0.5 * speed - 2.0, 0.5 * speed - 2.0
    out = jnp.where((k == 0) & (col == base - 2), 0.5, 0.0)
    out = out + jnp.where((k == 0) & (col == base - 1), lower, 0.0)
    out = out + jnp.where((k == 1) & (col == base - 1), 0.5, 0.0)
    out = out + jnp.where((k == 2) & (col == base + 4), 0.5, 0.0)
    out = out + jnp.where((k == 3) & (col == base + 4), upper, 0.0)
    return out + jnp.where((k == 3) & (col == base + 5), 0.5, 0.0)


def primitives(u):
    scale = 1.0 / u[0]
    vel = [u[1] * scale, u[2] * scale, u[3] * scale]
    kinetic = 0.5 * (vel[0] * vel[0] + vel[1] * vel[1] + vel[2] * vel[2])
    internal = jnp.maximum(u[4] * scale - kinetic, 0.25)
    return vel, internal, 0.4 * u[0] * internal


def fluxes(u, w, pressure, direction):
    out = [u[1 + direction]]
    for c in range(3):
        moment = u[1 + c] * w
        out.append(moment + pressure if c == direction else moment)
    return out + [(u[4] + pressure) * w]


def kernel(
    px, py, pz,
    tab_adv, flow, *refs,
):
    (
        tab_x, tab_y, tab_z, tab_rx, tab_ry, tab_rz,
        F, rms,
        adv, inv_x, inv_y, inv_z, red_x, red_y, red_z,
        U, PR, FZ, YS, YH, HY, PK, XH, XC, FS, XL, G, FG, XR, CT,
        YF, YR1, Y2, YR2, ZF, ZR1, Z2, ZR2, E, ER, CF, STX, STY, STZ,
        AX, WX, LX, MY, MZ, KY, KZ, SY, SZ,
        in_sem, hs, hr, xs, xrv, ysem, yr1s, y2sem, yr2s, zsem, zr1s, z2sem, zr2s, es, ers, ss, sr,
    ) = refs
    ix, iy, iz = lax.axis_index("gx"), lax.axis_index("gy"), lax.axis_index("gz")
    zc, yc = CZ // py, CY // pz
    yr, zr = 4 * zc, 4 * yc

    def peer(axis, d):
        me, n = {"gx": (ix, px), "gy": (iy, py), "gz": (iz, pz)}[axis]
        return {axis: (me + d + n) & (n - 1)}

    def remote(src, dst, send, recv, device):
        return pltpu.make_async_remote_copy(
            src_ref=src, dst_ref=dst, send_sem=send, recv_sem=recv,
            device_id=device, device_id_type=MESH,
        )

    def drain(ref, sem):
        pltpu.make_async_copy(ref, ref, sem).wait()

    load = pltpu.make_async_copy(flow, U.at[:, pl.ds(2 * PLANE, ROWS)], in_sem.at[0])
    load.start()
    tables = [
        pltpu.make_async_copy(src, dst, in_sem.at[1 + k])
        for k, (src, dst) in enumerate(zip(
            (tab_adv, tab_x, tab_y, tab_z, tab_rx, tab_ry, tab_rz),
            (adv, inv_x, inv_y, inv_z, red_x, red_y, red_z),
        ))
    ]
    for copy in tables:
        copy.start()
    barrier = pltpu.get_barrier_semaphore()
    for axis, n in (("gz", pz), ("gy", py), ("gx", px)):
        for d in range(1, n):
            pl.semaphore_signal(barrier, inc=1, device_id=peer(axis, d), device_id_type=MESH)
    load.wait()

    def pack_rows(v, carry):
        for r in range(2):
            for t in range(CZ // 8):
                for side, first in ((0, CY - 2), (1, 0)):
                    start = 2 * PLANE + 8 * t * PLANE + first + r
                    YS[side, v, pl.ds(r * CZ + 8 * t, 8), :] = U[v, pl.ds(start, 8, stride=PLANE), :]
        return carry

    lax.fori_loop(0, VARS, pack_rows, 0, unroll=True)
    lane = iota((CY, CX), 1)
    row = iota((CY, CX), 0)

    def pack_lanes(v, carry):
        acc = jnp.zeros((CY, CX), F32)
        for z in range(CZ):
            plane = U[v, pl.ds((2 + z) * PLANE, PLANE), :]
            acc = jnp.where((lane >> 2) == z, pltpu.roll(plane, (4 * z + 2) % CX, 1), acc)
        PK[v] = acc
        return carry

    lax.fori_loop(0, VARS, pack_lanes, 0, unroll=True)

    pl.semaphore_wait(barrier, px + py + pz - 3)
    last = 2 * PLANE + ROWS
    halos = [
        remote(flow.at[:, pl.ds(ROWS - 2 * PLANE, 2 * PLANE)], U.at[:, pl.ds(0, 2 * PLANE)],
               hs.at[0], hr.at[0], peer("gz", 1)),
        remote(flow.at[:, pl.ds(0, 2 * PLANE)], U.at[:, pl.ds(last, 2 * PLANE)],
               hs.at[1], hr.at[1], peer("gz", -1)),
        remote(YS.at[0], YH.at[0], hs.at[2], hr.at[2], peer("gy", 1)),
        remote(YS.at[1], YH.at[1], hs.at[3], hr.at[3], peer("gy", -1)),
        remote(PK, XH.at[0], hs.at[4], hr.at[4], peer("gx", 1)),
        remote(PK, XH.at[1], hs.at[5], hr.at[5], peer("gx", -1)),
    ]
    for copy in halos:
        copy.start()

    def plane_primitives(base):
        here = pl.ds(base, PLANE)
        u = [U[v, here, :] for v in range(VARS)]
        vel, internal, pressure = primitives(u)
        PR[0, here, :], PR[1, here, :], PR[2, here, :] = vel[0], vel[1], pressure
        for k, f in enumerate(fluxes(u, vel[2], pressure, 2)[1:]):
            FZ[k, here, :] = f
        return vel, internal

    def first_pass(step, top):
        for k in range(2):
            base = pl.multiple_of(2 * PLANE + (2 * step + k) * PLANE, PLANE)
            vel, internal = plane_primitives(base)
            speed = jnp.abs(vel[0]) + jnp.abs(vel[1]) + jnp.abs(vel[2]) + jnp.sqrt(3.0 * 1.4 * 0.4 * internal)
            top = jnp.maximum(top, speed)
        return top

    top = lax.fori_loop(0, CZ // 2, first_pass, jnp.zeros((CY, CX), F32))

    for copy in tables:
        copy.wait()
    def exact_dot(a, b):
        return mm3(*split(a), b)

    def columns(table, length):
        shape = (length, 4 * CX)
        pick = one_hot(iota(shape, 0) == edge(iota(shape, 1) >> 7, length))
        hi, lo = split(table)
        return dot(hi, pick) + dot(lo, pick)

    def build_first(v, carry):
        hi, lo = split(inv_x[v])
        AX[v] = jnp.concatenate([jnp.concatenate([hi, hi], 1), jnp.concatenate([lo, lo], 1)], 0)
        col = iota((CX, CX), 1)
        pick = one_hot(((col >> 2) == (v & 1)) & (iota((CX, CX), 0) == edge(col & 3, CX)))
        hi, lo = dot(hi, pick).astype(BF16), dot(lo, pick).astype(BF16)
        WX[v] = jnp.concatenate([jnp.concatenate([hi, hi], 1), jnp.concatenate([lo, lo], 1)], 0)

        pick = one_hot(iota((CY, CX), 0) == (iota((CY, CX), 1) & (CY - 1)))
        for part, table in enumerate(split(inv_y[v])):
            spread = dot(table, pick)
            for z in range(8):
                block = jnp.where((lane >> 4) == z, spread, 0.0)
                MY[v, part * CX + 16 * z : part * CX + 16 * z + 16, :] = block.astype(BF16)
        return carry

    lax.fori_loop(0, VARS, build_first, 0, unroll=True)
    for t in range(3):
        acc = jnp.zeros((8, 8 * px), F32)
        for v in (2 * t, 2 * t + 1):
            if v == VARS:
                continue
            own = coupling((8, 4 * px), adv[0, v], lambda r: (4 * ix, r & 3))
            rows = exact_dot(own, red_x[v])
            r, c = iota((4 * px, 8 * px), 0), iota((4 * px, 8 * px), 1)
            wide = exact_dot(rows, jnp.where(r == ((c >> 3) << 2) + (c & 3), 1.0, 0.0))
            r, c = iota((8, 8 * px), 0), iota((8, 8 * px), 1)
            acc = acc + jnp.where(((r >> 2) == v - 2 * t) & (((c >> 2) & 1) == v - 2 * t), wide, 0.0)
        LX[t] = acc

    ends = ((lane + 2) & (CX - 1)) < 4

    def residual_plane(group, z):
        base = pl.multiple_of(2 * PLANE + z * PLANE, PLANE)

        def at(ref, k, step):
            return ref[k, pl.ds(base + step * PLANE, PLANE), :]

        u = [at(U, v, 0) for v in range(VARS)]
        pressure = at(PR, 2, 0)
        x_flux = fluxes(u, at(PR, 0, 0), pressure, 0)
        y_flux = fluxes(u, at(PR, 1, 0), pressure, 1)
        for v in group:
            f = u[v]
            ahead, behind = at(U, v, 1), at(U, v, -1)
            if v == 0:
                slope = at(U, 3, 1) - at(U, 3, -1)
            else:
                slope = at(FZ, v - 1, 1) - at(FZ, v - 1, -1)

            far, quarter = -0.0625 * f, 0.25 * f
            half = 0.5 * y_flux[v]
            up = quarter + half + pltpu.roll(far, 1, 0)
            down = quarter - half + pltpu.roll(far, CY - 1, 0)
            r = pltpu.roll(up, 1, 0) + pltpu.roll(down, CY - 1, 0)
            half = 0.5 * x_flux[v]
            up = quarter + half + pltpu.roll(far, 1, 1)
            down = quarter - half + pltpu.roll(far, CX - 1, 1)
            r = r + (pltpu.roll(up, 1, 1) + pltpu.roll(down, CX - 1, 1))
            r = r + (0.25 * (ahead + behind) - 0.5 * slope)
            r = r - 0.0625 * (at(U, v, 2) + at(U, v, -2)) - 1.125 * f
            F[v, pl.ds(pl.multiple_of(z * PLANE, PLANE), PLANE), :] = r

    def interior(step, carry):
        for k in range(2):
            residual_plane(range(VARS), 2 + 2 * step + k)
        return carry

    lax.fori_loop(0, (CZ - 4) // 2, interior, 0)
    def build_z(v, carry):
        wide = iota((CZ, 8 * CZ), 1)
        pick = one_hot(iota((CZ, 8 * CZ), 0) == (wide >> 3))
        r, c = iota((16, 8 * CZ), 0), iota((16, 8 * CZ), 1)
        keep, first = (r & 7) == (c & 7), r < 8
        for part, table in enumerate(split(inv_z[v])):
            spread = dot(table, pick)
            for k in range(CZ // 2):
                pair = [jnp.broadcast_to(spread[z : z + 1], (16, 8 * CZ)) for z in (2 * k, 2 * k + 1)]
                block = jnp.where(keep, jnp.where(first, pair[0], pair[1]), 0.0)
                MZ[v, part * 256 + 16 * k : part * 256 + 16 * k + 16, :] = block.astype(BF16)
        return carry

    lax.fori_loop(0, VARS, build_z, 0, unroll=True)
    for copy in halos:
        copy.wait_recv()
    plane_primitives(PLANE)
    plane_primitives(last)
    for side in range(2):
        half = 0.5 - side
        parts = []
        for ref, which in ((YH, side), (YS, side)):
            near, far = pl.ds((1 - side) * CZ, CZ), pl.ds(side * CZ, CZ)
            u = [ref[which, v, near, :] for v in range(VARS)]
            vel, _, pressure = primitives(u)
            parts.append([
                (-0.0625 * u[v], 0.25 * u[v] + half * f - 0.0625 * ref[which, v, far, :])
                for v, f in enumerate(fluxes(u, vel[1], pressure, 1))
            ])
        for v in range(VARS):
            for k in range(2):
                HY[2 * side + k, v] = parts[0][v][k] - parts[1][v][k]
    j = lane & 3
    near = [jnp.where(j < 2, XH[0, v], XH[1, v]) for v in range(VARS)]
    mine = [PK[v] for v in range(VARS)]
    vel, _, pressure = primitives(near)
    near_flux = fluxes(near, vel[0], pressure, 0)
    vel, _, pressure = primitives(mine)
    mine_flux = fluxes(mine, vel[0], pressure, 0)
    for v in range(VARS):
        du, df = near[v] - mine[v], near_flux[v] - mine_flux[v]
        far = -0.0625 * jnp.where(j < 2, pltpu.roll(du, CX - 2, 1), pltpu.roll(du, 2, 1))
        right = pltpu.roll(-0.5 * df + 0.25 * du, CX - 1, 1)
        left = pltpu.roll(0.5 * df + 0.25 * du, 1, 1)
        XC[v] = far + jnp.where(j == 1, right, 0.0) + jnp.where(j == 2, left, 0.0)

    row8 = iota((8, 4 * CX), 0)
    groups = ((0, 1), (2, 3), (4,))
    sums = []
    for t, group in enumerate(groups):

        for z in (0, 1, CZ - 2, CZ - 1):
            residual_plane(group, z)
        for v in group:
            for k, y in ((1, 0), (0, 1), (2, CY - 2), (3, CY - 1)):
                for c in range(CZ // 8):
                    lines = pl.ds(8 * c * PLANE + y, 8, stride=PLANE)
                    F[v, lines, :] = F[v, lines, :] + HY[k, v, 8 * c : 8 * c + 8, :]

        def second_pass(step, sums, group=group):
            sums = list(sums)
            for k in range(4):
                z = 4 * step + k
                here = pl.ds(pl.multiple_of(z * PLANE, PLANE), PLANE)
                for i, v in enumerate(group):
                    fix = pltpu.roll(XC[v], (2 * CX - 2 - 4 * z) & (CX - 1), 1)
                    r = F[v, here, :] + jnp.where(ends, fix, 0.0)
                    sums[i] = sums[i] + r * r
                    FS[v, here, 0:CX], FS[v, here, CX : 2 * CX] = split(r)
            return sums

        sums += lax.fori_loop(0, CZ // 4, second_pass, [jnp.zeros((CY, CX), F32)] * len(group))
        pair = [jnp.zeros((8, ROWS), F32)] * 2
        for v in group:
            tile = jnp.where(iota((8, CX), 0) < 2, inv_x[v, 0:8, :], pltpu.roll(inv_x[v, CX - 8 : CX, :], 4, 0))
            if v & 1:
                tile = pltpu.roll(tile, 4, 0)
            hi, lo = split(tile)
            left = jnp.concatenate([jnp.concatenate([hi, hi], 1), jnp.concatenate([lo, lo], 1)], 0)
            both = dot_nt(left, FS[v])
            pair[v & 1] = both[0:8] + both[8:16]
        XR[t, ix] = jnp.where(row8 < 4, pair[0], pair[1])
        for d in range(1, px):
            remote(XR.at[t, ix], XR.at[t, ix], xs, xrv.at[t], peer("gx", d)).start()

    stat_row = iota((8, CX), 0)
    tile = jnp.where(stat_row == VARS, jnp.max(top), 0.0)
    for v in range(VARS):
        tile = jnp.where(stat_row == v, jnp.sum(sums[v]), tile)
    STX[ix] = tile
    for d in range(1, px):
        remote(STX.at[ix], STX.at[ix], ss.at[0], sr.at[0], peer("gx", d)).start()

    def combine(ref, n):
        total = ref[0]
        for k in range(1, n):
            total = jnp.where(stat_row == VARS, jnp.maximum(total, ref[k]), total + ref[k])
        return total

    def local_x(v, carry):
        XL[v] = nt2(FS[v], AX[v])
        return carry

    lax.fori_loop(0, VARS, local_x, 0, unroll=True)

    def exchange(axis, me, n, rows, src, dst, v, send, recv):
        mine = pl.ds(pl.multiple_of(me * rows, rows), rows)
        for d in range(1, n):
            to = peer(axis, d)
            there = pl.ds(pl.multiple_of(to[axis] * rows, rows), rows)
            remote(src.at[v, there], dst.at[v, mine], send, recv, to).start()
        dst[v, mine, :] = src[v, mine, :]

    faces = ((0, 0), (0, 1), (1, 6), (1, 7))

    def local_yz(group):
        for v in group:
            for half in range(2):
                here = slice(256 * half, 256 * half + 256)
                field = XL[v, here, :] - nt2(CT[v >> 1, here, :], WX[v])
                for g in range(2):
                    solved = mm2(MY[v], field[128 * g : 128 * g + 128])
                    for k in range(16):
                        z, h = 8 * (2 * half + g) + k // 2, k & 1
                        FG[v & 1, h, 8 * z : 8 * z + 8, :] = solved[8 * k : 8 * k + 8]
        for v in group:
            for h in range(2):
                G[v, h] = mm2(MZ[v], FG[v & 1, h])
        for v in group:
            for h in range(2):
                for k, z in enumerate((0, 1, CZ - 2, CZ - 1)):
                    ZF[v, pl.ds(yc * k + h, 8, stride=zr), :] = G[v, h, 8 * z : 8 * z + 8, :]
            exchange("gz", iz, pz, zr, ZF, ZR1, v, zsem, zr1s.at[v])
            for k, (h, y) in enumerate(faces):
                for t in range(zc):
                    YF[v, pl.ds(zc * k + t, 8, stride=yr), :] = G[v, h, pl.ds(64 * t + y, 8, stride=8), :]
            exchange("gy", iy, py, yr, YF, YR1, v, ysem, yr1s.at[v])

    for t, group in enumerate(groups):
        drain(XR.at[t, pl.ds(0, px - 1)], xrv.at[t])
        factors = mm3(*split(LX[t]), XR[t].reshape(8 * px, ROWS))
        factors = jnp.concatenate([factors, jnp.zeros((CX - 8, ROWS), F32)], axis=0).T
        CT[t] = jnp.concatenate(split(factors), axis=1)
        local_yz(group)
        if t == 0:
            drain(STX.at[pl.ds(0, px - 1)], sr.at[0])
            STY[iy] = combine(STX, px)
            for d in range(1, py):
                remote(STY.at[iy], STY.at[iy], ss.at[1], sr.at[1], peer("gy", d)).start()
        if t == 2:
            drain(STY.at[pl.ds(0, py - 1)], sr.at[1])
            STZ[iz] = combine(STY, py)
            for d in range(1, pz):
                remote(STZ.at[iz], STZ.at[iz], ss.at[2], sr.at[2], peer("gz", d)).start()

    def build_reduced(v, carry):
        def reduced(red, n, speed):
            g = coupling((4 * n, 4 * n), speed, lambda r: ((r >> 2) << 2, r & 3))
            return split(exact_dot(g, red))

        y_side = lambda r: (r >> log2(zc), r & (zc - 1))
        hi, lo = expand(reduced(red_y[v], py, adv[1, v]), 4 * CZ, y_side, 4 * CZ, y_side)
        KY[v, 0:CX, :], KY[v, CX : 2 * CX, :] = hi, lo
        z_side = lambda r: (r >> log2(yc), r & (yc - 1))
        KZ[0, v], KZ[1, v] = expand(reduced(red_z[v], pz, adv[2, v]), 4 * CY, z_side, 4 * CY, z_side)
        return carry

    lax.fori_loop(0, VARS, build_reduced, 0, unroll=True)

    def reduced_lines(v, carry):
        drain(YR1.at[v, pl.ds(0, (py - 1) * yr)], yr1s.at[v])
        Y2[v] = mm2(KY[v], YR1[v])
        exchange("gy", iy, py, yr, Y2, YR2, v, y2sem, yr2s.at[v])
        drain(ZR1.at[v, pl.ds(0, (pz - 1) * zr)], zr1s.at[v])
        Z2[v] = mm3(KZ[0, v], KZ[1, v], ZR1[v])
        exchange("gz", iz, pz, zr, Z2, ZR2, v, z2sem, zr2s.at[v])
        return carry

    lax.fori_loop(0, VARS, reduced_lines, 0)

    def build_columns(v, carry):
        SY[v] = columns(inv_y[v], CY)
        SZ[v] = columns(inv_z[v], CZ)
        return carry

    lax.fori_loop(0, VARS, build_columns, 0, unroll=True)

    def correct_z(v, carry):
        drain(ZR2.at[v, pl.ds(0, (pz - 1) * zr)], zr2s.at[v])
        for k, (h, y) in enumerate(faces):
            E[v, 4 * k : 4 * k + 4, :] = ZR2[v, pl.ds(zr * y + h, 4, stride=yc), :]
        mine = pl.ds(pl.multiple_of(16 * iy, 16), 16)
        for d in range(1, py):
            remote(E.at[v], ER.at[v, mine], es, ers.at[v], peer("gy", d)).start()
        ER[v, mine, :] = E[v]
        factor = [[ZR2[v, pl.ds(yc * k + h, 8, stride=zr), :] for h in range(2)] for k in range(4)]
        for z in range(CZ):
            weight = [jnp.broadcast_to(SZ[v, z : z + 1, CX * k : CX * k + CX], (8, CX)) for k in range(4)]
            for h in range(2):
                total = G[v, h, 8 * z : 8 * z + 8, :]
                for k in range(4):
                    total = total - weight[k] * factor[k][h]
                G[v, h, 8 * z : 8 * z + 8, :] = total
        return carry

    lax.fori_loop(0, VARS, correct_z, 0)
    drain(STZ.at[pl.ds(0, pz - 1)], sr.at[2])
    stats = combine(STZ, pz)
    step = 8000.0 / stats[VARS : VARS + 1]
    rms[...] = jnp.sqrt(stats / float(px * py * pz * ROWS * CX))

    def finish(v, carry):
        drain(YR2.at[v, pl.ds(0, (py - 1) * yr)], yr2s.at[v])
        drain(ER.at[v, pl.ds(0, (py - 1) * 16)], ers.at[v])
        left = [KY[v, pl.ds(pl.multiple_of(part * CX + 16 * iy, 16), 16), :] for part in range(2)]
        cross = mm2(jnp.concatenate(left, axis=0), ER[v])
        for t in range(zc):
            weight = [SZ[v, 8 * t : 8 * t + 8, CX * j : CX * j + CX] for j in range(4)]
            for k in range(4):
                total = YR2[v, pl.ds(zc * k + t, 8, stride=yr), :]
                for j in range(4):
                    total = total - weight[j] * jnp.broadcast_to(cross[4 * k + j : 4 * k + j + 1], (8, CX))
                CF[k, 8 * t : 8 * t + 8, :] = total
        column = [SY[v, :, CX * k : CX * k + CX] * step for k in range(4)]
        for z in range(CZ):
            line = [jnp.broadcast_to(CF[k, z : z + 1, :], (8, CX)) for k in range(4)]
            for h in range(2):
                total = step * G[v, h, 8 * z : 8 * z + 8, :]
                for k in range(4):
                    total = total - column[k][8 * h : 8 * h + 8] * line[k]
                F[v, z * PLANE + 8 * h : z * PLANE + 8 * h + 8, :] = total
        return carry

    lax.fori_loop(0, VARS, finish, 0)
    for copy in halos:
        copy.wait_send()
    drain(XR.at[:, pl.ds(0, px - 1)], xs)
    drain(STX.at[pl.ds(0, px - 1)], ss.at[0])
    drain(STY.at[pl.ds(0, py - 1)], ss.at[1])
    drain(STZ.at[pl.ds(0, pz - 1)], ss.at[2])
    drain(YF.at[:, pl.ds(0, (py - 1) * yr)], ysem)
    drain(Y2.at[:, pl.ds(0, (py - 1) * yr)], y2sem)
    drain(ZF.at[:, pl.ds(0, (pz - 1) * zr)], zsem)
    drain(Z2.at[:, pl.ds(0, (pz - 1) * zr)], z2sem)
    drain(ER.at[:, pl.ds(0, (py - 1) * 16)], es)


def shards(px, py, pz, flow_state, advection, *tables):
    vmem = pl.BlockSpec(memory_space=pltpu.VMEM)
    hbm = pl.BlockSpec(memory_space=pltpu.HBM)
    f32 = lambda *shape: pltpu.VMEM(shape, F32)
    b16 = lambda *shape: pltpu.VMEM(shape, BF16)
    dma = pltpu.SemaphoreType.DMA
    field = (VARS, ROWS, CX)
    padded_rows = ROWS + 4 * PLANE
    y_face, z_face = (VARS, 4 * CZ, CX), (VARS, 4 * CY, CX)
    update, rms = pl.pallas_call(
        functools.partial(kernel, px, py, pz),
        out_shape=(jax.ShapeDtypeStruct(field, F32), jax.ShapeDtypeStruct((8, CX), F32)),
        in_specs=[hbm] * 8,
        out_specs=(vmem, vmem),
        scratch_shapes=[
            pltpu.SMEM(advection.shape, F32), *[f32(*table.shape) for table in tables],
            f32(VARS, padded_rows, CX), f32(3, padded_rows, CX), f32(4, padded_rows, CX),
            f32(2, VARS, 2 * CZ, CX), f32(2, VARS, 2 * CZ, CX), f32(4, VARS, CZ, CX),
            f32(VARS, CY, CX), f32(2, VARS, CY, CX), f32(VARS, CY, CX),
            b16(VARS, ROWS, 2 * CX), f32(*field), f32(VARS, 2, ROWS // 2, CX), f32(2, 2, ROWS // 2, CX),
            f32(3, px, 8, ROWS), b16(3, ROWS, 2 * CX),
            *[f32(*y_face)] * 4, *[f32(*z_face)] * 4,
            f32(VARS, 16, CX), f32(VARS, 16 * py, CX), f32(4, CZ, CX),
            f32(px, 8, CX), f32(py, 8, CX), f32(pz, 8, CX),
            b16(VARS, 2 * CX, 2 * CX), b16(VARS, 2 * CX, 2 * CX), f32(3, 8, 8 * px),
            b16(VARS, 2 * CX, CX), b16(VARS, 512, 256),
            b16(VARS, 8 * CZ, 4 * CZ), b16(2, VARS, 4 * CY, 4 * CY),
            f32(VARS, CY, 4 * CX), f32(VARS, CZ, 4 * CX),
            dma((8,)), dma((6,)), dma((6,)), dma, dma((3,)),
            *[dma, dma((VARS,))] * 5,
            dma((3,)), dma((3,)),
        ],
        compiler_params=pltpu.CompilerParams(
            collective_id=0, has_side_effects=True, vmem_limit_bytes=32 * 1024 * 1024
        ),
        name="adi_step",
    )(*[pltpu.with_memory_space_constraint(x, pltpu.HBM) for x in (advection, flow_state.reshape(field), *tables)])
    return update.reshape(flow_state.shape), rms[:VARS, 0]


def solution(mesh):
    sizes = [mesh.shape[axis] for axis in ("gx", "gy", "gz")]
    return jax.shard_map(
        functools.partial(shards, *sizes),
        mesh=mesh,
        in_specs=(P(None, "gz", "gy", "gx"), P(), P(), P(), P(), P(), P(), P()),
        out_specs=(P(None, "gz", "gy", "gx"), P()),
        check_vma=False,
    )
```

```python
import functools

import jax
import jax.numpy as jnp
from jax import lax
from jax.experimental import pallas as pl
from jax.experimental.pallas import tpu as pltpu
from jax.sharding import PartitionSpec as P

VARS, CX, CY, CZ = 5, 128, 16, 32
PLANE = CY
ROWS = CZ * CY
F32, BF16 = jnp.float32, jnp.bfloat16
MESH = pl.DeviceIdType.MESH
NT = (((1,), (1,)), ((), ()))


def iota(shape, dim):
    return lax.broadcasted_iota(jnp.int32, shape, dim)


def log2(n):
    return n.bit_length() - 1


def split(x):
    hi = x.astype(BF16)
    return hi, (x - hi.astype(F32)).astype(BF16)


def dot(a, b):
    return jnp.dot(a, b, preferred_element_type=F32)


def dot_nt(a, b):
    return lax.dot_general(a, b, NT, preferred_element_type=F32)


def mm2(left, right):
    wide = dot(left, jnp.concatenate(split(right), axis=1))
    m, n = left.shape[0] // 2, right.shape[1]
    return (wide[:m, :n] + wide[:m, n:]) + wide[m:, :n]


def nt2(left, right):
    wide = dot_nt(left, right)
    n = right.shape[0] // 2
    return wide[:, :n] + wide[:, n:]


def mm3(left_hi, left_lo, right):
    hi, lo = split(right)
    return dot(left_hi, hi) + (dot(left_hi, lo) + dot(left_lo, hi))


def one_hot(cond):
    return jnp.where(cond, 1.0, 0.0).astype(BF16)


def edge(k, length):
    return jnp.where(k < 2, k, k + (length - 4))


def primitives(u):
    scale = 1.0 / u[0]
    vel = [u[1] * scale, u[2] * scale, u[3] * scale]
    kinetic = 0.5 * (vel[0] * vel[0] + vel[1] * vel[1] + vel[2] * vel[2])
    internal = jnp.maximum(u[4] * scale - kinetic, 0.25)
    return vel, internal, 0.4 * u[0] * internal


def fluxes(u, w, pressure, direction):
    out = [u[1 + direction]]
    for c in range(3):
        moment = u[1 + c] * w
        out.append(moment + pressure if c == direction else moment)
    return out + [(u[4] + pressure) * w]


def kernel(
    px, py, pz,
    tab_adv, flow, *refs,
):
    (
        tab_x, tab_y, tab_z, tab_rx, tab_ry, tab_rz,
        F, rms,
        adv, inv_x, inv_y, inv_z, RX, RP,
        U, PR, FZ, YS, YH, HY, PK, XH, XC, FS, XL, G, FG, XR, CT,
        YF, YR1, Y2, YR2, ZF, ZR1, Z2, ZR2, E, ER, CF, STX, STY, STZ,
        AX, WX, LX, MY, MZ, KY, KZ, SY, SZ,
        in_sem, hs, hr, xs, xrv, ysem, yr1s, y2sem, yr2s, zsem, zr1s, z2sem, zr2s, es, ers, ss, sr,
    ) = refs
    ix, iy, iz = lax.axis_index("gx"), lax.axis_index("gy"), lax.axis_index("gz")
    zc, yc = CZ // py, CY // pz
    yr, zr = 4 * zc, 4 * yc

    def peer(axis, d):
        me, n = {"gx": (ix, px), "gy": (iy, py), "gz": (iz, pz)}[axis]
        return {axis: (me + d + n) & (n - 1)}

    def remote(src, dst, send, recv, device):
        return pltpu.make_async_remote_copy(
            src_ref=src, dst_ref=dst, send_sem=send, recv_sem=recv,
            device_id=device, device_id_type=MESH,
        )

    def drain(ref, sem):
        pltpu.make_async_copy(ref, ref, sem).wait()

    load = pltpu.make_async_copy(flow, U.at[:, pl.ds(2 * PLANE, ROWS)], in_sem.at[0])
    load.start()
    tables = [
        pltpu.make_async_copy(src, dst, in_sem.at[1 + k])
        for k, (src, dst) in enumerate(zip(
            (tab_adv, tab_x, tab_y, tab_z, tab_rx, tab_ry, tab_rz),
            (adv, inv_x, inv_y, inv_z, RX.at[:, pl.ds(8, 4 * px)], RP.at[0, :, pl.ds(8, 4 * py)], RP.at[1, :, pl.ds(8, 4 * pz)]),
        ))
    ]
    for copy in tables:
        copy.start()
    for axis, n in enumerate((py, pz)):
        for start in (0, 8 + 4 * n):
            RP[axis, :, start : start + 8, :] = jnp.zeros((VARS, 8, 4 * n), F32)
    for start in (0, 8 + 4 * px):
        RX[:, start : start + 8, :] = jnp.zeros((VARS, 8, 4 * px), F32)
    barrier = pltpu.get_barrier_semaphore()
    for axis, n in (("gz", pz), ("gy", py), ("gx", px)):
        for d in range(1, n):
            pl.semaphore_signal(barrier, inc=1, device_id=peer(axis, d), device_id_type=MESH)
    load.wait()

    def pack_rows(v, carry):
        for r in range(2):
            for t in range(CZ // 8):
                for side, first in ((0, CY - 2), (1, 0)):
                    start = 2 * PLANE + 8 * t * PLANE + first + r
                    YS[side, v, pl.ds(r * CZ + 8 * t, 8), :] = U[v, pl.ds(start, 8, stride=PLANE), :]
        return carry

    lax.fori_loop(0, VARS, pack_rows, 0, unroll=True)
    lane = iota((CY, CX), 1)
    row = iota((CY, CX), 0)

    def pack_lanes(v, carry):
        acc = jnp.zeros((CY, CX), F32)
        for z in range(CZ):
            plane = U[v, pl.ds((2 + z) * PLANE, PLANE), :]
            acc = jnp.where((lane >> 2) == z, pltpu.roll(plane, (4 * z + 2) % CX, 1), acc)
        PK[v] = acc
        return carry

    lax.fori_loop(0, VARS, pack_lanes, 0, unroll=True)

    pl.semaphore_wait(barrier, px + py + pz - 3)
    last = 2 * PLANE + ROWS
    halos = [
        remote(flow.at[:, pl.ds(ROWS - 2 * PLANE, 2 * PLANE)], U.at[:, pl.ds(0, 2 * PLANE)],
               hs.at[0], hr.at[0], peer("gz", 1)),
        remote(flow.at[:, pl.ds(0, 2 * PLANE)], U.at[:, pl.ds(last, 2 * PLANE)],
               hs.at[1], hr.at[1], peer("gz", -1)),
        remote(YS.at[0], YH.at[0], hs.at[2], hr.at[2], peer("gy", 1)),
        remote(YS.at[1], YH.at[1], hs.at[3], hr.at[3], peer("gy", -1)),
        remote(PK, XH.at[0], hs.at[4], hr.at[4], peer("gx", 1)),
        remote(PK, XH.at[1], hs.at[5], hr.at[5], peer("gx", -1)),
    ]
    for copy in halos:
        copy.start()

    def plane_primitives(base):
        here = pl.ds(base, PLANE)
        u = [U[v, here, :] for v in range(VARS)]
        vel, internal, pressure = primitives(u)
        PR[0, here, :], PR[1, here, :], PR[2, here, :] = vel[0], vel[1], pressure
        for k, f in enumerate(fluxes(u, vel[2], pressure, 2)[1:]):
            FZ[k, here, :] = f
        return vel, internal

    top = jnp.zeros((CY, CX), F32)
    for z in range(CZ):
        vel, internal = plane_primitives((2 + z) * PLANE)
        speed = jnp.abs(vel[0]) + jnp.abs(vel[1]) + jnp.abs(vel[2]) + jnp.sqrt(3.0 * 1.4 * 0.4 * internal)
        top = jnp.maximum(top, speed)

    for copy in tables:
        copy.wait()
    def columns(table, length):
        shape = (length, 4 * CX)
        pick = one_hot(iota(shape, 0) == edge(iota(shape, 1) >> 7, length))
        hi, lo = split(table)
        return dot(hi, pick) + dot(lo, pick)

    def build_first(v, carry):
        hi, lo = split(inv_x[v])
        AX[v] = jnp.concatenate([jnp.concatenate([hi, hi], 1), jnp.concatenate([lo, lo], 1)], 0)
        col = iota((CX, CX), 1)
        pick = one_hot(((col >> 2) == (v & 1)) & (iota((CX, CX), 0) == edge(col & 3, CX)))
        hi, lo = dot(hi, pick).astype(BF16), dot(lo, pick).astype(BF16)
        WX[v] = jnp.concatenate([jnp.concatenate([hi, hi], 1), jnp.concatenate([lo, lo], 1)], 0)

        pick = one_hot(iota((CY, CX), 0) == (iota((CY, CX), 1) & (CY - 1)))
        for part, table in enumerate(split(inv_y[v])):
            spread = dot(table, pick)
            for z in range(8):
                block = jnp.where((lane >> 4) == z, spread, 0.0)
                MY[v, part * CX + 16 * z : part * CX + 16 * z + 16, :] = block.astype(BF16)
        return carry

    lax.fori_loop(0, VARS, build_first, 0, unroll=True)
    ends = ((lane + 2) & (CX - 1)) < 4

    def residual_plane(group, z):
        base = pl.multiple_of(2 * PLANE + z * PLANE, PLANE)

        def at(ref, k, step):
            return ref[k, pl.ds(base + step * PLANE, PLANE), :]

        u = [at(U, v, 0) for v in range(VARS)]
        pressure = at(PR, 2, 0)
        x_flux = fluxes(u, at(PR, 0, 0), pressure, 0)
        y_flux = fluxes(u, at(PR, 1, 0), pressure, 1)
        for v in group:
            f = u[v]
            ahead, behind = at(U, v, 1), at(U, v, -1)
            if v == 0:
                slope = at(U, 3, 1) - at(U, 3, -1)
            else:
                slope = at(FZ, v - 1, 1) - at(FZ, v - 1, -1)

            far, quarter = -0.0625 * f, 0.25 * f
            half = 0.5 * y_flux[v]
            up = quarter + half + pltpu.roll(far, 1, 0)
            down = quarter - half + pltpu.roll(far, CY - 1, 0)
            r = pltpu.roll(up, 1, 0) + pltpu.roll(down, CY - 1, 0)
            half = 0.5 * x_flux[v]
            up = quarter + half + pltpu.roll(far, 1, 1)
            down = quarter - half + pltpu.roll(far, CX - 1, 1)
            r = r + (pltpu.roll(up, 1, 1) + pltpu.roll(down, CX - 1, 1))
            r = r + (0.25 * (ahead + behind) - 0.5 * slope)
            r = r - 0.0625 * (at(U, v, 2) + at(U, v, -2)) - 1.125 * f
            F[v, pl.ds(pl.multiple_of(z * PLANE, PLANE), PLANE), :] = r

    def interior(step, carry):
        for k in range(2):
            residual_plane(range(VARS), 2 + 2 * step + k)
        return carry

    lax.fori_loop(0, (CZ - 4) // 2, interior, 0)

    def build_z(v, carry):
        wide = iota((CZ, 8 * CZ), 1)
        pick = one_hot(iota((CZ, 8 * CZ), 0) == (wide >> 3))
        r, c = iota((16, 8 * CZ), 0), iota((16, 8 * CZ), 1)
        keep, first = (r & 7) == (c & 7), r < 8
        for part, table in enumerate(split(inv_z[v])):
            spread = dot(table, pick)
            for k in range(CZ // 2):
                pair = [jnp.broadcast_to(spread[z : z + 1], (16, 8 * CZ)) for z in (2 * k, 2 * k + 1)]
                block = jnp.where(keep, jnp.where(first, pair[0], pair[1]), 0.0)
                MZ[v, part * 256 + 16 * k : part * 256 + 16 * k + 16, :] = block.astype(BF16)
        return carry

    lax.fori_loop(0, VARS, build_z, 0, unroll=True)
    for copy in halos:
        copy.wait_recv()
    plane_primitives(PLANE)
    plane_primitives(last)
    for side in range(2):
        half = 0.5 - side
        parts = []
        for ref, which in ((YH, side), (YS, side)):
            near, far = pl.ds((1 - side) * CZ, CZ), pl.ds(side * CZ, CZ)
            u = [ref[which, v, near, :] for v in range(VARS)]
            vel, _, pressure = primitives(u)
            parts.append([
                (-0.0625 * u[v], 0.25 * u[v] + half * f - 0.0625 * ref[which, v, far, :])
                for v, f in enumerate(fluxes(u, vel[1], pressure, 1))
            ])
        for v in range(VARS):
            for k in range(2):
                HY[2 * side + k, v] = parts[0][v][k] - parts[1][v][k]
    j = lane & 3
    near = [jnp.where(j < 2, XH[0, v], XH[1, v]) for v in range(VARS)]
    mine = [PK[v] for v in range(VARS)]
    vel, _, pressure = primitives(near)
    near_flux = fluxes(near, vel[0], pressure, 0)
    vel, _, pressure = primitives(mine)
    mine_flux = fluxes(mine, vel[0], pressure, 0)
    for v in range(VARS):
        du, df = near[v] - mine[v], near_flux[v] - mine_flux[v]
        far = -0.0625 * jnp.where(j < 2, pltpu.roll(du, CX - 2, 1), pltpu.roll(du, 2, 1))
        right = pltpu.roll(-0.5 * df + 0.25 * du, CX - 1, 1)
        left = pltpu.roll(0.5 * df + 0.25 * du, 1, 1)
        XC[v] = far + jnp.where(j == 1, right, 0.0) + jnp.where(j == 2, left, 0.0)

    row8 = iota((8, 4 * CX), 0)
    groups = ((0, 1), (2, 3), (4,))
    sums = []
    for t, group in enumerate(groups):

        for z in (0, 1, CZ - 2, CZ - 1):
            residual_plane(group, z)
        for v in group:
            for k, y in ((1, 0), (0, 1), (2, CY - 2), (3, CY - 1)):
                for c in range(CZ // 8):
                    lines = pl.ds(8 * c * PLANE + y, 8, stride=PLANE)
                    F[v, lines, :] = F[v, lines, :] + HY[k, v, 8 * c : 8 * c + 8, :]

        for v in group:
            total = jnp.zeros((CY, CX), F32)
            for z in range(CZ):
                here = slice(z * PLANE, z * PLANE + PLANE)
                r = F[v, here, :] + jnp.where(ends, pltpu.roll(XC[v], (2 * CX - 2 - 4 * z) % CX, 1), 0.0)
                total = total + r * r
                FS[v, here, 0:CX], FS[v, here, CX : 2 * CX] = split(r)
            sums.append(total)
        pair = [jnp.zeros((8, ROWS), F32)] * 2
        for v in group:
            tile = jnp.where(iota((8, CX), 0) < 2, inv_x[v, 0:8, :], pltpu.roll(inv_x[v, CX - 8 : CX, :], 4, 0))
            if v & 1:
                tile = pltpu.roll(tile, 4, 0)
            hi, lo = split(tile)
            left = jnp.concatenate([jnp.concatenate([hi, hi], 1), jnp.concatenate([lo, lo], 1)], 0)
            both = dot_nt(left, FS[v])
            pair[v & 1] = both[0:8] + both[8:16]
        XR[t, ix] = jnp.where(row8 < 4, pair[0], pair[1])
        for d in range(1, px):
            remote(XR.at[t, ix], XR.at[t, ix], xs, xrv.at[t], peer("gx", d)).start()

    stat_row = iota((8, CX), 0)
    tile = jnp.where(stat_row == VARS, jnp.max(top), 0.0)
    for v in range(VARS):
        tile = jnp.where(stat_row == v, jnp.sum(sums[v]), tile)
    STX[ix] = tile
    for d in range(1, px):
        remote(STX.at[ix], STX.at[ix], ss.at[0], sr.at[0], peer("gx", d)).start()

    def combine(ref, n):
        total = ref[0]
        for k in range(1, n):
            total = jnp.where(stat_row == VARS, jnp.maximum(total, ref[k]), total + ref[k])
        return total

    def local_x(v, carry):
        XL[v] = nt2(FS[v], AX[v])
        return carry

    lax.fori_loop(0, VARS, local_x, 0, unroll=True)

    rows = []
    for v in range(VARS):
        near = [RX[v, pl.ds(8 + 4 * ix + at, 1), :] for at in (-2, -1, 4, 5)]
        half = 0.5 * adv[0, v]
        rows += [0.5 * near[0] + (-half - 2.0) * near[1], 0.5 * near[1],
                 0.5 * near[2], (half - 2.0) * near[2] + 0.5 * near[3]]
    rows = jnp.concatenate(rows + [jnp.zeros((4, 4 * px), F32)], axis=0)
    r, c = iota((4 * px, 8 * px), 0), iota((4 * px, 8 * px), 1)
    pick = one_hot(r == ((c >> 3) << 2) + (c & 3))
    hi, lo = split(rows)
    rows = dot(hi, pick) + dot(lo, pick)
    own = ((iota((8, 8 * px), 1) >> 2) & 1) == (iota((8, 8 * px), 0) >> 2)
    for t in range(3):
        LX[t] = jnp.where(own, rows[8 * t : 8 * t + 8], 0.0)

    def build_reduced(axis, n, lines, out):
        shift = log2(lines)
        cols = 4 * n * lines
        pick = one_hot(iota((4 * n, cols), 0) == (iota((4 * n, cols), 1) >> shift))
        pick = jnp.concatenate([pick, pick], axis=0)
        spread = []
        for v in range(VARS):
            near = [RP[axis, v, pl.ds(8 + at, n, stride=4), :] for at in (-2, -1, 4, 5)]
            half = 0.5 * adv[axis + 1, v]
            rows = [0.5 * near[0] + (-half - 2.0) * near[1], 0.5 * near[1],
                    0.5 * near[2], (half - 2.0) * near[2] + 0.5 * near[3]]
            spread.append(dot(jnp.concatenate(split(jnp.concatenate(rows, axis=0)), axis=1), pick))
        which = iota((n, cols), 1) & (lines - 1)
        for v in range(VARS):
            for k in range(4):
                for line in range(lines):
                    block = jnp.where(which == line, spread[v][n * k : n * k + n], 0.0)
                    out[v, pl.ds(k * lines + line, n, stride=4 * lines), :] = block

    build_reduced(0, py, zc, KY)
    build_reduced(1, pz, yc, KZ)

    def build_columns(v, carry):
        SY[v] = columns(inv_y[v], CY)
        SZ[v] = columns(inv_z[v], CZ)
        return carry

    lax.fori_loop(0, VARS, build_columns, 0, unroll=True)

    def exchange(axis, me, n, rows, src, dst, v, send, recv):
        mine = pl.ds(pl.multiple_of(me * rows, rows), rows)
        for d in range(1, n):
            to = peer(axis, d)
            there = pl.ds(pl.multiple_of(to[axis] * rows, rows), rows)
            remote(src.at[v, there], dst.at[v, mine], send, recv, to).start()
        dst[v, mine, :] = src[v, mine, :]

    faces = ((0, 0), (0, 1), (1, 6), (1, 7))

    def local_y(group):
        for v in group:
            XL[v] = XL[v] - nt2(CT[v >> 1], WX[v])
        for v in group:
            for g in range(4):
                solved = mm2(MY[v], XL[v, 128 * g : 128 * g + 128, :])
                for k in range(16):
                    z, h = 8 * g + k // 2, k & 1
                    FG[v, h, 8 * z : 8 * z + 8, :] = solved[8 * k : 8 * k + 8]
        for v in group:
            for h in range(2):
                G[v, h] = mm2(MZ[v], FG[v, h])
        for v in group:
            for h in range(2):
                for k, z in enumerate((0, 1, CZ - 2, CZ - 1)):
                    ZF[v, pl.ds(yc * k + h, 8, stride=zr), :] = G[v, h, 8 * z : 8 * z + 8, :]
            exchange("gz", iz, pz, zr, ZF, ZR1, v, zsem, zr1s.at[v])
        for v in group:
            for k, (h, y) in enumerate(faces):
                for t in range(zc):
                    YF[v, pl.ds(zc * k + t, 8, stride=yr), :] = G[v, h, pl.ds(64 * t + y, 8, stride=8), :]
            exchange("gy", iy, py, yr, YF, YR1, v, ysem, yr1s.at[v])

    for t, group in enumerate(groups):
        drain(XR.at[t, pl.ds(0, px - 1)], xrv.at[t])
        factors = mm3(*split(LX[t]), XR[t].reshape(8 * px, ROWS))
        factors = jnp.concatenate([factors, jnp.zeros((CX - 8, ROWS), F32)], axis=0).T
        CT[t] = jnp.concatenate(split(factors), axis=1)
        local_y(group)
        if t == 1:
            drain(STX.at[pl.ds(0, px - 1)], sr.at[0])
            STY[iy] = combine(STX, px)
            for d in range(1, py):
                remote(STY.at[iy], STY.at[iy], ss.at[1], sr.at[1], peer("gy", d)).start()
    def both_parts(matrix):
        return jnp.concatenate(split(matrix), axis=0)

    def reduced_z(v):
        drain(ZR1.at[v, pl.ds(0, (pz - 1) * zr)], zr1s.at[v])
        Z2[v] = mm2(both_parts(KZ[v]), ZR1[v])
        exchange("gz", iz, pz, zr, Z2, ZR2, v, z2sem, zr2s.at[v])

    def reduced_y(v):
        drain(YR1.at[v, pl.ds(0, (py - 1) * yr)], yr1s.at[v])
        Y2[v] = mm2(both_parts(KY[v]), YR1[v])
        exchange("gy", iy, py, yr, Y2, YR2, v, y2sem, yr2s.at[v])

    reduced_y(0)
    reduced_y(1)
    reduced_z(0)
    reduced_z(1)
    drain(STY.at[pl.ds(0, py - 1)], sr.at[1])
    STZ[iz] = combine(STY, py)
    for d in range(1, pz):
        remote(STZ.at[iz], STZ.at[iz], ss.at[2], sr.at[2], peer("gz", d)).start()
    reduced_y(2)
    reduced_y(3)
    reduced_z(2)
    reduced_z(3)
    reduced_y(4)
    reduced_z(4)

    def correct_z(v, carry):
        drain(ZR2.at[v, pl.ds(0, (pz - 1) * zr)], zr2s.at[v])
        for k, (h, y) in enumerate(faces):
            E[v, 4 * k : 4 * k + 4, :] = ZR2[v, pl.ds(zr * y + h, 4, stride=yc), :]
        mine = pl.ds(pl.multiple_of(16 * iy, 16), 16)
        for d in range(1, py):
            remote(E.at[v], ER.at[v, mine], es, ers.at[v], peer("gy", d)).start()
        ER[v, mine, :] = E[v]
        factor = [[ZR2[v, pl.ds(yc * k + h, 8, stride=zr), :] for h in range(2)] for k in range(4)]
        for z in range(CZ):
            weight = [jnp.broadcast_to(SZ[v, z : z + 1, CX * k : CX * k + CX], (8, CX)) for k in range(4)]
            for h in range(2):
                total = G[v, h, 8 * z : 8 * z + 8, :]
                for k in range(4):
                    total = total - weight[k] * factor[k][h]
                G[v, h, 8 * z : 8 * z + 8, :] = total
        return carry

    lax.fori_loop(0, VARS, correct_z, 0, unroll=True)
    drain(STZ.at[pl.ds(0, pz - 1)], sr.at[2])
    stats = combine(STZ, pz)
    step = 8000.0 / stats[VARS : VARS + 1]
    rms[...] = jnp.sqrt(stats / float(px * py * pz * ROWS * CX))

    def finish(v, carry):
        drain(YR2.at[v, pl.ds(0, (py - 1) * yr)], yr2s.at[v])
        drain(ER.at[v, pl.ds(0, (py - 1) * 16)], ers.at[v])
        cross = mm2(both_parts(KY[v, pl.ds(pl.multiple_of(16 * iy, 16), 16), :]), ER[v])
        for t in range(zc):
            weight = [SZ[v, 8 * t : 8 * t + 8, CX * j : CX * j + CX] for j in range(4)]
            for k in range(4):
                total = YR2[v, pl.ds(zc * k + t, 8, stride=yr), :]
                for j in range(4):
                    total = total - weight[j] * jnp.broadcast_to(cross[4 * k + j : 4 * k + j + 1], (8, CX))
                CF[k, 8 * t : 8 * t + 8, :] = total
        column = [SY[v, :, CX * k : CX * k + CX] * step for k in range(4)]
        for z in range(CZ):
            line = [jnp.broadcast_to(CF[k, z : z + 1, :], (8, CX)) for k in range(4)]
            for h in range(2):
                total = step * G[v, h, 8 * z : 8 * z + 8, :]
                for k in range(4):
                    total = total - column[k][8 * h : 8 * h + 8] * line[k]
                F[v, z * PLANE + 8 * h : z * PLANE + 8 * h + 8, :] = total
        return carry

    lax.fori_loop(0, VARS, finish, 0, unroll=True)
    for copy in halos:
        copy.wait_send()
    drain(XR.at[:, pl.ds(0, px - 1)], xs)
    drain(STX.at[pl.ds(0, px - 1)], ss.at[0])
    drain(STY.at[pl.ds(0, py - 1)], ss.at[1])
    drain(STZ.at[pl.ds(0, pz - 1)], ss.at[2])
    drain(YF.at[:, pl.ds(0, (py - 1) * yr)], ysem)
    drain(Y2.at[:, pl.ds(0, (py - 1) * yr)], y2sem)
    drain(ZF.at[:, pl.ds(0, (pz - 1) * zr)], zsem)
    drain(Z2.at[:, pl.ds(0, (pz - 1) * zr)], z2sem)
    drain(ER.at[:, pl.ds(0, (py - 1) * 16)], es)


def shards(px, py, pz, flow_state, advection, *tables):
    vmem = pl.BlockSpec(memory_space=pltpu.VMEM)
    hbm = pl.BlockSpec(memory_space=pltpu.HBM)
    f32 = lambda *shape: pltpu.VMEM(shape, F32)
    b16 = lambda *shape: pltpu.VMEM(shape, BF16)
    dma = pltpu.SemaphoreType.DMA
    field = (VARS, ROWS, CX)
    padded_rows = ROWS + 4 * PLANE
    y_face, z_face = (VARS, 4 * CZ, CX), (VARS, 4 * CY, CX)
    update, rms = pl.pallas_call(
        functools.partial(kernel, px, py, pz),
        out_shape=(jax.ShapeDtypeStruct(field, F32), jax.ShapeDtypeStruct((8, CX), F32)),
        in_specs=[hbm] * 8,
        out_specs=(vmem, vmem),
        scratch_shapes=[
            pltpu.SMEM(advection.shape, F32), *[f32(*table.shape) for table in tables[:3]], f32(VARS, 4 * px + 16, 4 * px),
            f32(2, VARS, 4 * max(py, pz) + 16, 4 * max(py, pz)),
            f32(VARS, padded_rows, CX), f32(3, padded_rows, CX), f32(4, padded_rows, CX),
            f32(2, VARS, 2 * CZ, CX), f32(2, VARS, 2 * CZ, CX), f32(4, VARS, CZ, CX),
            f32(VARS, CY, CX), f32(2, VARS, CY, CX), f32(VARS, CY, CX),
            b16(VARS, ROWS, 2 * CX), f32(*field), f32(VARS, 2, ROWS // 2, CX), f32(VARS, 2, ROWS // 2, CX),
            f32(3, px, 8, ROWS), b16(3, ROWS, 2 * CX),
            *[f32(*y_face)] * 4, *[f32(*z_face)] * 4,
            f32(VARS, 16, CX), f32(VARS, 16 * py, CX), f32(4, CZ, CX),
            f32(px, 8, CX), f32(py, 8, CX), f32(pz, 8, CX),
            b16(VARS, 2 * CX, 2 * CX), b16(VARS, 2 * CX, 2 * CX), f32(3, 8, 8 * px),
            b16(VARS, 2 * CX, CX), b16(VARS, 512, 256),
            f32(VARS, 4 * CZ, 4 * CZ), f32(VARS, 4 * CY, 4 * CY),
            f32(VARS, CY, 4 * CX), f32(VARS, CZ, 4 * CX),
            dma((8,)), dma((6,)), dma((6,)), dma, dma((3,)),
            *[dma, dma((VARS,))] * 5,
            dma((3,)), dma((3,)),
        ],
        compiler_params=pltpu.CompilerParams(
            collective_id=0, has_side_effects=True, vmem_limit_bytes=32 * 1024 * 1024
        ),
        name="adi_step",
    )(*[pltpu.with_memory_space_constraint(x, pltpu.HBM) for x in (advection, flow_state.reshape(field), *tables)])
    return update.reshape(flow_state.shape), rms[:VARS, 0]


def solution(mesh):
    sizes = [mesh.shape[axis] for axis in ("gx", "gy", "gz")]
    return jax.shard_map(
        functools.partial(shards, *sizes),
        mesh=mesh,
        in_specs=(P(None, "gz", "gy", "gx"), P(), P(), P(), P(), P(), P(), P()),
        out_specs=(P(None, "gz", "gy", "gx"), P()),
        check_vma=False,
    )
```

```python
import functools

import jax
import jax.numpy as jnp
from jax import lax
from jax.experimental import pallas as pl
from jax.experimental.pallas import tpu as pltpu
from jax.sharding import PartitionSpec as P

VARS, CX, CY, CZ = 5, 128, 16, 32
PLANE = CY
ROWS = CZ * CY
F32, BF16 = jnp.float32, jnp.bfloat16
MESH = pl.DeviceIdType.MESH
NT = (((1,), (1,)), ((), ()))


def iota(shape, dim):
    return lax.broadcasted_iota(jnp.int32, shape, dim)


def log2(n):
    return n.bit_length() - 1


def split(x):
    hi = x.astype(BF16)
    return hi, (x - hi.astype(F32)).astype(BF16)


def dot(a, b):
    return jnp.dot(a, b, preferred_element_type=F32)


def dot_nt(a, b):
    return lax.dot_general(a, b, NT, preferred_element_type=F32)


def mm2(left, right):
    wide = dot(left, jnp.concatenate(split(right), axis=1))
    m, n = left.shape[0] // 2, right.shape[1]
    return (wide[:m, :n] + wide[:m, n:]) + wide[m:, :n]


def nt2(left, right):
    wide = dot_nt(left, right)
    n = right.shape[0] // 2
    return wide[:, :n] + wide[:, n:]


def mm3(left_hi, left_lo, right):
    hi, lo = split(right)
    return dot(left_hi, hi) + (dot(left_hi, lo) + dot(left_lo, hi))


def one_hot(cond):
    return jnp.where(cond, 1.0, 0.0).astype(BF16)


def edge(k, length):
    return jnp.where(k < 2, k, k + (length - 4))


def primitives(u):
    scale = 1.0 / u[0]
    vel = [u[1] * scale, u[2] * scale, u[3] * scale]
    kinetic = 0.5 * (vel[0] * vel[0] + vel[1] * vel[1] + vel[2] * vel[2])
    internal = jnp.maximum(u[4] * scale - kinetic, 0.25)
    return vel, internal, 0.4 * u[0] * internal


def fluxes(u, w, pressure, direction):
    out = [u[1 + direction]]
    for c in range(3):
        moment = u[1 + c] * w
        out.append(moment + pressure if c == direction else moment)
    return out + [(u[4] + pressure) * w]


def kernel(
    px, py, pz,
    tab_adv, flow, *refs,
):
    (
        tab_x, tab_y, tab_z, tab_rx, tab_ry, tab_rz,
        F, rms,
        adv, inv_x, inv_y, inv_z, RX, RP,
        U, PR, FZ, YS, YH, HY, PK, XH, XC, FS, XL, G, FG, XR, CT,
        YF, YR1, Y2, YR2, ZF, ZR1, Z2, ZR2, E, ER, CF, STX, STY, STZ,
        AX, WX, LX, MY, MZ, KY, KZ, SY, SZ,
        in_sem, hs, hr, xs, xrv, ysem, yr1s, y2sem, yr2s, zsem, zr1s, z2sem, zr2s, es, ers, ss, sr,
    ) = refs
    ix, iy, iz = lax.axis_index("gx"), lax.axis_index("gy"), lax.axis_index("gz")
    zc, yc = CZ // py, CY // pz
    yr, zr = 4 * zc, 4 * yc

    def peer(axis, d):
        me, n = {"gx": (ix, px), "gy": (iy, py), "gz": (iz, pz)}[axis]
        return {axis: (me + d + n) & (n - 1)}

    def remote(src, dst, send, recv, device):
        return pltpu.make_async_remote_copy(
            src_ref=src, dst_ref=dst, send_sem=send, recv_sem=recv,
            device_id=device, device_id_type=MESH,
        )

    def others(n):
        return sorted(range(1, n), key=lambda d: -min(d, n - d))

    def drain(ref, sem):
        pltpu.make_async_copy(ref, ref, sem).wait()

    load = pltpu.make_async_copy(flow, U.at[:, pl.ds(2 * PLANE, ROWS)], in_sem.at[0])
    load.start()
    tables = [
        pltpu.make_async_copy(src, dst, in_sem.at[1 + k])
        for k, (src, dst) in enumerate(zip(
            (tab_adv, tab_x, tab_y, tab_z, tab_rx, tab_ry, tab_rz),
            (adv, inv_x, inv_y, inv_z, RX.at[:, pl.ds(8, 4 * px)], RP.at[0, :, pl.ds(8, 4 * py)], RP.at[1, :, pl.ds(8, 4 * pz)]),
        ))
    ]
    for copy in tables:
        copy.start()
    for axis, n in enumerate((py, pz)):
        for start in (0, 8 + 4 * n):
            RP[axis, :, start : start + 8, :] = jnp.zeros((VARS, 8, 4 * n), F32)
    for start in (0, 8 + 4 * px):
        RX[:, start : start + 8, :] = jnp.zeros((VARS, 8, 4 * px), F32)
    barrier = pltpu.get_barrier_semaphore()
    for axis, n in (("gz", pz), ("gy", py), ("gx", px)):
        for d in range(1, n):
            pl.semaphore_signal(barrier, inc=1, device_id=peer(axis, d), device_id_type=MESH)
    load.wait()

    def pack_rows(v, carry):
        for r in range(2):
            for t in range(CZ // 8):
                for side, first in ((0, CY - 2), (1, 0)):
                    start = 2 * PLANE + 8 * t * PLANE + first + r
                    YS[side, v, pl.ds(r * CZ + 8 * t, 8), :] = U[v, pl.ds(start, 8, stride=PLANE), :]
        return carry

    lax.fori_loop(0, VARS, pack_rows, 0, unroll=True)
    lane = iota((CY, CX), 1)
    row = iota((CY, CX), 0)

    def pack_lanes(v, carry):
        acc = jnp.zeros((CY, CX), F32)
        for z in range(CZ):
            plane = U[v, pl.ds((2 + z) * PLANE, PLANE), :]
            acc = jnp.where((lane >> 2) == z, pltpu.roll(plane, (4 * z + 2) % CX, 1), acc)
        PK[v] = acc
        return carry

    lax.fori_loop(0, VARS, pack_lanes, 0, unroll=True)

    pl.semaphore_wait(barrier, px + py + pz - 3)
    last = 2 * PLANE + ROWS
    halos = [
        remote(flow.at[:, pl.ds(ROWS - 2 * PLANE, 2 * PLANE)], U.at[:, pl.ds(0, 2 * PLANE)],
               hs.at[0], hr.at[0], peer("gz", 1)),
        remote(flow.at[:, pl.ds(0, 2 * PLANE)], U.at[:, pl.ds(last, 2 * PLANE)],
               hs.at[1], hr.at[1], peer("gz", -1)),
        remote(YS.at[0], YH.at[0], hs.at[2], hr.at[2], peer("gy", 1)),
        remote(YS.at[1], YH.at[1], hs.at[3], hr.at[3], peer("gy", -1)),
        remote(PK, XH.at[0], hs.at[4], hr.at[4], peer("gx", 1)),
        remote(PK, XH.at[1], hs.at[5], hr.at[5], peer("gx", -1)),
    ]
    for copy in halos:
        copy.start()

    def plane_primitives(base):
        here = pl.ds(base, PLANE)
        u = [U[v, here, :] for v in range(VARS)]
        vel, internal, pressure = primitives(u)
        PR[0, here, :], PR[1, here, :], PR[2, here, :] = vel[0], vel[1], pressure
        for k, f in enumerate(fluxes(u, vel[2], pressure, 2)[1:]):
            FZ[k, here, :] = f
        return vel, internal

    top = jnp.zeros((CY, CX), F32)
    for z in range(CZ):
        vel, internal = plane_primitives((2 + z) * PLANE)
        speed = jnp.abs(vel[0]) + jnp.abs(vel[1]) + jnp.abs(vel[2]) + jnp.sqrt(3.0 * 1.4 * 0.4 * internal)
        top = jnp.maximum(top, speed)

    for copy in tables:
        copy.wait()
    def columns(table, length):
        shape = (length, 4 * CX)
        pick = one_hot(iota(shape, 0) == edge(iota(shape, 1) >> 7, length))
        hi, lo = split(table)
        return dot(hi, pick) + dot(lo, pick)

    def build_first(v, carry):
        hi, lo = split(inv_x[v])
        AX[v] = jnp.concatenate([jnp.concatenate([hi, hi], 1), jnp.concatenate([lo, lo], 1)], 0)
        col = iota((CX, CX), 1)
        pick = one_hot(((col >> 2) == (v & 1)) & (iota((CX, CX), 0) == edge(col & 3, CX)))
        hi, lo = dot(hi, pick).astype(BF16), dot(lo, pick).astype(BF16)
        WX[v] = jnp.concatenate([jnp.concatenate([hi, hi], 1), jnp.concatenate([lo, lo], 1)], 0)

        pick = one_hot(iota((CY, CX), 0) == (iota((CY, CX), 1) & (CY - 1)))
        for part, table in enumerate(split(inv_y[v])):
            spread = dot(table, pick)
            for z in range(8):
                block = jnp.where((lane >> 4) == z, spread, 0.0)
                MY[v, part * CX + 16 * z : part * CX + 16 * z + 16, :] = block.astype(BF16)
        return carry

    lax.fori_loop(0, VARS, build_first, 0, unroll=True)
    ends = ((lane + 2) & (CX - 1)) < 4

    def residual_plane(group, z):
        base = pl.multiple_of(2 * PLANE + z * PLANE, PLANE)

        def at(ref, k, step):
            return ref[k, pl.ds(base + step * PLANE, PLANE), :]

        u = [at(U, v, 0) for v in range(VARS)]
        pressure = at(PR, 2, 0)
        x_flux = fluxes(u, at(PR, 0, 0), pressure, 0)
        y_flux = fluxes(u, at(PR, 1, 0), pressure, 1)
        for v in group:
            f = u[v]
            ahead, behind = at(U, v, 1), at(U, v, -1)
            if v == 0:
                slope = at(U, 3, 1) - at(U, 3, -1)
            else:
                slope = at(FZ, v - 1, 1) - at(FZ, v - 1, -1)

            far, quarter = -0.0625 * f, 0.25 * f
            half = 0.5 * y_flux[v]
            up = quarter + half + pltpu.roll(far, 1, 0)
            down = quarter - half + pltpu.roll(far, CY - 1, 0)
            r = pltpu.roll(up, 1, 0) + pltpu.roll(down, CY - 1, 0)
            half = 0.5 * x_flux[v]
            up = quarter + half + pltpu.roll(far, 1, 1)
            down = quarter - half + pltpu.roll(far, CX - 1, 1)
            r = r + (pltpu.roll(up, 1, 1) + pltpu.roll(down, CX - 1, 1))
            r = r + (0.25 * (ahead + behind) - 0.5 * slope)
            r = r - 0.0625 * (at(U, v, 2) + at(U, v, -2)) - 1.125 * f
            F[v, pl.ds(pl.multiple_of(z * PLANE, PLANE), PLANE), :] = r

    def interior(step, carry):
        for k in range(2):
            residual_plane(range(VARS), 2 + 2 * step + k)
        return carry

    lax.fori_loop(0, (CZ - 4) // 2, interior, 0)

    def build_z(v, carry):
        wide = iota((CZ, 8 * CZ), 1)
        pick = one_hot(iota((CZ, 8 * CZ), 0) == (wide >> 3))
        r, c = iota((16, 8 * CZ), 0), iota((16, 8 * CZ), 1)
        keep, first = (r & 7) == (c & 7), r < 8
        for part, table in enumerate(split(inv_z[v])):
            spread = dot(table, pick)
            for k in range(CZ // 2):
                pair = [jnp.broadcast_to(spread[z : z + 1], (16, 8 * CZ)) for z in (2 * k, 2 * k + 1)]
                block = jnp.where(keep, jnp.where(first, pair[0], pair[1]), 0.0)
                MZ[v, part * 256 + 16 * k : part * 256 + 16 * k + 16, :] = block.astype(BF16)
        return carry

    lax.fori_loop(0, VARS, build_z, 0, unroll=True)
    for copy in halos:
        copy.wait_recv()
    plane_primitives(PLANE)
    plane_primitives(last)
    for side in range(2):
        half = 0.5 - side
        parts = []
        for ref, which in ((YH, side), (YS, side)):
            near, far = pl.ds((1 - side) * CZ, CZ), pl.ds(side * CZ, CZ)
            u = [ref[which, v, near, :] for v in range(VARS)]
            vel, _, pressure = primitives(u)
            parts.append([
                (-0.0625 * u[v], 0.25 * u[v] + half * f - 0.0625 * ref[which, v, far, :])
                for v, f in enumerate(fluxes(u, vel[1], pressure, 1))
            ])
        for v in range(VARS):
            for k in range(2):
                HY[2 * side + k, v] = parts[0][v][k] - parts[1][v][k]
    j = lane & 3
    near = [jnp.where(j < 2, XH[0, v], XH[1, v]) for v in range(VARS)]
    mine = [PK[v] for v in range(VARS)]
    vel, _, pressure = primitives(near)
    near_flux = fluxes(near, vel[0], pressure, 0)
    vel, _, pressure = primitives(mine)
    mine_flux = fluxes(mine, vel[0], pressure, 0)
    for v in range(VARS):
        du, df = near[v] - mine[v], near_flux[v] - mine_flux[v]
        far = -0.0625 * jnp.where(j < 2, pltpu.roll(du, CX - 2, 1), pltpu.roll(du, 2, 1))
        right = pltpu.roll(-0.5 * df + 0.25 * du, CX - 1, 1)
        left = pltpu.roll(0.5 * df + 0.25 * du, 1, 1)
        XC[v] = far + jnp.where(j == 1, right, 0.0) + jnp.where(j == 2, left, 0.0)

    row8 = iota((8, 4 * CX), 0)
    groups = ((0, 1), (2, 3), (4,))
    sums = []
    for t, group in enumerate(groups):

        for z in (0, 1, CZ - 2, CZ - 1):
            residual_plane(group, z)
        for v in group:
            for k, y in ((1, 0), (0, 1), (2, CY - 2), (3, CY - 1)):
                for c in range(CZ // 8):
                    lines = pl.ds(8 * c * PLANE + y, 8, stride=PLANE)
                    F[v, lines, :] = F[v, lines, :] + HY[k, v, 8 * c : 8 * c + 8, :]

        for v in group:
            total = jnp.zeros((CY, CX), F32)
            for z in range(CZ):
                here = slice(z * PLANE, z * PLANE + PLANE)
                r = F[v, here, :] + jnp.where(ends, pltpu.roll(XC[v], (2 * CX - 2 - 4 * z) % CX, 1), 0.0)
                total = total + r * r
                FS[v, here, 0:CX], FS[v, here, CX : 2 * CX] = split(r)
            sums.append(total)
        pair = [jnp.zeros((8, ROWS), F32)] * 2
        for v in group:
            tile = jnp.where(iota((8, CX), 0) < 2, inv_x[v, 0:8, :], pltpu.roll(inv_x[v, CX - 8 : CX, :], 4, 0))
            if v & 1:
                tile = pltpu.roll(tile, 4, 0)
            hi, lo = split(tile)
            left = jnp.concatenate([jnp.concatenate([hi, hi], 1), jnp.concatenate([lo, lo], 1)], 0)
            both = dot_nt(left, FS[v])
            pair[v & 1] = both[0:8] + both[8:16]
        XR[t, ix] = jnp.where(row8 < 4, pair[0], pair[1])
        for d in others(px):
            remote(XR.at[t, ix], XR.at[t, ix], xs, xrv.at[t], peer("gx", d)).start()

    stat_row = iota((8, CX), 0)
    tile = jnp.where(stat_row == VARS, jnp.max(top), 0.0)
    for v in range(VARS):
        tile = jnp.where(stat_row == v, jnp.sum(sums[v]), tile)
    STX[ix] = tile
    for d in others(px):
        remote(STX.at[ix], STX.at[ix], ss.at[0], sr.at[0], peer("gx", d)).start()

    def combine(ref, n):
        total = ref[0]
        for k in range(1, n):
            total = jnp.where(stat_row == VARS, jnp.maximum(total, ref[k]), total + ref[k])
        return total

    def local_x(v, carry):
        XL[v] = nt2(FS[v], AX[v])
        return carry

    lax.fori_loop(0, VARS, local_x, 0, unroll=True)

    rows = []
    for v in range(VARS):
        near = [RX[v, pl.ds(8 + 4 * ix + at, 1), :] for at in (-2, -1, 4, 5)]
        half = 0.5 * adv[0, v]
        rows += [0.5 * near[0] + (-half - 2.0) * near[1], 0.5 * near[1],
                 0.5 * near[2], (half - 2.0) * near[2] + 0.5 * near[3]]
    rows = jnp.concatenate(rows + [jnp.zeros((4, 4 * px), F32)], axis=0)
    r, c = iota((4 * px, 8 * px), 0), iota((4 * px, 8 * px), 1)
    pick = one_hot(r == ((c >> 3) << 2) + (c & 3))
    hi, lo = split(rows)
    rows = dot(hi, pick) + dot(lo, pick)
    own = ((iota((8, 8 * px), 1) >> 2) & 1) == (iota((8, 8 * px), 0) >> 2)
    for t in range(3):
        LX[t] = jnp.where(own, rows[8 * t : 8 * t + 8], 0.0)

    def build_reduced(axis, n, lines, out):
        shift = log2(lines)
        cols = 4 * n * lines
        pick = one_hot(iota((4 * n, cols), 0) == (iota((4 * n, cols), 1) >> shift))
        pick = jnp.concatenate([pick, pick], axis=0)
        spread = []
        for v in range(VARS):
            near = [RP[axis, v, pl.ds(8 + at, n, stride=4), :] for at in (-2, -1, 4, 5)]
            half = 0.5 * adv[axis + 1, v]
            rows = [0.5 * near[0] + (-half - 2.0) * near[1], 0.5 * near[1],
                    0.5 * near[2], (half - 2.0) * near[2] + 0.5 * near[3]]
            spread.append(dot(jnp.concatenate(split(jnp.concatenate(rows, axis=0)), axis=1), pick))
        which = iota((n, cols), 1) & (lines - 1)
        for v in range(VARS):
            for k in range(4):
                for line in range(lines):
                    block = jnp.where(which == line, spread[v][n * k : n * k + n], 0.0)
                    out[v, pl.ds(k * lines + line, n, stride=4 * lines), :] = block

    build_reduced(0, py, zc, KY)
    build_reduced(1, pz, yc, KZ)

    def build_columns(v, carry):
        SY[v] = columns(inv_y[v], CY)
        SZ[v] = columns(inv_z[v], CZ)
        return carry

    lax.fori_loop(0, VARS, build_columns, 0, unroll=True)

    def exchange(axis, me, n, rows, src, dst, v, send, recv):
        mine = pl.ds(pl.multiple_of(me * rows, rows), rows)
        for d in others(n):
            to = peer(axis, d)
            there = pl.ds(pl.multiple_of(to[axis] * rows, rows), rows)
            remote(src.at[v, there], dst.at[v, mine], send, recv, to).start()
        dst[v, mine, :] = src[v, mine, :]

    faces = ((0, 0), (0, 1), (1, 6), (1, 7))

    def local_y(group):
        for v in group:
            XL[v] = XL[v] - nt2(CT[v >> 1], WX[v])
        for v in group:
            for g in range(4):
                solved = mm2(MY[v], XL[v, 128 * g : 128 * g + 128, :])
                for k in range(16):
                    z, h = 8 * g + k // 2, k & 1
                    FG[v, h, 8 * z : 8 * z + 8, :] = solved[8 * k : 8 * k + 8]
        for v in group:
            for h in range(2):
                G[v, h] = mm2(MZ[v], FG[v, h])
        for v in group:
            for h in range(2):
                for k, z in enumerate((0, 1, CZ - 2, CZ - 1)):
                    ZF[v, pl.ds(yc * k + h, 8, stride=zr), :] = G[v, h, 8 * z : 8 * z + 8, :]
            exchange("gz", iz, pz, zr, ZF, ZR1, v, zsem, zr1s.at[v])
        for v in group:
            for k, (h, y) in enumerate(faces):
                for t in range(zc):
                    YF[v, pl.ds(zc * k + t, 8, stride=yr), :] = G[v, h, pl.ds(64 * t + y, 8, stride=8), :]
            exchange("gy", iy, py, yr, YF, YR1, v, ysem, yr1s.at[v])

    for t, group in enumerate(groups):
        drain(XR.at[t, pl.ds(0, px - 1)], xrv.at[t])
        factors = mm3(*split(LX[t]), XR[t].reshape(8 * px, ROWS))
        factors = jnp.concatenate([factors, jnp.zeros((CX - 8, ROWS), F32)], axis=0).T
        CT[t] = jnp.concatenate(split(factors), axis=1)
        local_y(group)
        if t == 1:
            drain(STX.at[pl.ds(0, px - 1)], sr.at[0])
            STY[iy] = combine(STX, px)
            for d in others(py):
                remote(STY.at[iy], STY.at[iy], ss.at[1], sr.at[1], peer("gy", d)).start()
    def both_parts(matrix):
        return jnp.concatenate(split(matrix), axis=0)

    def reduced_z(v):
        drain(ZR1.at[v, pl.ds(0, (pz - 1) * zr)], zr1s.at[v])
        Z2[v] = mm2(both_parts(KZ[v]), ZR1[v])
        exchange("gz", iz, pz, zr, Z2, ZR2, v, z2sem, zr2s.at[v])

    def reduced_y(v):
        drain(YR1.at[v, pl.ds(0, (py - 1) * yr)], yr1s.at[v])
        Y2[v] = mm2(both_parts(KY[v]), YR1[v])
        exchange("gy", iy, py, yr, Y2, YR2, v, y2sem, yr2s.at[v])

    for v in range(VARS):
        reduced_z(v)
        reduced_y(v)
    drain(STY.at[pl.ds(0, py - 1)], sr.at[1])
    STZ[iz] = combine(STY, py)
    for d in others(pz):
        remote(STZ.at[iz], STZ.at[iz], ss.at[2], sr.at[2], peer("gz", d)).start()

    def correct_z(v, carry):
        drain(ZR2.at[v, pl.ds(0, (pz - 1) * zr)], zr2s.at[v])
        for k, (h, y) in enumerate(faces):
            E[v, 4 * k : 4 * k + 4, :] = ZR2[v, pl.ds(zr * y + h, 4, stride=yc), :]
        mine = pl.ds(pl.multiple_of(16 * iy, 16), 16)
        for d in others(py):
            remote(E.at[v], ER.at[v, mine], es, ers.at[v], peer("gy", d)).start()
        ER[v, mine, :] = E[v]
        factor = [[ZR2[v, pl.ds(yc * k + h, 8, stride=zr), :] for h in range(2)] for k in range(4)]
        for z in range(CZ):
            weight = [jnp.broadcast_to(SZ[v, z : z + 1, CX * k : CX * k + CX], (8, CX)) for k in range(4)]
            for h in range(2):
                total = G[v, h, 8 * z : 8 * z + 8, :]
                for k in range(4):
                    total = total - weight[k] * factor[k][h]
                G[v, h, 8 * z : 8 * z + 8, :] = total
        return carry

    lax.fori_loop(0, VARS, correct_z, 0, unroll=True)
    drain(STZ.at[pl.ds(0, pz - 1)], sr.at[2])
    stats = combine(STZ, pz)
    step = 8000.0 / stats[VARS : VARS + 1]
    rms[...] = jnp.sqrt(stats / float(px * py * pz * ROWS * CX))

    def finish(v, carry):
        drain(YR2.at[v, pl.ds(0, (py - 1) * yr)], yr2s.at[v])
        drain(ER.at[v, pl.ds(0, (py - 1) * 16)], ers.at[v])
        cross = mm2(both_parts(KY[v, pl.ds(pl.multiple_of(16 * iy, 16), 16), :]), ER[v])
        for t in range(zc):
            weight = [SZ[v, 8 * t : 8 * t + 8, CX * j : CX * j + CX] for j in range(4)]
            for k in range(4):
                total = YR2[v, pl.ds(zc * k + t, 8, stride=yr), :]
                for j in range(4):
                    total = total - weight[j] * jnp.broadcast_to(cross[4 * k + j : 4 * k + j + 1], (8, CX))
                CF[k, 8 * t : 8 * t + 8, :] = total
        column = [SY[v, :, CX * k : CX * k + CX] * step for k in range(4)]
        for z in range(CZ):
            line = [jnp.broadcast_to(CF[k, z : z + 1, :], (8, CX)) for k in range(4)]
            for h in range(2):
                total = step * G[v, h, 8 * z : 8 * z + 8, :]
                for k in range(4):
                    total = total - column[k][8 * h : 8 * h + 8] * line[k]
                F[v, z * PLANE + 8 * h : z * PLANE + 8 * h + 8, :] = total
        return carry

    lax.fori_loop(0, VARS, finish, 0, unroll=True)
    for copy in halos:
        copy.wait_send()
    drain(XR.at[:, pl.ds(0, px - 1)], xs)
    drain(STX.at[pl.ds(0, px - 1)], ss.at[0])
    drain(STY.at[pl.ds(0, py - 1)], ss.at[1])
    drain(STZ.at[pl.ds(0, pz - 1)], ss.at[2])
    drain(YF.at[:, pl.ds(0, (py - 1) * yr)], ysem)
    drain(Y2.at[:, pl.ds(0, (py - 1) * yr)], y2sem)
    drain(ZF.at[:, pl.ds(0, (pz - 1) * zr)], zsem)
    drain(Z2.at[:, pl.ds(0, (pz - 1) * zr)], z2sem)
    drain(ER.at[:, pl.ds(0, (py - 1) * 16)], es)


def shards(px, py, pz, flow_state, advection, *tables):
    vmem = pl.BlockSpec(memory_space=pltpu.VMEM)
    hbm = pl.BlockSpec(memory_space=pltpu.HBM)
    f32 = lambda *shape: pltpu.VMEM(shape, F32)
    b16 = lambda *shape: pltpu.VMEM(shape, BF16)
    dma = pltpu.SemaphoreType.DMA
    field = (VARS, ROWS, CX)
    padded_rows = ROWS + 4 * PLANE
    y_face, z_face = (VARS, 4 * CZ, CX), (VARS, 4 * CY, CX)
    update, rms = pl.pallas_call(
        functools.partial(kernel, px, py, pz),
        out_shape=(jax.ShapeDtypeStruct(field, F32), jax.ShapeDtypeStruct((8, CX), F32)),
        in_specs=[hbm] * 8,
        out_specs=(vmem, vmem),
        scratch_shapes=[
            pltpu.SMEM(advection.shape, F32), *[f32(*table.shape) for table in tables[:3]], f32(VARS, 4 * px + 16, 4 * px),
            f32(2, VARS, 4 * max(py, pz) + 16, 4 * max(py, pz)),
            f32(VARS, padded_rows, CX), f32(3, padded_rows, CX), f32(4, padded_rows, CX),
            f32(2, VARS, 2 * CZ, CX), f32(2, VARS, 2 * CZ, CX), f32(4, VARS, CZ, CX),
            f32(VARS, CY, CX), f32(2, VARS, CY, CX), f32(VARS, CY, CX),
            b16(VARS, ROWS, 2 * CX), f32(*field), f32(VARS, 2, ROWS // 2, CX), f32(VARS, 2, ROWS // 2, CX),
            f32(3, px, 8, ROWS), b16(3, ROWS, 2 * CX),
            *[f32(*y_face)] * 4, *[f32(*z_face)] * 4,
            f32(VARS, 16, CX), f32(VARS, 16 * py, CX), f32(4, CZ, CX),
            f32(px, 8, CX), f32(py, 8, CX), f32(pz, 8, CX),
            b16(VARS, 2 * CX, 2 * CX), b16(VARS, 2 * CX, 2 * CX), f32(3, 8, 8 * px),
            b16(VARS, 2 * CX, CX), b16(VARS, 512, 256),
            f32(VARS, 4 * CZ, 4 * CZ), f32(VARS, 4 * CY, 4 * CY),
            f32(VARS, CY, 4 * CX), f32(VARS, CZ, 4 * CX),
            dma((8,)), dma((6,)), dma((6,)), dma, dma((3,)),
            *[dma, dma((VARS,))] * 5,
            dma((3,)), dma((3,)),
        ],
        compiler_params=pltpu.CompilerParams(
            collective_id=0, has_side_effects=True, vmem_limit_bytes=32 * 1024 * 1024
        ),
        name="adi_step",
    )(*[pltpu.with_memory_space_constraint(x, pltpu.HBM) for x in (advection, flow_state.reshape(field), *tables)])
    return update.reshape(flow_state.shape), rms[:VARS, 0]


def solution(mesh):
    sizes = [mesh.shape[axis] for axis in ("gx", "gy", "gz")]
    return jax.shard_map(
        functools.partial(shards, *sizes),
        mesh=mesh,
        in_specs=(P(None, "gz", "gy", "gx"), P(), P(), P(), P(), P(), P(), P()),
        out_specs=(P(None, "gz", "gy", "gx"), P()),
        check_vma=False,
    )
```

```python
import functools

import jax
import jax.numpy as jnp
from jax import lax
from jax.experimental import pallas as pl
from jax.experimental.pallas import tpu as pltpu
from jax.sharding import PartitionSpec as P

VARS, CX, CY, CZ = 5, 128, 16, 32
PLANE = CY
ROWS = CZ * CY
F32, BF16 = jnp.float32, jnp.bfloat16
MESH = pl.DeviceIdType.MESH
NT = (((1,), (1,)), ((), ()))


def iota(shape, dim):
    return lax.broadcasted_iota(jnp.int32, shape, dim)


def log2(n):
    return n.bit_length() - 1


def split(x):
    hi = x.astype(BF16)
    return hi, (x - hi.astype(F32)).astype(BF16)


def dot(a, b):
    return jnp.dot(a, b, preferred_element_type=F32)


def dot_nt(a, b):
    return lax.dot_general(a, b, NT, preferred_element_type=F32)


def mm2(left, right):
    wide = dot(left, jnp.concatenate(split(right), axis=1))
    m, n = left.shape[0] // 2, right.shape[1]
    return (wide[:m, :n] + wide[:m, n:]) + wide[m:, :n]


def nt2(left, right):
    wide = dot_nt(left, right)
    n = right.shape[0] // 2
    return wide[:, :n] + wide[:, n:]


def mm3(left_hi, left_lo, right):
    hi, lo = split(right)
    return dot(left_hi, hi) + (dot(left_hi, lo) + dot(left_lo, hi))


def one_hot(cond):
    return jnp.where(cond, 1.0, 0.0).astype(BF16)


def edge(k, length):
    return jnp.where(k < 2, k, k + (length - 4))


def primitives(u):
    scale = 1.0 / u[0]
    vel = [u[1] * scale, u[2] * scale, u[3] * scale]
    kinetic = 0.5 * (vel[0] * vel[0] + vel[1] * vel[1] + vel[2] * vel[2])
    internal = jnp.maximum(u[4] * scale - kinetic, 0.25)
    return vel, internal, 0.4 * u[0] * internal


def fluxes(u, w, pressure, direction):
    out = [u[1 + direction]]
    for c in range(3):
        moment = u[1 + c] * w
        out.append(moment + pressure if c == direction else moment)
    return out + [(u[4] + pressure) * w]


def kernel(
    px, py, pz,
    tab_adv, flow, *refs,
):
    (
        tab_x, tab_y, tab_z, tab_rx, tab_ry, tab_rz,
        F, rms,
        adv, inv_x, inv_y, inv_z, RX, RP,
        U, PR, FZ, YS, YH, HY, PK, XH, XC, FS, XL, G, FG, XR, CT,
        YF, YR1, Y2, YR2, ZF, ZR1, Z2, ZR2, E, ER, CF, STX, STY, STZ,
        AX, WX, LX, MY, MZ, KY, KZ, SY, SZ,
        in_sem, hs, hr, xs, xrv, ysem, yr1s, y2sem, yr2s, zsem, zr1s, z2sem, zr2s, es, ers, ss, sr, known,
    ) = refs
    ix, iy, iz = lax.axis_index("gx"), lax.axis_index("gy"), lax.axis_index("gz")
    zc, yc = CZ // py, CY // pz
    yr, zr = 4 * zc, 4 * yc

    def peer(axis, d):
        me, n = {"gx": (ix, px), "gy": (iy, py), "gz": (iz, pz)}[axis]
        return {axis: (me + d + n) & (n - 1)}

    def remote(src, dst, send, recv, device):
        return pltpu.make_async_remote_copy(
            src_ref=src, dst_ref=dst, send_sem=send, recv_sem=recv,
            device_id=device, device_id_type=MESH,
        )

    def others(n):
        return sorted(range(1, n), key=lambda d: -min(d, n - d))

    def drain(ref, sem):
        pltpu.make_async_copy(ref, ref, sem).wait()

    load = pltpu.make_async_copy(flow, U.at[:, pl.ds(2 * PLANE, ROWS)], in_sem.at[0])
    load.start()
    tables = [
        pltpu.make_async_copy(src, dst, in_sem.at[1 + k])
        for k, (src, dst) in enumerate(zip(
            (tab_adv, tab_x, tab_y, tab_z, tab_rx, tab_ry, tab_rz),
            (adv, inv_x, inv_y, inv_z, RX.at[:, pl.ds(8, 4 * px)], RP.at[0, :, pl.ds(8, 4 * py)], RP.at[1, :, pl.ds(8, 4 * pz)]),
        ))
    ]
    for copy in tables:
        copy.start()
    for axis, n in enumerate((py, pz)):
        for start in (0, 8 + 4 * n):
            RP[axis, :, start : start + 8, :] = jnp.zeros((VARS, 8, 4 * n), F32)
    for start in (0, 8 + 4 * px):
        RX[:, start : start + 8, :] = jnp.zeros((VARS, 8, 4 * px), F32)
    barrier = pltpu.get_barrier_semaphore()
    axes = (("gz", pz), ("gy", py), ("gx", px))
    for axis, _ in axes:
        for d in (1, -1):
            pl.semaphore_signal(barrier, inc=1, device_id=peer(axis, d), device_id_type=MESH)

    def spread(turn):
        for a, (axis, n) in enumerate(axes):
            if turn < n // 2:
                for d in (1, -1):
                    pl.semaphore_signal(known.at[a, turn - 1], inc=1, device_id=peer(axis, d), device_id_type=MESH)

    def heard(turn):
        for a, (axis, n) in enumerate(axes):
            if turn < n // 2:
                pl.semaphore_wait(known.at[a, turn - 1], 2)

    load.wait()

    def pack_rows(v, carry):
        for r in range(2):
            for t in range(CZ // 8):
                for side, first in ((0, CY - 2), (1, 0)):
                    start = 2 * PLANE + 8 * t * PLANE + first + r
                    YS[side, v, pl.ds(r * CZ + 8 * t, 8), :] = U[v, pl.ds(start, 8, stride=PLANE), :]
        return carry

    lax.fori_loop(0, VARS, pack_rows, 0, unroll=True)
    lane = iota((CY, CX), 1)
    row = iota((CY, CX), 0)

    def pack_lanes(v, carry):
        acc = jnp.zeros((CY, CX), F32)
        for z in range(CZ):
            plane = U[v, pl.ds((2 + z) * PLANE, PLANE), :]
            acc = jnp.where((lane >> 2) == z, pltpu.roll(plane, (4 * z + 2) % CX, 1), acc)
        PK[v] = acc
        return carry

    lax.fori_loop(0, VARS, pack_lanes, 0, unroll=True)

    pl.semaphore_wait(barrier, 6)
    spread(1)
    last = 2 * PLANE + ROWS
    halos = [
        remote(flow.at[:, pl.ds(ROWS - 2 * PLANE, 2 * PLANE)], U.at[:, pl.ds(0, 2 * PLANE)],
               hs.at[0], hr.at[0], peer("gz", 1)),
        remote(flow.at[:, pl.ds(0, 2 * PLANE)], U.at[:, pl.ds(last, 2 * PLANE)],
               hs.at[1], hr.at[1], peer("gz", -1)),
        remote(YS.at[0], YH.at[0], hs.at[2], hr.at[2], peer("gy", 1)),
        remote(YS.at[1], YH.at[1], hs.at[3], hr.at[3], peer("gy", -1)),
        remote(PK, XH.at[0], hs.at[4], hr.at[4], peer("gx", 1)),
        remote(PK, XH.at[1], hs.at[5], hr.at[5], peer("gx", -1)),
    ]
    for copy in halos:
        copy.start()

    def plane_primitives(base):
        here = pl.ds(base, PLANE)
        u = [U[v, here, :] for v in range(VARS)]
        vel, internal, pressure = primitives(u)
        PR[0, here, :], PR[1, here, :], PR[2, here, :] = vel[0], vel[1], pressure
        for k, f in enumerate(fluxes(u, vel[2], pressure, 2)[1:]):
            FZ[k, here, :] = f
        return vel, internal

    top = jnp.zeros((CY, CX), F32)
    for z in range(CZ):
        vel, internal = plane_primitives((2 + z) * PLANE)
        speed = jnp.abs(vel[0]) + jnp.abs(vel[1]) + jnp.abs(vel[2]) + jnp.sqrt(3.0 * 1.4 * 0.4 * internal)
        top = jnp.maximum(top, speed)

    for copy in tables:
        copy.wait()
    def columns(table, length):
        shape = (length, 4 * CX)
        pick = one_hot(iota(shape, 0) == edge(iota(shape, 1) >> 7, length))
        hi, lo = split(table)
        return dot(hi, pick) + dot(lo, pick)

    def build_first(v, carry):
        hi, lo = split(inv_x[v])
        AX[v] = jnp.concatenate([jnp.concatenate([hi, hi], 1), jnp.concatenate([lo, lo], 1)], 0)
        col = iota((CX, CX), 1)
        pick = one_hot(((col >> 2) == (v & 1)) & (iota((CX, CX), 0) == edge(col & 3, CX)))
        hi, lo = dot(hi, pick).astype(BF16), dot(lo, pick).astype(BF16)
        WX[v] = jnp.concatenate([jnp.concatenate([hi, hi], 1), jnp.concatenate([lo, lo], 1)], 0)

        pick = one_hot(iota((CY, CX), 0) == (iota((CY, CX), 1) & (CY - 1)))
        for part, table in enumerate(split(inv_y[v])):
            spread = dot(table, pick)
            for z in range(8):
                block = jnp.where((lane >> 4) == z, spread, 0.0)
                MY[v, part * CX + 16 * z : part * CX + 16 * z + 16, :] = block.astype(BF16)
        return carry

    lax.fori_loop(0, VARS, build_first, 0, unroll=True)
    ends = ((lane + 2) & (CX - 1)) < 4

    def residual_plane(group, z):
        base = pl.multiple_of(2 * PLANE + z * PLANE, PLANE)

        def at(ref, k, step):
            return ref[k, pl.ds(base + step * PLANE, PLANE), :]

        u = [at(U, v, 0) for v in range(VARS)]
        pressure = at(PR, 2, 0)
        x_flux = fluxes(u, at(PR, 0, 0), pressure, 0)
        y_flux = fluxes(u, at(PR, 1, 0), pressure, 1)
        for v in group:
            f = u[v]
            ahead, behind = at(U, v, 1), at(U, v, -1)
            if v == 0:
                slope = at(U, 3, 1) - at(U, 3, -1)
            else:
                slope = at(FZ, v - 1, 1) - at(FZ, v - 1, -1)

            far, quarter = -0.0625 * f, 0.25 * f
            half = 0.5 * y_flux[v]
            up = quarter + half + pltpu.roll(far, 1, 0)
            down = quarter - half + pltpu.roll(far, CY - 1, 0)
            r = pltpu.roll(up, 1, 0) + pltpu.roll(down, CY - 1, 0)
            half = 0.5 * x_flux[v]
            up = quarter + half + pltpu.roll(far, 1, 1)
            down = quarter - half + pltpu.roll(far, CX - 1, 1)
            r = r + (pltpu.roll(up, 1, 1) + pltpu.roll(down, CX - 1, 1))
            r = r + (0.25 * (ahead + behind) - 0.5 * slope)
            r = r - 0.0625 * (at(U, v, 2) + at(U, v, -2)) - 1.125 * f
            F[v, pl.ds(pl.multiple_of(z * PLANE, PLANE), PLANE), :] = r

    def interior(step, carry):
        for k in range(2):
            residual_plane(range(VARS), 2 + 2 * step + k)
        return carry

    lax.fori_loop(0, (CZ - 4) // 2, interior, 0)

    def build_z(v, carry):
        wide = iota((CZ, 8 * CZ), 1)
        pick = one_hot(iota((CZ, 8 * CZ), 0) == (wide >> 3))
        r, c = iota((16, 8 * CZ), 0), iota((16, 8 * CZ), 1)
        keep, first = (r & 7) == (c & 7), r < 8
        for part, table in enumerate(split(inv_z[v])):
            spread = dot(table, pick)
            for k in range(CZ // 2):
                pair = [jnp.broadcast_to(spread[z : z + 1], (16, 8 * CZ)) for z in (2 * k, 2 * k + 1)]
                block = jnp.where(keep, jnp.where(first, pair[0], pair[1]), 0.0)
                MZ[v, part * 256 + 16 * k : part * 256 + 16 * k + 16, :] = block.astype(BF16)
        return carry

    lax.fori_loop(0, VARS, build_z, 0, unroll=True)
    heard(1)
    spread(2)
    for copy in halos:
        copy.wait_recv()
    plane_primitives(PLANE)
    plane_primitives(last)
    for side in range(2):
        half = 0.5 - side
        parts = []
        for ref, which in ((YH, side), (YS, side)):
            near, far = pl.ds((1 - side) * CZ, CZ), pl.ds(side * CZ, CZ)
            u = [ref[which, v, near, :] for v in range(VARS)]
            vel, _, pressure = primitives(u)
            parts.append([
                (-0.0625 * u[v], 0.25 * u[v] + half * f - 0.0625 * ref[which, v, far, :])
                for v, f in enumerate(fluxes(u, vel[1], pressure, 1))
            ])
        for v in range(VARS):
            for k in range(2):
                HY[2 * side + k, v] = parts[0][v][k] - parts[1][v][k]
    j = lane & 3
    near = [jnp.where(j < 2, XH[0, v], XH[1, v]) for v in range(VARS)]
    mine = [PK[v] for v in range(VARS)]
    vel, _, pressure = primitives(near)
    near_flux = fluxes(near, vel[0], pressure, 0)
    vel, _, pressure = primitives(mine)
    mine_flux = fluxes(mine, vel[0], pressure, 0)
    for v in range(VARS):
        du, df = near[v] - mine[v], near_flux[v] - mine_flux[v]
        far = -0.0625 * jnp.where(j < 2, pltpu.roll(du, CX - 2, 1), pltpu.roll(du, 2, 1))
        right = pltpu.roll(-0.5 * df + 0.25 * du, CX - 1, 1)
        left = pltpu.roll(0.5 * df + 0.25 * du, 1, 1)
        XC[v] = far + jnp.where(j == 1, right, 0.0) + jnp.where(j == 2, left, 0.0)

    row8 = iota((8, 4 * CX), 0)
    groups = ((0, 1), (2, 3), (4,))
    sums = []
    for t, group in enumerate(groups):

        for z in (0, 1, CZ - 2, CZ - 1):
            residual_plane(group, z)
        for v in group:
            for k, y in ((1, 0), (0, 1), (2, CY - 2), (3, CY - 1)):
                for c in range(CZ // 8):
                    lines = pl.ds(8 * c * PLANE + y, 8, stride=PLANE)
                    F[v, lines, :] = F[v, lines, :] + HY[k, v, 8 * c : 8 * c + 8, :]

        for v in group:
            total = jnp.zeros((CY, CX), F32)
            for z in range(CZ):
                here = slice(z * PLANE, z * PLANE + PLANE)
                r = F[v, here, :] + jnp.where(ends, pltpu.roll(XC[v], (2 * CX - 2 - 4 * z) % CX, 1), 0.0)
                total = total + r * r
                FS[v, here, 0:CX], FS[v, here, CX : 2 * CX] = split(r)
            sums.append(total)
        pair = [jnp.zeros((8, ROWS), F32)] * 2
        for v in group:
            tile = jnp.where(iota((8, CX), 0) < 2, inv_x[v, 0:8, :], pltpu.roll(inv_x[v, CX - 8 : CX, :], 4, 0))
            if v & 1:
                tile = pltpu.roll(tile, 4, 0)
            hi, lo = split(tile)
            left = jnp.concatenate([jnp.concatenate([hi, hi], 1), jnp.concatenate([lo, lo], 1)], 0)
            both = dot_nt(left, FS[v])
            pair[v & 1] = both[0:8] + both[8:16]
        XR[t, ix] = jnp.where(row8 < 4, pair[0], pair[1])
        for d in others(px):
            remote(XR.at[t, ix], XR.at[t, ix], xs, xrv.at[t], peer("gx", d)).start()

    heard(2)
    spread(3)
    stat_row = iota((8, CX), 0)
    tile = jnp.where(stat_row == VARS, jnp.max(top), 0.0)
    for v in range(VARS):
        tile = jnp.where(stat_row == v, jnp.sum(sums[v]), tile)
    STX[ix] = tile
    for d in others(px):
        remote(STX.at[ix], STX.at[ix], ss.at[0], sr.at[0], peer("gx", d)).start()

    def combine(ref, n):
        total = ref[0]
        for k in range(1, n):
            total = jnp.where(stat_row == VARS, jnp.maximum(total, ref[k]), total + ref[k])
        return total

    def local_x(v, carry):
        XL[v] = nt2(FS[v], AX[v])
        return carry

    lax.fori_loop(0, VARS, local_x, 0, unroll=True)

    rows = []
    for v in range(VARS):
        near = [RX[v, pl.ds(8 + 4 * ix + at, 1), :] for at in (-2, -1, 4, 5)]
        half = 0.5 * adv[0, v]
        rows += [0.5 * near[0] + (-half - 2.0) * near[1], 0.5 * near[1],
                 0.5 * near[2], (half - 2.0) * near[2] + 0.5 * near[3]]
    rows = jnp.concatenate(rows + [jnp.zeros((4, 4 * px), F32)], axis=0)
    r, c = iota((4 * px, 8 * px), 0), iota((4 * px, 8 * px), 1)
    pick = one_hot(r == ((c >> 3) << 2) + (c & 3))
    hi, lo = split(rows)
    rows = dot(hi, pick) + dot(lo, pick)
    own = ((iota((8, 8 * px), 1) >> 2) & 1) == (iota((8, 8 * px), 0) >> 2)
    for t in range(3):
        LX[t] = jnp.where(own, rows[8 * t : 8 * t + 8], 0.0)

    def build_reduced(axis, n, lines, out):
        shift = log2(lines)
        cols = 4 * n * lines
        pick = one_hot(iota((4 * n, cols), 0) == (iota((4 * n, cols), 1) >> shift))
        pick = jnp.concatenate([pick, pick], axis=0)
        spread = []
        for v in range(VARS):
            near = [RP[axis, v, pl.ds(8 + at, n, stride=4), :] for at in (-2, -1, 4, 5)]
            half = 0.5 * adv[axis + 1, v]
            rows = [0.5 * near[0] + (-half - 2.0) * near[1], 0.5 * near[1],
                    0.5 * near[2], (half - 2.0) * near[2] + 0.5 * near[3]]
            spread.append(dot(jnp.concatenate(split(jnp.concatenate(rows, axis=0)), axis=1), pick))
        which = iota((n, cols), 1) & (lines - 1)
        for v in range(VARS):
            for k in range(4):
                for line in range(lines):
                    block = jnp.where(which == line, spread[v][n * k : n * k + n], 0.0)
                    out[v, pl.ds(k * lines + line, n, stride=4 * lines), :] = block

    build_reduced(0, py, zc, KY)
    build_reduced(1, pz, yc, KZ)

    def build_columns(v, carry):
        SY[v] = columns(inv_y[v], CY)
        SZ[v] = columns(inv_z[v], CZ)
        return carry

    lax.fori_loop(0, VARS, build_columns, 0, unroll=True)

    def exchange(axis, me, n, rows, src, dst, v, send, recv):
        mine = pl.ds(pl.multiple_of(me * rows, rows), rows)
        for d in others(n):
            to = peer(axis, d)
            there = pl.ds(pl.multiple_of(to[axis] * rows, rows), rows)
            remote(src.at[v, there], dst.at[v, mine], send, recv, to).start()
        dst[v, mine, :] = src[v, mine, :]

    faces = ((0, 0), (0, 1), (1, 6), (1, 7))

    def local_y(group):
        for v in group:
            XL[v] = XL[v] - nt2(CT[v >> 1], WX[v])
        for v in group:
            for g in range(4):
                solved = mm2(MY[v], XL[v, 128 * g : 128 * g + 128, :])
                for k in range(16):
                    z, h = 8 * g + k // 2, k & 1
                    FG[v, h, 8 * z : 8 * z + 8, :] = solved[8 * k : 8 * k + 8]
        for v in group:
            for h in range(2):
                G[v, h] = mm2(MZ[v], FG[v, h])
        for v in group:
            for h in range(2):
                for k, z in enumerate((0, 1, CZ - 2, CZ - 1)):
                    ZF[v, pl.ds(yc * k + h, 8, stride=zr), :] = G[v, h, 8 * z : 8 * z + 8, :]
            exchange("gz", iz, pz, zr, ZF, ZR1, v, zsem, zr1s.at[v])
        for v in group:
            for k, (h, y) in enumerate(faces):
                for t in range(zc):
                    YF[v, pl.ds(zc * k + t, 8, stride=yr), :] = G[v, h, pl.ds(64 * t + y, 8, stride=8), :]
            exchange("gy", iy, py, yr, YF, YR1, v, ysem, yr1s.at[v])

    heard(3)
    for t, group in enumerate(groups):
        drain(XR.at[t, pl.ds(0, px - 1)], xrv.at[t])
        factors = mm3(*split(LX[t]), XR[t].reshape(8 * px, ROWS))
        factors = jnp.concatenate([factors, jnp.zeros((CX - 8, ROWS), F32)], axis=0).T
        CT[t] = jnp.concatenate(split(factors), axis=1)
        local_y(group)
        if t == 1:
            drain(STX.at[pl.ds(0, px - 1)], sr.at[0])
            STY[iy] = combine(STX, px)
            for d in others(py):
                remote(STY.at[iy], STY.at[iy], ss.at[1], sr.at[1], peer("gy", d)).start()
    def both_parts(matrix):
        return jnp.concatenate(split(matrix), axis=0)

    def reduced_z(v):
        drain(ZR1.at[v, pl.ds(0, (pz - 1) * zr)], zr1s.at[v])
        Z2[v] = mm2(both_parts(KZ[v]), ZR1[v])
        exchange("gz", iz, pz, zr, Z2, ZR2, v, z2sem, zr2s.at[v])

    def reduced_y(v):
        drain(YR1.at[v, pl.ds(0, (py - 1) * yr)], yr1s.at[v])
        Y2[v] = mm2(both_parts(KY[v]), YR1[v])
        exchange("gy", iy, py, yr, Y2, YR2, v, y2sem, yr2s.at[v])

    for v in range(VARS):
        reduced_z(v)
        reduced_y(v)
    drain(STY.at[pl.ds(0, py - 1)], sr.at[1])
    STZ[iz] = combine(STY, py)
    for d in others(pz):
        remote(STZ.at[iz], STZ.at[iz], ss.at[2], sr.at[2], peer("gz", d)).start()

    def correct_z(v, carry):
        drain(ZR2.at[v, pl.ds(0, (pz - 1) * zr)], zr2s.at[v])
        for k, (h, y) in enumerate(faces):
            E[v, 4 * k : 4 * k + 4, :] = ZR2[v, pl.ds(zr * y + h, 4, stride=yc), :]
        mine = pl.ds(pl.multiple_of(16 * iy, 16), 16)
        for d in others(py):
            remote(E.at[v], ER.at[v, mine], es, ers.at[v], peer("gy", d)).start()
        ER[v, mine, :] = E[v]
        factor = [[ZR2[v, pl.ds(yc * k + h, 8, stride=zr), :] for h in range(2)] for k in range(4)]
        for z in range(CZ):
            weight = [jnp.broadcast_to(SZ[v, z : z + 1, CX * k : CX * k + CX], (8, CX)) for k in range(4)]
            for h in range(2):
                total = G[v, h, 8 * z : 8 * z + 8, :]
                for k in range(4):
                    total = total - weight[k] * factor[k][h]
                G[v, h, 8 * z : 8 * z + 8, :] = total
        return carry

    lax.fori_loop(0, VARS, correct_z, 0, unroll=True)
    drain(STZ.at[pl.ds(0, pz - 1)], sr.at[2])
    stats = combine(STZ, pz)
    step = 8000.0 / stats[VARS : VARS + 1]
    rms[...] = jnp.sqrt(stats / float(px * py * pz * ROWS * CX))

    def finish(v, carry):
        drain(YR2.at[v, pl.ds(0, (py - 1) * yr)], yr2s.at[v])
        drain(ER.at[v, pl.ds(0, (py - 1) * 16)], ers.at[v])
        cross = mm2(both_parts(KY[v, pl.ds(pl.multiple_of(16 * iy, 16), 16), :]), ER[v])
        for t in range(zc):
            weight = [SZ[v, 8 * t : 8 * t + 8, CX * j : CX * j + CX] for j in range(4)]
            for k in range(4):
                total = YR2[v, pl.ds(zc * k + t, 8, stride=yr), :]
                for j in range(4):
                    total = total - weight[j] * jnp.broadcast_to(cross[4 * k + j : 4 * k + j + 1], (8, CX))
                CF[k, 8 * t : 8 * t + 8, :] = total
        column = [SY[v, :, CX * k : CX * k + CX] * step for k in range(4)]
        for z in range(CZ):
            line = [jnp.broadcast_to(CF[k, z : z + 1, :], (8, CX)) for k in range(4)]
            for h in range(2):
                total = step * G[v, h, 8 * z : 8 * z + 8, :]
                for k in range(4):
                    total = total - column[k][8 * h : 8 * h + 8] * line[k]
                F[v, z * PLANE + 8 * h : z * PLANE + 8 * h + 8, :] = total
        return carry

    lax.fori_loop(0, VARS, finish, 0, unroll=True)
    for copy in halos:
        copy.wait_send()
    drain(XR.at[:, pl.ds(0, px - 1)], xs)
    drain(STX.at[pl.ds(0, px - 1)], ss.at[0])
    drain(STY.at[pl.ds(0, py - 1)], ss.at[1])
    drain(STZ.at[pl.ds(0, pz - 1)], ss.at[2])
    drain(YF.at[:, pl.ds(0, (py - 1) * yr)], ysem)
    drain(Y2.at[:, pl.ds(0, (py - 1) * yr)], y2sem)
    drain(ZF.at[:, pl.ds(0, (pz - 1) * zr)], zsem)
    drain(Z2.at[:, pl.ds(0, (pz - 1) * zr)], z2sem)
    drain(ER.at[:, pl.ds(0, (py - 1) * 16)], es)


def shards(px, py, pz, flow_state, advection, *tables):
    vmem = pl.BlockSpec(memory_space=pltpu.VMEM)
    hbm = pl.BlockSpec(memory_space=pltpu.HBM)
    f32 = lambda *shape: pltpu.VMEM(shape, F32)
    b16 = lambda *shape: pltpu.VMEM(shape, BF16)
    dma = pltpu.SemaphoreType.DMA
    field = (VARS, ROWS, CX)
    padded_rows = ROWS + 4 * PLANE
    y_face, z_face = (VARS, 4 * CZ, CX), (VARS, 4 * CY, CX)
    update, rms = pl.pallas_call(
        functools.partial(kernel, px, py, pz),
        out_shape=(jax.ShapeDtypeStruct(field, F32), jax.ShapeDtypeStruct((8, CX), F32)),
        in_specs=[hbm] * 8,
        out_specs=(vmem, vmem),
        scratch_shapes=[
            pltpu.SMEM(advection.shape, F32), *[f32(*table.shape) for table in tables[:3]], f32(VARS, 4 * px + 16, 4 * px),
            f32(2, VARS, 4 * max(py, pz) + 16, 4 * max(py, pz)),
            f32(VARS, padded_rows, CX), f32(3, padded_rows, CX), f32(4, padded_rows, CX),
            f32(2, VARS, 2 * CZ, CX), f32(2, VARS, 2 * CZ, CX), f32(4, VARS, CZ, CX),
            f32(VARS, CY, CX), f32(2, VARS, CY, CX), f32(VARS, CY, CX),
            b16(VARS, ROWS, 2 * CX), f32(*field), f32(VARS, 2, ROWS // 2, CX), f32(VARS, 2, ROWS // 2, CX),
            f32(3, px, 8, ROWS), b16(3, ROWS, 2 * CX),
            *[f32(*y_face)] * 4, *[f32(*z_face)] * 4,
            f32(VARS, 16, CX), f32(VARS, 16 * py, CX), f32(4, CZ, CX),
            f32(px, 8, CX), f32(py, 8, CX), f32(pz, 8, CX),
            b16(VARS, 2 * CX, 2 * CX), b16(VARS, 2 * CX, 2 * CX), f32(3, 8, 8 * px),
            b16(VARS, 2 * CX, CX), b16(VARS, 512, 256),
            f32(VARS, 4 * CZ, 4 * CZ), f32(VARS, 4 * CY, 4 * CY),
            f32(VARS, CY, 4 * CX), f32(VARS, CZ, 4 * CX),
            dma((8,)), dma((6,)), dma((6,)), dma, dma((3,)),
            *[dma, dma((VARS,))] * 5,
            dma((3,)), dma((3,)), pltpu.SemaphoreType.REGULAR((3, 3)),
        ],
        compiler_params=pltpu.CompilerParams(
            collective_id=0, has_side_effects=True, vmem_limit_bytes=32 * 1024 * 1024
        ),
        name="adi_step",
    )(*[pltpu.with_memory_space_constraint(x, pltpu.HBM) for x in (advection, flow_state.reshape(field), *tables)])
    return update.reshape(flow_state.shape), rms[:VARS, 0]


def solution(mesh):
    sizes = [mesh.shape[axis] for axis in ("gx", "gy", "gz")]
    return jax.shard_map(
        functools.partial(shards, *sizes),
        mesh=mesh,
        in_specs=(P(None, "gz", "gy", "gx"), P(), P(), P(), P(), P(), P(), P()),
        out_specs=(P(None, "gz", "gy", "gx"), P()),
        check_vma=False,
    )
```

```python
import functools

import jax
import jax.numpy as jnp
from jax import lax
from jax.experimental import pallas as pl
from jax.experimental.pallas import tpu as pltpu
from jax.sharding import PartitionSpec as P

VARS, CX, CY, CZ = 5, 128, 16, 32
PLANE = CY
ROWS = CZ * CY
F32, BF16 = jnp.float32, jnp.bfloat16
MESH = pl.DeviceIdType.MESH
NT = (((1,), (1,)), ((), ()))


def iota(shape, dim):
    return lax.broadcasted_iota(jnp.int32, shape, dim)


def log2(n):
    return n.bit_length() - 1


def split(x):
    hi = x.astype(BF16)
    return hi, (x - hi.astype(F32)).astype(BF16)


def dot(a, b):
    return jnp.dot(a, b, preferred_element_type=F32)


def dot_nt(a, b):
    return lax.dot_general(a, b, NT, preferred_element_type=F32)


def mm2(left, right):
    wide = dot(left, jnp.concatenate(split(right), axis=1))
    m, n = left.shape[0] // 2, right.shape[1]
    return (wide[:m, :n] + wide[:m, n:]) + wide[m:, :n]


def nt2(left, right):
    wide = dot_nt(left, right)
    n = right.shape[0] // 2
    return wide[:, :n] + wide[:, n:]


def mm3(left_hi, left_lo, right):
    hi, lo = split(right)
    return dot(left_hi, hi) + (dot(left_hi, lo) + dot(left_lo, hi))


def one_hot(cond):
    return jnp.where(cond, 1.0, 0.0).astype(BF16)


def edge(k, length):
    return jnp.where(k < 2, k, k + (length - 4))


def primitives(u):
    scale = 1.0 / u[0]
    vel = [u[1] * scale, u[2] * scale, u[3] * scale]
    kinetic = 0.5 * (vel[0] * vel[0] + vel[1] * vel[1] + vel[2] * vel[2])
    internal = jnp.maximum(u[4] * scale - kinetic, 0.25)
    return vel, internal, 0.4 * u[0] * internal


def fluxes(u, w, pressure, direction):
    out = [u[1 + direction]]
    for c in range(3):
        moment = u[1 + c] * w
        out.append(moment + pressure if c == direction else moment)
    return out + [(u[4] + pressure) * w]


def kernel(
    px, py, pz,
    tab_adv, flow, *refs,
):
    (
        tab_x, tab_y, tab_z, tab_rx, tab_ry, tab_rz,
        F, rms,
        adv, inv_x, inv_y, inv_z, RX, RP,
        U, PR, FZ, YS, YH, HY, PK, XH, XC, FS, XL, G, FG, XR, CT,
        YF, YR1, Y2, YR2, ZF, ZR1, Z2, ZR2, E, ER, CF, STX, STY, STZ,
        AX, WX, LX, MY, MZ, KY, KZ, SY, SZ,
        in_sem, hs, hr, xs, xrv, ysem, yr1s, y2sem, yr2s, zsem, zr1s, z2sem, zr2s, es, ers, ss, sr, known,
    ) = refs
    ix, iy, iz = lax.axis_index("gx"), lax.axis_index("gy"), lax.axis_index("gz")
    zc, yc = CZ // py, CY // pz
    yr, zr = 4 * zc, 4 * yc

    def peer(axis, d):
        me, n = {"gx": (ix, px), "gy": (iy, py), "gz": (iz, pz)}[axis]
        return {axis: (me + d + n) & (n - 1)}

    def remote(src, dst, send, recv, device):
        return pltpu.make_async_remote_copy(
            src_ref=src, dst_ref=dst, send_sem=send, recv_sem=recv,
            device_id=device, device_id_type=MESH,
        )

    def others(n):
        return sorted(range(1, n), key=lambda d: -min(d, n - d))

    def drain(ref, sem):
        pltpu.make_async_copy(ref, ref, sem).wait()

    load = pltpu.make_async_copy(flow, U.at[:, pl.ds(2 * PLANE, ROWS)], in_sem.at[0])
    load.start()
    tables = [
        pltpu.make_async_copy(src, dst, in_sem.at[1 + k])
        for k, (src, dst) in enumerate(zip(
            (tab_adv, tab_x, tab_y, tab_z, tab_rx, tab_ry, tab_rz),
            (adv, inv_x, inv_y, inv_z, RX.at[:, pl.ds(8, 4 * px)], RP.at[0, :, pl.ds(8, 4 * py)], RP.at[1, :, pl.ds(8, 4 * pz)]),
        ))
    ]
    for copy in tables:
        copy.start()
    for axis, n in enumerate((py, pz)):
        for start in (0, 8 + 4 * n):
            RP[axis, :, start : start + 8, :] = jnp.zeros((VARS, 8, 4 * n), F32)
    for start in (0, 8 + 4 * px):
        RX[:, start : start + 8, :] = jnp.zeros((VARS, 8, 4 * px), F32)
    barrier = pltpu.get_barrier_semaphore()
    axes = (("gz", pz), ("gy", py), ("gx", px))
    for axis, _ in axes:
        for d in (1, -1):
            pl.semaphore_signal(barrier, inc=1, device_id=peer(axis, d), device_id_type=MESH)

    def spread(turn):
        for a, (axis, n) in enumerate(axes):
            if turn < n // 2:
                for d in (1, -1):
                    pl.semaphore_signal(known.at[a, turn - 1], inc=1, device_id=peer(axis, d), device_id_type=MESH)

    def heard(turn):
        for a, (axis, n) in enumerate(axes):
            if turn < n // 2:
                pl.semaphore_wait(known.at[a, turn - 1], 2)

    load.wait()

    def pack_rows(v, carry):
        for r in range(2):
            for t in range(CZ // 8):
                for side, first in ((0, CY - 2), (1, 0)):
                    start = 2 * PLANE + 8 * t * PLANE + first + r
                    YS[side, v, pl.ds(r * CZ + 8 * t, 8), :] = U[v, pl.ds(start, 8, stride=PLANE), :]
        return carry

    lax.fori_loop(0, VARS, pack_rows, 0, unroll=True)
    lane = iota((CY, CX), 1)
    row = iota((CY, CX), 0)

    pl.semaphore_wait(barrier, 6)
    spread(1)
    last = 2 * PLANE + ROWS
    halos = [
        remote(flow.at[:, pl.ds(ROWS - 2 * PLANE, 2 * PLANE)], U.at[:, pl.ds(0, 2 * PLANE)],
               hs.at[0], hr.at[0], peer("gz", 1)),
        remote(flow.at[:, pl.ds(0, 2 * PLANE)], U.at[:, pl.ds(last, 2 * PLANE)],
               hs.at[1], hr.at[1], peer("gz", -1)),
        remote(YS.at[0], YH.at[0], hs.at[2], hr.at[2], peer("gy", 1)),
        remote(YS.at[1], YH.at[1], hs.at[3], hr.at[3], peer("gy", -1)),
        remote(PK, XH.at[0], hs.at[4], hr.at[4], peer("gx", 1)),
        remote(PK, XH.at[1], hs.at[5], hr.at[5], peer("gx", -1)),
    ]
    for copy in halos[:4]:
        copy.start()
    def pack_lanes(v, carry):
        acc = jnp.zeros((CY, CX), F32)
        for z in range(CZ):
            plane = U[v, pl.ds((2 + z) * PLANE, PLANE), :]
            acc = jnp.where((lane >> 2) == z, pltpu.roll(plane, (4 * z + 2) % CX, 1), acc)
        PK[v] = acc
        return carry

    lax.fori_loop(0, VARS, pack_lanes, 0, unroll=True)
    for copy in halos[4:]:
        copy.start()

    def plane_primitives(base):
        here = pl.ds(base, PLANE)
        u = [U[v, here, :] for v in range(VARS)]
        vel, internal, pressure = primitives(u)
        PR[0, here, :], PR[1, here, :], PR[2, here, :] = vel[0], vel[1], pressure
        for k, f in enumerate(fluxes(u, vel[2], pressure, 2)[1:]):
            FZ[k, here, :] = f
        return vel, internal

    top = jnp.zeros((CY, CX), F32)
    for z in range(CZ):
        vel, internal = plane_primitives((2 + z) * PLANE)
        speed = jnp.abs(vel[0]) + jnp.abs(vel[1]) + jnp.abs(vel[2]) + jnp.sqrt(3.0 * 1.4 * 0.4 * internal)
        top = jnp.maximum(top, speed)

    for copy in tables:
        copy.wait()
    def columns(table, length):
        shape = (length, 4 * CX)
        pick = one_hot(iota(shape, 0) == edge(iota(shape, 1) >> 7, length))
        hi, lo = split(table)
        return dot(hi, pick) + dot(lo, pick)

    def build_first(v, carry):
        hi, lo = split(inv_x[v])
        AX[v] = jnp.concatenate([jnp.concatenate([hi, hi], 1), jnp.concatenate([lo, lo], 1)], 0)
        col = iota((CX, CX), 1)
        pick = one_hot(((col >> 2) == (v & 1)) & (iota((CX, CX), 0) == edge(col & 3, CX)))
        hi, lo = dot(hi, pick).astype(BF16), dot(lo, pick).astype(BF16)
        WX[v] = jnp.concatenate([jnp.concatenate([hi, hi], 1), jnp.concatenate([lo, lo], 1)], 0)

        pick = one_hot(iota((CY, CX), 0) == (iota((CY, CX), 1) & (CY - 1)))
        for part, table in enumerate(split(inv_y[v])):
            spread = dot(table, pick)
            for z in range(8):
                block = jnp.where((lane >> 4) == z, spread, 0.0)
                MY[v, part * CX + 16 * z : part * CX + 16 * z + 16, :] = block.astype(BF16)
        return carry

    lax.fori_loop(0, VARS, build_first, 0, unroll=True)
    ends = ((lane + 2) & (CX - 1)) < 4

    def residual_plane(group, z):
        base = pl.multiple_of(2 * PLANE + z * PLANE, PLANE)

        def at(ref, k, step):
            return ref[k, pl.ds(base + step * PLANE, PLANE), :]

        u = [at(U, v, 0) for v in range(VARS)]
        pressure = at(PR, 2, 0)
        x_flux = fluxes(u, at(PR, 0, 0), pressure, 0)
        y_flux = fluxes(u, at(PR, 1, 0), pressure, 1)
        for v in group:
            f = u[v]
            ahead, behind = at(U, v, 1), at(U, v, -1)
            if v == 0:
                slope = at(U, 3, 1) - at(U, 3, -1)
            else:
                slope = at(FZ, v - 1, 1) - at(FZ, v - 1, -1)

            far, quarter = -0.0625 * f, 0.25 * f
            half = 0.5 * y_flux[v]
            up = quarter + half + pltpu.roll(far, 1, 0)
            down = quarter - half + pltpu.roll(far, CY - 1, 0)
            r = pltpu.roll(up, 1, 0) + pltpu.roll(down, CY - 1, 0)
            half = 0.5 * x_flux[v]
            up = quarter + half + pltpu.roll(far, 1, 1)
            down = quarter - half + pltpu.roll(far, CX - 1, 1)
            r = r + (pltpu.roll(up, 1, 1) + pltpu.roll(down, CX - 1, 1))
            r = r + (0.25 * (ahead + behind) - 0.5 * slope)
            r = r - 0.0625 * (at(U, v, 2) + at(U, v, -2)) - 1.125 * f
            F[v, pl.ds(pl.multiple_of(z * PLANE, PLANE), PLANE), :] = r

    def interior(step, carry):
        for k in range(2):
            residual_plane(range(VARS), 2 + 2 * step + k)
        return carry

    lax.fori_loop(0, (CZ - 4) // 2, interior, 0)

    def build_z(v, carry):
        wide = iota((CZ, 8 * CZ), 1)
        pick = one_hot(iota((CZ, 8 * CZ), 0) == (wide >> 3))
        r, c = iota((16, 8 * CZ), 0), iota((16, 8 * CZ), 1)
        keep, first = (r & 7) == (c & 7), r < 8
        for part, table in enumerate(split(inv_z[v])):
            spread = dot(table, pick)
            for k in range(CZ // 2):
                pair = [jnp.broadcast_to(spread[z : z + 1], (16, 8 * CZ)) for z in (2 * k, 2 * k + 1)]
                block = jnp.where(keep, jnp.where(first, pair[0], pair[1]), 0.0)
                MZ[v, part * 256 + 16 * k : part * 256 + 16 * k + 16, :] = block.astype(BF16)
        return carry

    lax.fori_loop(0, VARS, build_z, 0, unroll=True)
    heard(1)
    spread(2)
    for copy in halos:
        copy.wait_recv()
    plane_primitives(PLANE)
    plane_primitives(last)
    for side in range(2):
        half = 0.5 - side
        parts = []
        for ref, which in ((YH, side), (YS, side)):
            near, far = pl.ds((1 - side) * CZ, CZ), pl.ds(side * CZ, CZ)
            u = [ref[which, v, near, :] for v in range(VARS)]
            vel, _, pressure = primitives(u)
            parts.append([
                (-0.0625 * u[v], 0.25 * u[v] + half * f - 0.0625 * ref[which, v, far, :])
                for v, f in enumerate(fluxes(u, vel[1], pressure, 1))
            ])
        for v in range(VARS):
            for k in range(2):
                HY[2 * side + k, v] = parts[0][v][k] - parts[1][v][k]
    j = lane & 3
    near = [jnp.where(j < 2, XH[0, v], XH[1, v]) for v in range(VARS)]
    mine = [PK[v] for v in range(VARS)]
    vel, _, pressure = primitives(near)
    near_flux = fluxes(near, vel[0], pressure, 0)
    vel, _, pressure = primitives(mine)
    mine_flux = fluxes(mine, vel[0], pressure, 0)
    for v in range(VARS):
        du, df = near[v] - mine[v], near_flux[v] - mine_flux[v]
        far = -0.0625 * jnp.where(j < 2, pltpu.roll(du, CX - 2, 1), pltpu.roll(du, 2, 1))
        right = pltpu.roll(-0.5 * df + 0.25 * du, CX - 1, 1)
        left = pltpu.roll(0.5 * df + 0.25 * du, 1, 1)
        XC[v] = far + jnp.where(j == 1, right, 0.0) + jnp.where(j == 2, left, 0.0)

    row8 = iota((8, 4 * CX), 0)
    groups = ((0, 1), (2, 3), (4,))
    sums = []
    for t, group in enumerate(groups):

        for z in (0, 1, CZ - 2, CZ - 1):
            residual_plane(group, z)
        for v in group:
            for k, y in ((1, 0), (0, 1), (2, CY - 2), (3, CY - 1)):
                for c in range(CZ // 8):
                    lines = pl.ds(8 * c * PLANE + y, 8, stride=PLANE)
                    F[v, lines, :] = F[v, lines, :] + HY[k, v, 8 * c : 8 * c + 8, :]

        for v in group:
            total = jnp.zeros((CY, CX), F32)
            for z in range(CZ):
                here = slice(z * PLANE, z * PLANE + PLANE)
                r = F[v, here, :] + jnp.where(ends, pltpu.roll(XC[v], (2 * CX - 2 - 4 * z) % CX, 1), 0.0)
                total = total + r * r
                FS[v, here, 0:CX], FS[v, here, CX : 2 * CX] = split(r)
            sums.append(total)
        pair = [jnp.zeros((8, ROWS), F32)] * 2
        for v in group:
            tile = jnp.where(iota((8, CX), 0) < 2, inv_x[v, 0:8, :], pltpu.roll(inv_x[v, CX - 8 : CX, :], 4, 0))
            if v & 1:
                tile = pltpu.roll(tile, 4, 0)
            hi, lo = split(tile)
            left = jnp.concatenate([jnp.concatenate([hi, hi], 1), jnp.concatenate([lo, lo], 1)], 0)
            both = dot_nt(left, FS[v])
            pair[v & 1] = both[0:8] + both[8:16]
        XR[t, ix] = jnp.where(row8 < 4, pair[0], pair[1])
        for d in others(px):
            remote(XR.at[t, ix], XR.at[t, ix], xs, xrv.at[t], peer("gx", d)).start()

    heard(2)
    spread(3)
    stat_row = iota((8, CX), 0)
    tile = jnp.where(stat_row == VARS, jnp.max(top), 0.0)
    for v in range(VARS):
        tile = jnp.where(stat_row == v, jnp.sum(sums[v]), tile)
    STX[ix] = tile
    for d in others(px):
        remote(STX.at[ix], STX.at[ix], ss.at[0], sr.at[0], peer("gx", d)).start()

    def combine(ref, n):
        total = ref[0]
        for k in range(1, n):
            total = jnp.where(stat_row == VARS, jnp.maximum(total, ref[k]), total + ref[k])
        return total

    def local_x(v, carry):
        XL[v] = nt2(FS[v], AX[v])
        return carry

    lax.fori_loop(0, VARS, local_x, 0, unroll=True)

    rows = []
    for v in range(VARS):
        near = [RX[v, pl.ds(8 + 4 * ix + at, 1), :] for at in (-2, -1, 4, 5)]
        half = 0.5 * adv[0, v]
        rows += [0.5 * near[0] + (-half - 2.0) * near[1], 0.5 * near[1],
                 0.5 * near[2], (half - 2.0) * near[2] + 0.5 * near[3]]
    rows = jnp.concatenate(rows + [jnp.zeros((4, 4 * px), F32)], axis=0)
    r, c = iota((4 * px, 8 * px), 0), iota((4 * px, 8 * px), 1)
    pick = one_hot(r == ((c >> 3) << 2) + (c & 3))
    hi, lo = split(rows)
    rows = dot(hi, pick) + dot(lo, pick)
    own = ((iota((8, 8 * px), 1) >> 2) & 1) == (iota((8, 8 * px), 0) >> 2)
    for t in range(3):
        LX[t] = jnp.where(own, rows[8 * t : 8 * t + 8], 0.0)

    def build_reduced(axis, n, lines, out):
        shift = log2(lines)
        cols = 4 * n * lines
        pick = one_hot(iota((4 * n, cols), 0) == (iota((4 * n, cols), 1) >> shift))
        pick = jnp.concatenate([pick, pick], axis=0)
        spread = []
        for v in range(VARS):
            near = [RP[axis, v, pl.ds(8 + at, n, stride=4), :] for at in (-2, -1, 4, 5)]
            half = 0.5 * adv[axis + 1, v]
            rows = [0.5 * near[0] + (-half - 2.0) * near[1], 0.5 * near[1],
                    0.5 * near[2], (half - 2.0) * near[2] + 0.5 * near[3]]
            spread.append(dot(jnp.concatenate(split(jnp.concatenate(rows, axis=0)), axis=1), pick))
        which = iota((n, cols), 1) & (lines - 1)
        for v in range(VARS):
            for k in range(4):
                for line in range(lines):
                    block = jnp.where(which == line, spread[v][n * k : n * k + n], 0.0)
                    out[v, pl.ds(k * lines + line, n, stride=4 * lines), :] = block

    build_reduced(0, py, zc, KY)
    build_reduced(1, pz, yc, KZ)

    def build_columns(v, carry):
        SY[v] = columns(inv_y[v], CY)
        SZ[v] = columns(inv_z[v], CZ)
        return carry

    lax.fori_loop(0, VARS, build_columns, 0, unroll=True)

    def exchange(axis, me, n, rows, src, dst, v, send, recv):
        mine = pl.ds(pl.multiple_of(me * rows, rows), rows)
        for d in others(n):
            to = peer(axis, d)
            there = pl.ds(pl.multiple_of(to[axis] * rows, rows), rows)
            remote(src.at[v, there], dst.at[v, mine], send, recv, to).start()
        dst[v, mine, :] = src[v, mine, :]

    faces = ((0, 0), (0, 1), (1, 6), (1, 7))

    def local_y(group):
        for v in group:
            XL[v] = XL[v] - nt2(CT[v >> 1], WX[v])
        for v in group:
            for g in range(4):
                solved = mm2(MY[v], XL[v, 128 * g : 128 * g + 128, :])
                for k in range(16):
                    z, h = 8 * g + k // 2, k & 1
                    FG[v, h, 8 * z : 8 * z + 8, :] = solved[8 * k : 8 * k + 8]

    def local_z(group):
        for v in group:
            for h in range(2):
                G[v, h] = mm2(MZ[v], FG[v, h])
        for v in group:
            for h in range(2):
                for k, z in enumerate((0, 1, CZ - 2, CZ - 1)):
                    ZF[v, pl.ds(yc * k + h, 8, stride=zr), :] = G[v, h, 8 * z : 8 * z + 8, :]
            exchange("gz", iz, pz, zr, ZF, ZR1, v, zsem, zr1s.at[v])
        for v in group:
            for k, (h, y) in enumerate(faces):
                for t in range(zc):
                    YF[v, pl.ds(zc * k + t, 8, stride=yr), :] = G[v, h, pl.ds(64 * t + y, 8, stride=8), :]
            exchange("gy", iy, py, yr, YF, YR1, v, ysem, yr1s.at[v])

    def line_factors(t):
        drain(XR.at[t, pl.ds(0, px - 1)], xrv.at[t])
        factors = mm3(*split(LX[t]), XR[t].reshape(8 * px, ROWS))
        factors = jnp.concatenate([factors, jnp.zeros((CX - 8, ROWS), F32)], axis=0).T
        CT[t] = jnp.concatenate(split(factors), axis=1)

    heard(3)
    line_factors(0)
    for t, group in enumerate(groups):
        local_y(group)
        if t < 2:
            line_factors(t + 1)
        local_z(group)
        if t == 1:
            drain(STX.at[pl.ds(0, px - 1)], sr.at[0])
            STY[iy] = combine(STX, px)
            for d in others(py):
                remote(STY.at[iy], STY.at[iy], ss.at[1], sr.at[1], peer("gy", d)).start()
    def both_parts(matrix):
        return jnp.concatenate(split(matrix), axis=0)

    def reduced_z(v):
        drain(ZR1.at[v, pl.ds(0, (pz - 1) * zr)], zr1s.at[v])
        Z2[v] = mm2(both_parts(KZ[v]), ZR1[v])
        exchange("gz", iz, pz, zr, Z2, ZR2, v, z2sem, zr2s.at[v])

    def reduced_y(v):
        drain(YR1.at[v, pl.ds(0, (py - 1) * yr)], yr1s.at[v])
        Y2[v] = mm2(both_parts(KY[v]), YR1[v])
        exchange("gy", iy, py, yr, Y2, YR2, v, y2sem, yr2s.at[v])

    for v in range(VARS):
        reduced_z(v)
        reduced_y(v)
    drain(STY.at[pl.ds(0, py - 1)], sr.at[1])
    STZ[iz] = combine(STY, py)
    for d in others(pz):
        remote(STZ.at[iz], STZ.at[iz], ss.at[2], sr.at[2], peer("gz", d)).start()

    def correct_z(v, carry):
        drain(ZR2.at[v, pl.ds(0, (pz - 1) * zr)], zr2s.at[v])
        for k, (h, y) in enumerate(faces):
            E[v, 4 * k : 4 * k + 4, :] = ZR2[v, pl.ds(zr * y + h, 4, stride=yc), :]
        mine = pl.ds(pl.multiple_of(16 * iy, 16), 16)
        for d in others(py):
            remote(E.at[v], ER.at[v, mine], es, ers.at[v], peer("gy", d)).start()
        ER[v, mine, :] = E[v]
        factor = [[ZR2[v, pl.ds(yc * k + h, 8, stride=zr), :] for h in range(2)] for k in range(4)]
        for z in range(CZ):
            weight = [jnp.broadcast_to(SZ[v, z : z + 1, CX * k : CX * k + CX], (8, CX)) for k in range(4)]
            for h in range(2):
                total = G[v, h, 8 * z : 8 * z + 8, :]
                for k in range(4):
                    total = total - weight[k] * factor[k][h]
                G[v, h, 8 * z : 8 * z + 8, :] = total
        return carry

    lax.fori_loop(0, VARS, correct_z, 0, unroll=True)
    drain(STZ.at[pl.ds(0, pz - 1)], sr.at[2])
    stats = combine(STZ, pz)
    step = 8000.0 / stats[VARS : VARS + 1]
    rms[...] = jnp.sqrt(stats / float(px * py * pz * ROWS * CX))

    def finish(v, carry):
        drain(YR2.at[v, pl.ds(0, (py - 1) * yr)], yr2s.at[v])
        drain(ER.at[v, pl.ds(0, (py - 1) * 16)], ers.at[v])
        cross = mm2(both_parts(KY[v, pl.ds(pl.multiple_of(16 * iy, 16), 16), :]), ER[v])
        for t in range(zc):
            weight = [SZ[v, 8 * t : 8 * t + 8, CX * j : CX * j + CX] for j in range(4)]
            for k in range(4):
                total = YR2[v, pl.ds(zc * k + t, 8, stride=yr), :]
                for j in range(4):
                    total = total - weight[j] * jnp.broadcast_to(cross[4 * k + j : 4 * k + j + 1], (8, CX))
                CF[k, 8 * t : 8 * t + 8, :] = total
        column = [SY[v, :, CX * k : CX * k + CX] * step for k in range(4)]
        for z in range(CZ):
            line = [jnp.broadcast_to(CF[k, z : z + 1, :], (8, CX)) for k in range(4)]
            for h in range(2):
                total = step * G[v, h, 8 * z : 8 * z + 8, :]
                for k in range(4):
                    total = total - column[k][8 * h : 8 * h + 8] * line[k]
                F[v, z * PLANE + 8 * h : z * PLANE + 8 * h + 8, :] = total
        return carry

    lax.fori_loop(0, VARS, finish, 0, unroll=True)
    for copy in halos:
        copy.wait_send()
    drain(XR.at[:, pl.ds(0, px - 1)], xs)
    drain(STX.at[pl.ds(0, px - 1)], ss.at[0])
    drain(STY.at[pl.ds(0, py - 1)], ss.at[1])
    drain(STZ.at[pl.ds(0, pz - 1)], ss.at[2])
    drain(YF.at[:, pl.ds(0, (py - 1) * yr)], ysem)
    drain(Y2.at[:, pl.ds(0, (py - 1) * yr)], y2sem)
    drain(ZF.at[:, pl.ds(0, (pz - 1) * zr)], zsem)
    drain(Z2.at[:, pl.ds(0, (pz - 1) * zr)], z2sem)
    drain(ER.at[:, pl.ds(0, (py - 1) * 16)], es)


def shards(px, py, pz, flow_state, advection, *tables):
    vmem = pl.BlockSpec(memory_space=pltpu.VMEM)
    hbm = pl.BlockSpec(memory_space=pltpu.HBM)
    f32 = lambda *shape: pltpu.VMEM(shape, F32)
    b16 = lambda *shape: pltpu.VMEM(shape, BF16)
    dma = pltpu.SemaphoreType.DMA
    field = (VARS, ROWS, CX)
    padded_rows = ROWS + 4 * PLANE
    y_face, z_face = (VARS, 4 * CZ, CX), (VARS, 4 * CY, CX)
    update, rms = pl.pallas_call(
        functools.partial(kernel, px, py, pz),
        out_shape=(jax.ShapeDtypeStruct(field, F32), jax.ShapeDtypeStruct((8, CX), F32)),
        in_specs=[hbm] * 8,
        out_specs=(vmem, vmem),
        scratch_shapes=[
            pltpu.SMEM(advection.shape, F32), *[f32(*table.shape) for table in tables[:3]], f32(VARS, 4 * px + 16, 4 * px),
            f32(2, VARS, 4 * max(py, pz) + 16, 4 * max(py, pz)),
            f32(VARS, padded_rows, CX), f32(3, padded_rows, CX), f32(4, padded_rows, CX),
            f32(2, VARS, 2 * CZ, CX), f32(2, VARS, 2 * CZ, CX), f32(4, VARS, CZ, CX),
            f32(VARS, CY, CX), f32(2, VARS, CY, CX), f32(VARS, CY, CX),
            b16(VARS, ROWS, 2 * CX), f32(*field), f32(VARS, 2, ROWS // 2, CX), f32(VARS, 2, ROWS // 2, CX),
            f32(3, px, 8, ROWS), b16(3, ROWS, 2 * CX),
            *[f32(*y_face)] * 4, *[f32(*z_face)] * 4,
            f32(VARS, 16, CX), f32(VARS, 16 * py, CX), f32(4, CZ, CX),
            f32(px, 8, CX), f32(py, 8, CX), f32(pz, 8, CX),
            b16(VARS, 2 * CX, 2 * CX), b16(VARS, 2 * CX, 2 * CX), f32(3, 8, 8 * px),
            b16(VARS, 2 * CX, CX), b16(VARS, 512, 256),
            f32(VARS, 4 * CZ, 4 * CZ), f32(VARS, 4 * CY, 4 * CY),
            f32(VARS, CY, 4 * CX), f32(VARS, CZ, 4 * CX),
            dma((8,)), dma((6,)), dma((6,)), dma, dma((3,)),
            *[dma, dma((VARS,))] * 5,
            dma((3,)), dma((3,)), pltpu.SemaphoreType.REGULAR((3, 3)),
        ],
        compiler_params=pltpu.CompilerParams(
            collective_id=0, has_side_effects=True, vmem_limit_bytes=32 * 1024 * 1024
        ),
        name="adi_step",
    )(*[pltpu.with_memory_space_constraint(x, pltpu.HBM) for x in (advection, flow_state.reshape(field), *tables)])
    return update.reshape(flow_state.shape), rms[:VARS, 0]


def solution(mesh):
    sizes = [mesh.shape[axis] for axis in ("gx", "gy", "gz")]
    return jax.shard_map(
        functools.partial(shards, *sizes),
        mesh=mesh,
        in_specs=(P(None, "gz", "gy", "gx"), P(), P(), P(), P(), P(), P(), P()),
        out_specs=(P(None, "gz", "gy", "gx"), P()),
        check_vma=False,
    )
```
